128 devices in a mesh: angle: 8 (over z, x_hi), pos: 16 (over y, x_lo, core).
Axes of the slice: x: 4 (x_hi: 2, x_lo: 2; x = x_hi * 2 + x_lo), y: 4, z: 4, core: 2. Of those that a mesh axis runs over, the one named last changes fastest.
Arguments:
- amplitude: float32 [8, 64, 128, 128], P('angle', 'pos'), may hold values from 0 to 2.5
- offsets: int32 [8, 64, 2], P('angle', 'pos'), may hold values from 0 to 896, as said below
- probe_field: float32 [2, 128, 128], replicated, may hold values from -5 to 5
- object_field: float32 [8, 2, 1024, 1024], P('angle', None, 'pos'), may hold values from -5 to 5
- interp_index: int32 [8, 2, 1024], replicated, may hold values from 0 to 1022
- interp_weight: float32 [8, 2, 1024], replicated, may hold values from 0 to 1
Outputs:
- new_object: float32 [8, 2, 1024, 1024], P('angle', None, 'pos')
- new_probe: float32 [2, 128, 128], replicated
- recon: float32 [16, 64, 2, 1024], P('pos', 'angle')
The draws below stay inside these ranges and needn't reach their ends.
Inputs may be any that keep to these rules, and one draw needn't show every extreme that they name: For position j, offsets[a, j, 0] = max(0, min(896, (j // 4) * 64 - 128 // 2 + u)) with 0 <= u < 64; offsets[a, j, 1] lies in 0 to 896.
All inputs are finite; a program needn't handle non-finite values.
Results may differ from the reference program's by a relative error of at most 0.00007.
Values sent between devices are 32-bit elements; how exact they have to be, the bound alone decides.
A program may use at most 64 MiB of HBM per device.

```python
import math
import jax
import jax.numpy as jnp
from jax import lax

NOBJ = 1024
PATCH = 128
POS_DEV = 4
ZWIN = 2
ANGLES = 8
POSITIONS = 64
BAND = 64
N_POS = 16


def draw_offsets(key, part):
    key_rows = jax.random.fold_in(key, 11)
    key_cols = jax.random.fold_in(key, 12)
    owners = jnp.arange(POSITIONS, dtype=jnp.int32) // POS_DEV
    base = owners * BAND - PATCH // 2
    shifts = jax.random.randint(key_rows, (ANGLES, POSITIONS), 0, BAND, dtype=jnp.int32)
    first_rows = jnp.clip(base[None, :] + shifts, 0, NOBJ - PATCH)
    first_cols = jax.random.randint(key_cols, (ANGLES, POSITIONS), 0, NOBJ - PATCH + 1, dtype=jnp.int32)
    return jnp.stack([first_rows, first_cols], axis=-1).astype(jnp.int32)


def with_ends(array, own_key, low, high):
    longest = array.shape.index(max(array.shape))
    spots = []
    for shift in (0, 1):
        where = [jax.random.randint(jax.random.fold_in(own_key, axis), (), 0, length) for axis, length in enumerate(array.shape)]
        where[longest] = (where[longest] + shift) % array.shape[longest]
        spots.append(tuple(where))
    return array.at[spots[0]].set(low).at[spots[1]].set(high)


def block_scale(rng, dims, pieces, smallest, largest):
    factor_of, own = 1.0, jax.random.fold_in(rng, 6)
    for position, blocks in pieces:
        steps = jnp.exp(jax.random.uniform(jax.random.fold_in(own, position), (blocks,), jnp.float32, smallest / len(pieces), largest / len(pieces)))
        factor_of = factor_of * jnp.repeat(steps, dims[position] // blocks).reshape([-1 if axis == position else 1 for axis in range(len(dims))])
    return factor_of


def bell_draw(key, extent, scale, bound, split=(), kind=jnp.bfloat16):
    values = jax.random.normal(key, extent, jnp.float32) * scale
    if len(split) > 0:
        values = block_scale(key, extent, split, -0.22, 0.18) * values
    return jnp.clip(values, min=-bound, max=bound).astype(kind)


def setup_inputs(seed: int = 0) -> dict:
    seeds = jax.random.split(jax.random.key(seed), 7)
    amplitude = jnp.clip(2.5 * jax.random.uniform(seeds[0], (ANGLES, POSITIONS, PATCH, PATCH), jnp.float32) ** block_scale(seeds[0], (ANGLES, POSITIONS, PATCH, PATCH), ((0, 8), (1, 16)), -0.2, 0.2), 0.0, 2.5)
    offsets = draw_offsets(jax.random.fold_in(seeds[6], 71), 0)
    probe_field = bell_draw(seeds[2], (2, PATCH, PATCH), 0.8, 5.0, (), jnp.float32)
    object_field = bell_draw(seeds[3], (ANGLES, 2, NOBJ, NOBJ), 0.8, 5.0, ((0, 8), (2, 16)), jnp.float32)
    interp_index = with_ends(jax.random.randint(seeds[4], (ANGLES, ZWIN, NOBJ), 0, NOBJ - 1), jax.random.fold_in(seeds[4], 1), 0, (NOBJ - 1) - 1).astype(jnp.int32)
    interp_weight = jnp.clip(jax.random.uniform(seeds[5], (ANGLES, ZWIN, NOBJ), jnp.float32, 0.0, 1.0), 0.0, 1.0)
    return dict(amplitude=amplitude, offsets=offsets, probe_field=probe_field, object_field=object_field, interp_index=interp_index, interp_weight=interp_weight)


def ramp_matrix(length):
    ramp = jnp.arange(length, dtype=jnp.int32)
    differ = ramp[:, None] - ramp[None, :]
    spread = differ.astype(jnp.float32)
    squared = jnp.maximum(spread * spread, 1.0)
    odd_terms = jnp.where(differ % 2 != 0, -1.0 / (math.pi * math.pi * squared), 0.0)
    return jnp.where(differ == 0, 0.25, odd_terms).astype(jnp.float32)


def reference(amplitude, offsets, probe_field, object_field, interp_index, interp_weight):
    probe_c = lax.complex(probe_field[0], probe_field[1])
    power = probe_field[0] * probe_field[0] + probe_field[1] * probe_field[1]

    def one_angle(inputs):
        amps, places, layer = inputs
        field = lax.complex(layer[0], layer[1])

        def take_patch(place):
            return lax.dynamic_slice(field, (place[0], place[1]), (PATCH, PATCH))

        patches = jax.vmap(take_patch)(places)
        exit_wave = probe_c * patches
        spectrum = jnp.fft.fft2(exit_wave, norm="ortho")
        magnitude = jnp.abs(spectrum)
        fixed = spectrum * (amps / jnp.maximum(magnitude, 0.5))
        change = jnp.fft.ifft2(fixed, norm="ortho") - exit_wave
        contrib = jnp.conj(probe_c) * change
        numer = jnp.sum(jnp.conj(patches) * change, axis=0)
        denom = jnp.sum(jnp.real(patches) ** 2 + jnp.imag(patches) ** 2, axis=0)
        stacked = jnp.stack([jnp.real(contrib), jnp.imag(contrib), jnp.broadcast_to(power, contrib.shape)], axis=1)

        def accumulate(count, total):
            start = (jnp.int32(0), places[count, 0], places[count, 1])
            current = lax.dynamic_slice(total, start, (3, PATCH, PATCH))
            return lax.dynamic_update_slice(total, current + stacked[count], start)

        total = lax.fori_loop(0, POSITIONS, accumulate, jnp.zeros((3, NOBJ, NOBJ), jnp.float32))
        updated = layer + total[:2] / (total[2] + 1.0)
        return updated, jnp.stack([jnp.real(numer), jnp.imag(numer)]), denom

    new_object, numers, denoms = lax.map(one_angle, (amplitude, offsets, object_field))
    new_probe = probe_field + jnp.sum(numers, axis=0) / (jnp.sum(denoms, axis=0) + 1.0)
    sinogram = jnp.transpose(new_object[:, 1], (1, 0, 2))
    filtered = jnp.dot(sinogram.reshape(NOBJ * ANGLES, NOBJ), ramp_matrix(NOBJ), precision=lax.Precision.HIGHEST)
    filtered = jnp.moveaxis(filtered.reshape(NOBJ, ANGLES, NOBJ), 1, 0)

    def project_back(total, inputs):
        rows_angle, index_angle, weight_angle = inputs
        lower = jnp.take(rows_angle, index_angle, axis=1)
        upper = jnp.take(rows_angle, index_angle + 1, axis=1)
        return total + (1.0 - weight_angle) * lower + weight_angle * upper, None

    total, unused = lax.scan(project_back, jnp.zeros((NOBJ, ZWIN * NOBJ), jnp.float32),
                             (filtered, interp_index.reshape(ANGLES, ZWIN * NOBJ), interp_weight.reshape(ANGLES, ZWIN * NOBJ)))
    recon = (total * (math.pi / ANGLES)).reshape(N_POS, NOBJ // N_POS, ZWIN, NOBJ)
    return new_object, new_probe, recon
```

```python
import math

import jax
import jax.numpy as jnp
import ml_dtypes
import numpy as np
from jax import lax
from jax.experimental import pallas as pl
from jax.experimental.pallas import tpu as pltpu
from jax.sharding import PartitionSpec as P

MESH = pl.DeviceIdType.MESH
F32 = jnp.float32
BF16 = jnp.bfloat16
LANES = 128


def halves(table):
    high = table.astype(np.float32).astype(ml_dtypes.bfloat16)
    low = (table.astype(np.float32) - high.astype(np.float32)).astype(ml_dtypes.bfloat16)
    return high, low


def dft_constant(n):
    ramp = np.arange(n)
    theta = (ramp[:, None] * ramp[None, :] % n) * (2.0 * math.pi / n)
    real, imag = np.cos(theta) / math.sqrt(n), -np.sin(theta) / math.sqrt(n)
    forward = np.block([[real, imag], [-imag, real]])
    return np.stack([*halves(forward), *halves(forward.T)])


def ramp_constant(length, tile):
    differ = (length - tile) + np.arange(tile)[None, :] - np.arange(2 * length - tile)[:, None]
    squared = np.maximum(differ.astype(np.float64) ** 2, 1.0)
    odd = np.where(differ % 2 != 0, -1.0 / (math.pi * math.pi * squared), 0.0)
    return np.stack(halves(np.where(differ == 0, 0.25, odd)))


def split(value):
    high = value.astype(BF16)
    return high, (value - high.astype(F32)).astype(BF16)


def dot(left, right):
    return jnp.dot(left, right, preferred_element_type=F32)


def product(left, right):
    return dot(left[0], right[0]) + (dot(left[1], right[0]) + dot(left[0], right[1]))


def make_kernel(angles, positions, patch, band, per_device, width, zwin):
    blocks = width // LANES
    half = patch // 2
    rows_each = band // angles
    share = patch // positions

    def kernel(
        off, amp_hbm, probe_hbm, obj_hbm, index_hbm, weight_hbm, dft_hbm, ramp_hbm,
        obj_out, probe_out, recon_out,
        off_up, off_down, amp, probe, field, index, weight, dft, ramp,
        send_down, send_up, halo_up, halo_down, grad, grad_up, grad_down, pad_up, pad_down,
        power, inverse, spread, fresh, sino, filt, slope, recon,
        part, parts, merged, merges, new_probe,
        load_sem, field_sem, store_sem, off_send, off_recv,
        halo_send, halo_recv, grad_send, grad_recv,
        swap_send, swap_recv, part_send, part_recv, merge_send, merge_recv, share_send, share_recv,
    ):
        me_a = lax.axis_index("angle")
        me_p = lax.axis_index("pos")
        down = lax.rem(me_p + 1, positions)
        up = lax.rem(me_p + positions - 1, positions)

        def remote(src, dst, send, recv, angle, pos):
            return pltpu.make_async_remote_copy(
                src_ref=src, dst_ref=dst, send_sem=send, recv_sem=recv,
                device_id=(angle, pos), device_id_type=MESH,
            )

        field_loads = []
        for c in range(2):
            for b in range(blocks):
                field_loads.append(pltpu.make_async_copy(
                    obj_hbm.at[0, c, :, pl.ds(b * LANES, LANES)],
                    field.at[c, b, pl.ds(half, band), :], field_sem.at[c * blocks + b]))
        loads = [
            pltpu.make_async_copy(probe_hbm, probe, load_sem.at[0]),
            pltpu.make_async_copy(amp_hbm.at[0], amp, load_sem.at[1]),
            pltpu.make_async_copy(dft_hbm, dft, load_sem.at[2]),
            pltpu.make_async_copy(ramp_hbm, ramp, load_sem.at[3]),
            pltpu.make_async_copy(index_hbm, index, load_sem.at[4]),
            pltpu.make_async_copy(weight_hbm, weight, load_sem.at[5]),
        ]
        for copy in field_loads + loads:
            copy.start()

        barrier = pltpu.get_barrier_semaphore()
        for d in range(1, positions):
            pl.semaphore_signal(barrier, inc=1, device_id=(me_a, lax.rem(me_p + d, positions)), device_id_type=MESH)
        for d in range(1, angles):
            pl.semaphore_signal(barrier, inc=1, device_id=(lax.rem(me_a + d, angles), me_p), device_id_type=MESH)
        pl.semaphore_wait(barrier, positions + angles - 2)

        off_copies = [
            remote(off, off_up, off_send.at[0], off_recv.at[0], me_a, down),
            remote(off, off_down, off_send.at[1], off_recv.at[1], me_a, up),
        ]
        for copy in off_copies:
            copy.start()

        lane = lax.broadcasted_iota(jnp.int32, (half, LANES), 1)
        row = lax.broadcasted_iota(jnp.int32, (half, LANES), 0)

        loads[0].wait()
        pr = probe[0]
        pi = probe[1]
        power[pl.ds(0, half), :] = jnp.zeros((half, LANES), F32)
        power[pl.ds(half, patch), :] = pr * pr + pi * pi
        power[pl.ds(half + patch, half), :] = jnp.zeros((half, LANES), F32)
        for c in range(2):
            pad_up[c, pl.ds(half, half), :] = jnp.zeros((half, LANES), F32)
            pad_down[c, pl.ds(0, half), :] = jnp.zeros((half, LANES), F32)
        part[...] = jnp.zeros(part.shape, F32)
        for copy in field_loads:
            copy.wait()

        def place(table, owner, p):
            first = table[0, 0, p] - (owner * band - half)
            return jnp.minimum(jnp.maximum(first, 0), band), jnp.minimum(jnp.maximum(table[0, 1, p], 0), width - patch)

        def window(c, first, count, column):
            block = column >> 7
            shift = column & (LANES - 1)
            back = (LANES - shift) & (LANES - 1)
            left = pltpu.roll(field[c, block, pl.ds(first, count), :], back, 1)
            right = pltpu.roll(field[c, block + 1, pl.ds(first, count), :], back, 1)
            if count == half:
                return jnp.where(lane < LANES - shift, left, right)
            wide = lax.broadcasted_iota(jnp.int32, (count, LANES), 1)
            return jnp.where(wide < LANES - shift, left, right)

        for copy in off_copies:
            copy.wait()

        def halo_copy(p, which):
            if which == 0:
                return remote(send_down.at[p], halo_up.at[p], halo_send.at[0, p], halo_recv.at[0, p], me_a, down)
            return remote(send_up.at[p], halo_down.at[p], halo_send.at[1, p], halo_recv.at[1, p], me_a, up)

        def send_halo(p, _):
            r, column = place(off_down, down, p)
            for c in range(2):
                send_down[p, c] = window(c, half + r, half, column)
            halo_copy(p, 0).start()
            r, column = place(off_up, up, p)
            for c in range(2):
                send_up[p, c] = window(c, r, half, column)
            halo_copy(p, 1).start()
            return 0

        lax.fori_loop(0, per_device, send_halo, 0)

        tables = ((off, me_p, 2 * half), (off_up, up, 3 * half), (off_down, down, half))

        def spread_power(p, _):
            for k, (table, owner, base) in enumerate(tables):
                r, column = place(table, owner, p)
                spread[k * per_device + p, 0] = pltpu.roll(
                    power[pl.ds(base - r, half), :], column & (LANES - 1), 1)
            return 0

        lax.fori_loop(0, per_device, spread_power, 0)

        def covers(b, k, p):
            table, _, _ = tables[k]
            away = lane + (b * LANES - table[0, 1, p])
            return (away >= 0) & (away < LANES)

        def weigh(b, _):
            total = jnp.ones((half, LANES), F32)
            for k in range(3):
                for p in range(per_device):
                    total += jnp.where(covers(b, k, p), spread[k * per_device + p, 0], 0.0)
            inverse[b] = 1.0 / total
            return 0

        lax.fori_loop(0, blocks, weigh, 0)

        loads[1].wait()
        loads[2].wait()

        def grad_copy(p, which):
            if which == 0:
                return remote(grad.at[p, :, pl.ds(half, half), :], grad_up.at[p],
                              grad_send.at[0, p], grad_recv.at[0, p], me_a, down)
            return remote(grad.at[p, :, pl.ds(0, half), :], grad_down.at[p],
                          grad_send.at[1, p], grad_recv.at[1, p], me_a, up)

        def one_patch(p, _):
            r, column = place(off, me_p, p)
            own = [window(c, r, patch, column) for c in range(2)]
            halo_copy(p, 0).wait_recv()
            halo_copy(p, 1).wait_recv()
            low = row < half - r
            q = [
                jnp.concatenate([
                    jnp.where(low, halo_up[p, c], own[c][:half]),
                    jnp.where(low, own[c][half:], halo_down[p, c])], axis=0)
                for c in range(2)
            ]
            qr, qi = q
            pr = probe[0]
            pi = probe[1]
            wr = pr * qr - pi * qi
            wi = pr * qi + pi * qr
            forward = (dft[0], dft[1])
            backward = (dft[2], dft[3])
            mid = product(split(jnp.concatenate([wr, wi], axis=1)), forward)
            spec = product(backward, split(jnp.concatenate([mid[:, :patch], mid[:, patch:]], axis=0)))
            sr, si = spec[:patch], spec[patch:]
            factor = amp[p] / jnp.maximum(jnp.sqrt(sr * sr + si * si), 0.5)
            mid = product(split(jnp.concatenate([factor * sr, factor * si], axis=1)), backward)
            wave = product(forward, split(jnp.concatenate([mid[:, :patch], mid[:, patch:]], axis=0)))
            dr = wave[:patch] - wr
            di = wave[patch:] - wi
            grad[p, 0] = pr * dr + pi * di
            grad[p, 1] = pr * di - pi * dr
            grad_copy(p, 0).start()
            grad_copy(p, 1).start()
            part[0] += qr * dr + qi * di
            part[1] += qr * di - qi * dr
            part[2] += qr * qr + qi * qi
            return 0

        lax.fori_loop(0, per_device, one_patch, 0)

        def part_copy(d):
            to = lax.rem(me_p + d, positions)
            return remote(part.at[:, pl.ds(pl.multiple_of(to * share, share), share), :], parts.at[d],
                          part_send.at[d], part_recv.at[d], me_a, to)

        for d in range(1, positions):
            part_copy(d).start()

        def spread_grad(k, p, source):
            table, owner, _ = tables[k]
            r, column = place(table, owner, p)
            for c in range(2):
                spread[k * per_device + p, c] = pltpu.roll(
                    source(c)[pl.ds(half - r, half), :], column & (LANES - 1), 1)

        def spread_own(p, _):
            spread_grad(0, p, lambda c: grad.at[p, c])
            return 0

        lax.fori_loop(0, per_device, spread_own, 0)

        def spread_near(p, _):
            grad_copy(p, 0).wait_recv()
            for c in range(2):
                pad_up[c, pl.ds(0, half), :] = grad_up[p, c]
            spread_grad(1, p, lambda c: pad_up.at[c])
            grad_copy(p, 1).wait_recv()
            for c in range(2):
                pad_down[c, pl.ds(half, half), :] = grad_down[p, c]
            spread_grad(2, p, lambda c: pad_down.at[c])
            return 0

        lax.fori_loop(0, per_device, spread_near, 0)

        def update(b, _):
            total = [jnp.zeros((half, LANES), F32) for _ in range(2)]
            for k in range(3):
                for p in range(per_device):
                    inside = covers(b, k, p)
                    for c in range(2):
                        total[c] += jnp.where(inside, spread[k * per_device + p, c], 0.0)
            at = pl.ds(pl.multiple_of(b * LANES, LANES), LANES)
            for c in range(2):
                fresh[c, :, at] = field[c, b, pl.ds(half, band), :] + total[c] * inverse[b]
            return 0

        lax.fori_loop(0, blocks, update, 0)

        def swap_copy(d):
            to = lax.rem(me_a + d, angles)
            return remote(
                fresh.at[1, pl.ds(pl.multiple_of(to * rows_each, rows_each), rows_each), :],
                sino.at[pl.ds(pl.multiple_of(me_a * rows_each, rows_each), rows_each), :],
                swap_send.at[d], swap_recv.at[d], to, me_p)

        for d in range(1, angles):
            swap_copy(d).start()
        mine = pl.ds(pl.multiple_of(me_a * rows_each, rows_each), rows_each)
        sino[mine, :] = fresh[1, mine, :]
        stores = [pltpu.make_async_copy(fresh, obj_out.at[0], store_sem.at[0])]
        stores[0].start()

        for d in range(1, positions):
            part_copy(d).wait_recv()
        own_share = pl.ds(pl.multiple_of(me_p * share, share), share)
        total = part[:, own_share, :]
        for d in range(1, positions):
            total += parts[d]
        merged[...] = total

        def merge_copy(d):
            to = lax.rem(me_a + d, angles)
            return remote(merged, merges.at[me_a], merge_send.at[d], merge_recv.at[d], to, me_p)

        for d in range(1, angles):
            merge_copy(d).start()
        merges[me_a] = merged[...]

        for d in range(1, angles):
            swap_copy(d).wait_recv()
        loads[3].wait()
        high, low = split(sino[...])
        both = jnp.concatenate([high, low], axis=0)
        tile = ramp.shape[2]
        for j in range(width // tile):
            rows = pl.ds(width - tile - j * tile, width)
            twice = dot(both, ramp[0, rows, :])
            filt[:, pl.ds(j * tile, tile)] = twice[:band] + (twice[band:] + dot(high, ramp[1, rows, :]))

        for d in range(1, angles):
            merge_copy(d).wait_recv()
        total = merges[0]
        for a in range(1, angles):
            total += merges[a]
        bottom = total[2] + 1.0
        for c in range(2):
            new_probe[c, own_share, :] = probe[c, own_share, :] + total[c] / bottom

        def share_copy(d):
            to = lax.rem(me_p + d, positions)
            return remote(new_probe.at[:, own_share, :], new_probe.at[:, own_share, :],
                          share_send.at[d], share_recv.at[d], me_a, to)

        for d in range(1, positions):
            share_copy(d).start()

        loads[4].wait()
        loads[5].wait()
        slope[...] = pltpu.roll(filt[...], width - 1, 1) - filt[...]

        def back(b, _):
            at = pl.ds(pl.multiple_of(b * LANES, LANES), LANES)
            for z in range(zwin):
                total = jnp.zeros((rows_each, LANES), F32)
                for a in range(angles):
                    k = jnp.broadcast_to(index[a, pl.ds(z, 1), at], (rows_each, LANES))
                    w = jnp.broadcast_to(weight[a, pl.ds(z, 1), at], (rows_each, LANES))
                    where = k >> 7
                    inside = k & (LANES - 1)
                    rows = pl.ds(a * rows_each, rows_each)
                    lower = jnp.zeros((rows_each, LANES), F32)
                    rise = jnp.zeros((rows_each, LANES), F32)
                    for s in range(blocks):
                        source = pl.ds(s * LANES, LANES)
                        here = where == s
                        lower = jnp.where(here, jnp.take_along_axis(filt[rows, source], inside, axis=1), lower)
                        rise = jnp.where(here, jnp.take_along_axis(slope[rows, source], inside, axis=1), rise)
                    total += lower + w * rise
                recon[z, :, at] = total * (math.pi / angles)
            return 0

        lax.fori_loop(0, blocks, back, 0)
        for z in range(zwin):
            stores.append(pltpu.make_async_copy(recon.at[z], recon_out.at[0, :, z, :], store_sem.at[1 + z]))
            stores[-1].start()

        for d in range(1, positions):
            share_copy(d).wait_recv()
        stores.append(pltpu.make_async_copy(new_probe, probe_out, store_sem.at[1 + zwin]))
        stores[-1].start()

        for p in range(per_device):
            for which in range(2):
                halo_copy(p, which).wait_send()
                grad_copy(p, which).wait_send()
        for d in range(1, positions):
            part_copy(d).wait_send()
            share_copy(d).wait_send()
        for d in range(1, angles):
            swap_copy(d).wait_send()
            merge_copy(d).wait_send()
        for copy in stores:
            copy.wait()

    def scratch():
        vm = pltpu.VMEM
        dma = pltpu.SemaphoreType.DMA
        slab = (per_device, 2, half, LANES)
        tile = 256
        return [
            pltpu.SMEM((1, 2, per_device), jnp.int32),
            pltpu.SMEM((1, 2, per_device), jnp.int32),
            vm((per_device, patch, patch), F32),
            vm((2, patch, patch), F32),
            vm((2, blocks + 1, band + patch, LANES), F32),
            vm((angles, zwin, width), jnp.int32),
            vm((angles, zwin, width), F32),
            vm((4, 2 * patch, 2 * patch), BF16),
            vm((2, 2 * width - tile, tile), BF16),
            vm(slab, F32),
            vm(slab, F32),
            vm(slab, F32),
            vm(slab, F32),
            vm((per_device, 2, patch, LANES), F32),
            vm(slab, F32),
            vm(slab, F32),
            vm((2, patch, LANES), F32),
            vm((2, patch, LANES), F32),
            vm((2 * patch, LANES), F32),
            vm((blocks, band, LANES), F32),
            vm((3 * per_device, 2, half, LANES), F32),
            vm((2, band, width), F32),
            vm((band, width), F32),
            vm((band, width), F32),
            vm((band, width), F32),
            vm((zwin, rows_each, width), F32),
            vm((3, patch, LANES), F32),
            vm((positions, 3, share, LANES), F32),
            vm((3, share, LANES), F32),
            vm((angles, 3, share, LANES), F32),
            vm((2, patch, LANES), F32),
            dma((6,)),
            dma((2 * blocks,)),
            dma((2 + zwin,)),
            dma((2,)), dma((2,)),
            dma((2, per_device)), dma((2, per_device)),
            dma((2, per_device)), dma((2, per_device)),
            dma((angles,)), dma((angles,)),
            dma((positions,)), dma((positions,)),
            dma((angles,)), dma((angles,)),
            dma((positions,)), dma((positions,)),
        ]

    return kernel, scratch


def solution(mesh):
    angles, positions = mesh.shape["angle"], mesh.shape["pos"]

    def on_device(amplitude, offsets, probe_field, object_field, interp_index, interp_weight):
        band, width = object_field.shape[2:]
        patch = probe_field.shape[1]
        zwin = interp_index.shape[1]
        kernel, scratch = make_kernel(angles, positions, patch, band, offsets.shape[1], width, zwin)
        anywhere = pl.BlockSpec(memory_space=pl.ANY)
        return pl.pallas_call(
            kernel,
            name="ptycho",
            out_shape=(
                jax.ShapeDtypeStruct(object_field.shape, F32),
                jax.ShapeDtypeStruct(probe_field.shape, F32),
                jax.ShapeDtypeStruct((1, band // angles, zwin, width), F32),
            ),
            in_specs=[pl.BlockSpec(memory_space=pltpu.SMEM)] + [anywhere] * 7,
            out_specs=(anywhere,) * 3,
            scratch_shapes=scratch(),
            compiler_params=pltpu.CompilerParams(
                collective_id=0, has_side_effects=True, vmem_limit_bytes=60 * 1024 * 1024
            ),
        )(
            jnp.swapaxes(offsets, 1, 2), amplitude, probe_field, object_field, interp_index, interp_weight,
            jnp.asarray(dft_constant(patch)), jnp.asarray(ramp_constant(width, 256)),
        )

    return jax.shard_map(
        on_device,
        mesh=mesh,
        in_specs=(
            P("angle", "pos", None, None),
            P("angle", "pos", None),
            P(),
            P("angle", None, "pos", None),
            P(),
            P(),
        ),
        out_specs=(P("angle", None, "pos", None), P(), P("pos", "angle", None, None)),
        check_vma=False,
    )
```

```python
import math

import jax
import jax.numpy as jnp
import ml_dtypes
import numpy as np
from jax import lax
from jax.experimental import pallas as pl
from jax.experimental.pallas import tpu as pltpu
from jax.sharding import PartitionSpec as P

MESH = pl.DeviceIdType.MESH
F32 = jnp.float32
BF16 = jnp.bfloat16
LANES = 128


def halves(table):
    high = table.astype(np.float32).astype(ml_dtypes.bfloat16)
    low = (table.astype(np.float32) - high.astype(np.float32)).astype(ml_dtypes.bfloat16)
    return high, low


def dft_constant(n):
    ramp = np.arange(n)
    theta = (ramp[:, None] * ramp[None, :] % n) * (2.0 * math.pi / n)
    real, imag = np.cos(theta) / math.sqrt(n), -np.sin(theta) / math.sqrt(n)
    forward = np.block([[real, imag], [-imag, real]])
    return np.stack([*halves(forward), *halves(forward.T)])


def ramp_constant(length, tile):
    differ = (length - tile) + np.arange(tile)[None, :] - np.arange(2 * length - tile)[:, None]
    squared = np.maximum(differ.astype(np.float64) ** 2, 1.0)
    odd = np.where(differ % 2 != 0, -1.0 / (math.pi * math.pi * squared), 0.0)
    return np.stack(halves(np.where(differ == 0, 0.25, odd)))


def split(value):
    high = value.astype(BF16)
    return high, (value - high.astype(F32)).astype(BF16)


def dot(left, right):
    return jnp.dot(left, right, preferred_element_type=F32)


def product(left, right):
    return dot(left[0], right[0]) + (dot(left[1], right[0]) + dot(left[0], right[1]))


def pick(values, lanes):
    return jnp.take_along_axis(values, lanes, axis=1, mode="promise_in_bounds")


def put_out(obj, probe, recon, obj_out, probe_out, recon_out, sems):
    copies = [
        pltpu.make_async_copy(obj, obj_out, sems.at[0]),
        pltpu.make_async_copy(probe, probe_out, sems.at[1]),
    ]
    for depth in range(recon.shape[0]):
        copies.append(pltpu.make_async_copy(recon.at[depth], recon_out.at[0, :, depth, :], sems.at[2 + depth]))
    for copy in copies:
        copy.start()
    for copy in copies:
        copy.wait()


def make_kernel(angles, positions, patch, band, per_device, width, zwin):
    blocks = width // LANES
    half = patch // 2
    rows_each = band // angles
    share = patch // positions

    def kernel(
        off_hbm, amp_hbm, probe_hbm, obj_hbm, index_hbm, weight_hbm, dft_hbm, ramp_hbm,
        fresh, probe_out, recon,
        off, off_up, off_down, amp, probe, field, index, weight, dft, ramp,
        send_down, send_up, halo_up, halo_down, grad, grad_up, grad_down, pad_up, pad_down,
        power, inverse, spread, filt, sino, total_recon,
        part, parts, merged, merges, new_probe,
        load_sem, field_sem, off_send, off_recv,
        halo_send, halo_recv, grad_send, grad_recv,
        swap_send, swap_recv, part_send, part_recv, merge_send, merge_recv, share_send, share_recv,
    ):
        me_a = lax.axis_index("angle")
        me_p = lax.axis_index("pos")
        down = lax.rem(me_p + 1, positions)
        up = lax.rem(me_p + positions - 1, positions)

        def remote(src, dst, send, recv, peer):
            return pltpu.make_async_remote_copy(
                src_ref=src, dst_ref=dst, send_sem=send, recv_sem=recv,
                device_id=peer, device_id_type=MESH,
            )

        field_loads = []
        for c in range(2):
            for b in range(blocks):
                field_loads.append(pltpu.make_async_copy(
                    obj_hbm.at[0, c, :, pl.ds(b * LANES, LANES)],
                    field.at[c, b, pl.ds(half, band), :], field_sem.at[c * blocks + b]))
        loads = [
            pltpu.make_async_copy(probe_hbm, probe, load_sem.at[0]),
            pltpu.make_async_copy(amp_hbm.at[0], amp, load_sem.at[1]),
            pltpu.make_async_copy(dft_hbm, dft, load_sem.at[2]),
            pltpu.make_async_copy(ramp_hbm, ramp, load_sem.at[3]),
            pltpu.make_async_copy(index_hbm, index, load_sem.at[4]),
            pltpu.make_async_copy(weight_hbm, weight, load_sem.at[5]),
        ]
        off_load = pltpu.make_async_copy(off_hbm, off, load_sem.at[6])
        for copy in [off_load] + field_loads + loads:
            copy.start()

        z, far = me_a >> 1, me_a & 1
        y, side = me_p >> 2, me_p & 3

        def plane_peer(d):
            return (((z + (d >> 2)) & 3) * 2 + far, ((y + (d & 3)) & 3) * 4 + side)

        def line_peer(d):
            return (z * 2 + (far ^ (d >> 2)), y * 4 + (side ^ (d & 3)))

        def angle_peer(d):
            return (((z + (d & 3)) & 3) * 2 + (far ^ (d >> 2)), me_p)

        def angle_source(d):
            return ((z - (d & 3)) & 3) * 2 + (far ^ (d >> 2))

        barrier = pltpu.get_barrier_semaphore()
        greeted = [(me_a, up), (me_a, down)]
        greeted += [line_peer(d) for d in range(1, 8)]
        greeted += [plane_peer(d) for d in range(1, 16)]
        greeted += [angle_peer(d) for d in range(5, 8)]
        for peer in greeted:
            pl.semaphore_signal(barrier, inc=1, device_id=peer, device_id_type=MESH)
        pl.semaphore_wait(barrier, len(greeted))

        off_copies = [
            remote(off, off_up, off_send.at[0], off_recv.at[0], (me_a, down)),
            remote(off, off_down, off_send.at[1], off_recv.at[1], (me_a, up)),
        ]
        off_load.wait()
        for copy in off_copies:
            copy.start()

        lane = lax.broadcasted_iota(jnp.int32, (half, LANES), 1)
        row = lax.broadcasted_iota(jnp.int32, (half, LANES), 0)

        loads[0].wait()
        pr = probe[0]
        pi = probe[1]
        power[pl.ds(0, half), :] = jnp.zeros((half, LANES), F32)
        power[pl.ds(half, patch), :] = pr * pr + pi * pi
        power[pl.ds(half + patch, half), :] = jnp.zeros((half, LANES), F32)
        for c in range(2):
            pad_up[c, pl.ds(half, half), :] = jnp.zeros((half, LANES), F32)
            pad_down[c, pl.ds(0, half), :] = jnp.zeros((half, LANES), F32)
        part[...] = jnp.zeros(part.shape, F32)
        for copy in field_loads:
            copy.wait()

        def place(table, owner, p):
            first = table[0, 0, p] - (owner * band - half)
            return jnp.minimum(jnp.maximum(first, 0), band), jnp.minimum(jnp.maximum(table[0, 1, p], 0), width - patch)

        def window(c, first, count, column):
            block = column >> 7
            shift = column & (LANES - 1)
            back = (LANES - shift) & (LANES - 1)
            left = pltpu.roll(field[c, block, pl.ds(first, count), :], back, 1)
            right = pltpu.roll(field[c, block + 1, pl.ds(first, count), :], back, 1)
            if count == half:
                return jnp.where(lane < LANES - shift, left, right)
            wide = lax.broadcasted_iota(jnp.int32, (count, LANES), 1)
            return jnp.where(wide < LANES - shift, left, right)

        for copy in off_copies:
            copy.wait()

        def halo_copy(p, which):
            if which == 0:
                return remote(send_down.at[p], halo_up.at[p], halo_send.at[0, p], halo_recv.at[0, p], (me_a, down))
            return remote(send_up.at[p], halo_down.at[p], halo_send.at[1, p], halo_recv.at[1, p], (me_a, up))

        def send_halo(p, _):
            r, column = place(off_down, down, p)
            for c in range(2):
                send_down[p, c] = window(c, half + r, half, column)
            halo_copy(p, 0).start()
            r, column = place(off_up, up, p)
            for c in range(2):
                send_up[p, c] = window(c, r, half, column)
            halo_copy(p, 1).start()
            return 0

        lax.fori_loop(0, per_device, send_halo, 0)

        tables = ((off, me_p, 2 * half), (off_up, up, 3 * half), (off_down, down, half))

        def spread_power(p, _):
            for k, (table, owner, base) in enumerate(tables):
                r, column = place(table, owner, p)
                spread[k * per_device + p, 0] = pltpu.roll(
                    power[pl.ds(base - r, half), :], column & (LANES - 1), 1)
            return 0

        lax.fori_loop(0, per_device, spread_power, 0)

        def covers(b, k, p):
            table, _, _ = tables[k]
            away = lane + (b * LANES - table[0, 1, p])
            return (away >= 0) & (away < LANES)

        def weigh(b, _):
            total = jnp.ones((half, LANES), F32)
            for k in range(3):
                for p in range(per_device):
                    total += jnp.where(covers(b, k, p), spread[k * per_device + p, 0], 0.0)
            inverse[b] = 1.0 / total
            return 0

        lax.fori_loop(0, blocks, weigh, 0)

        loads[1].wait()
        loads[2].wait()

        def grad_copy(p, which):
            if which == 0:
                return remote(grad.at[p, :, pl.ds(half, half), :], grad_up.at[p],
                              grad_send.at[0, p], grad_recv.at[0, p], (me_a, down))
            return remote(grad.at[p, :, pl.ds(0, half), :], grad_down.at[p],
                          grad_send.at[1, p], grad_recv.at[1, p], (me_a, up))

        def one_patch(p, _):
            r, column = place(off, me_p, p)
            own = [window(c, r, patch, column) for c in range(2)]
            halo_copy(p, 0).wait_recv()
            halo_copy(p, 1).wait_recv()
            low = row < half - r
            q = [
                jnp.concatenate([
                    jnp.where(low, halo_up[p, c], own[c][:half]),
                    jnp.where(low, own[c][half:], halo_down[p, c])], axis=0)
                for c in range(2)
            ]
            qr, qi = q
            pr = probe[0]
            pi = probe[1]
            wr = pr * qr - pi * qi
            wi = pr * qi + pi * qr
            forward = (dft[0], dft[1])
            backward = (dft[2], dft[3])
            mid = product(split(jnp.concatenate([wr, wi], axis=1)), forward)
            spec = product(backward, split(jnp.concatenate([mid[:, :patch], mid[:, patch:]], axis=0)))
            sr, si = spec[:patch], spec[patch:]
            factor = amp[p] / jnp.maximum(jnp.sqrt(sr * sr + si * si), 0.5)
            mid = product(split(jnp.concatenate([factor * sr, factor * si], axis=1)), backward)
            wave = product(forward, split(jnp.concatenate([mid[:, :patch], mid[:, patch:]], axis=0)))
            dr = wave[:patch] - wr
            di = wave[patch:] - wi
            grad[p, 0] = pr * dr + pi * di
            grad[p, 1] = pr * di - pi * dr
            grad_copy(p, 0).start()
            grad_copy(p, 1).start()
            part[0] += qr * dr + qi * di
            part[1] += qr * di - qi * dr
            part[2] += qr * qr + qi * qi
            return 0

        lax.fori_loop(0, per_device, one_patch, 0)

        lot = z * 4 + y

        def part_copy(d):
            theirs = ((z + (d >> 2)) & 3) * 4 + ((y + (d & 3)) & 3)
            return remote(part.at[:, pl.ds(pl.multiple_of(theirs * share, share), share), :], parts.at[d],
                          part_send.at[d], part_recv.at[d], plane_peer(d))

        for d in range(1, positions):
            part_copy(d).start()

        def spread_grad(k, p, source):
            table, owner, _ = tables[k]
            r, column = place(table, owner, p)
            for c in range(2):
                spread[k * per_device + p, c] = pltpu.roll(
                    source(c)[pl.ds(half - r, half), :], column & (LANES - 1), 1)

        def spread_own(p, _):
            spread_grad(0, p, lambda c: grad.at[p, c])
            return 0

        lax.fori_loop(0, per_device, spread_own, 0)

        def spread_near(p, _):
            grad_copy(p, 0).wait_recv()
            for c in range(2):
                pad_up[c, pl.ds(0, half), :] = grad_up[p, c]
            spread_grad(1, p, lambda c: pad_up.at[c])
            grad_copy(p, 1).wait_recv()
            for c in range(2):
                pad_down[c, pl.ds(half, half), :] = grad_down[p, c]
            spread_grad(2, p, lambda c: pad_down.at[c])
            return 0

        lax.fori_loop(0, per_device, spread_near, 0)

        def update(b, _):
            total = [jnp.zeros((half, LANES), F32) for _ in range(2)]
            for k in range(3):
                for p in range(per_device):
                    inside = covers(b, k, p)
                    for c in range(2):
                        total[c] += jnp.where(inside, spread[k * per_device + p, c], 0.0)
            at = pl.ds(pl.multiple_of(b * LANES, LANES), LANES)
            for c in range(2):
                fresh[0, c, :, at] = field[c, b, pl.ds(half, band), :] + total[c] * inverse[b]
            return 0

        lax.fori_loop(0, blocks, update, 0)

        loads[3].wait()
        high, low = split(fresh[0, 1])
        both = jnp.concatenate([high, low], axis=0)
        tile = ramp.shape[2]
        for j in range(width // tile):
            rows = pl.ds(width - tile - j * tile, width)
            twice = dot(both, ramp[0, rows, :])
            piece = twice[:band] + (twice[band:] + dot(high, ramp[1, rows, :]))
            for a in range(angles):
                filt[a, :, pl.ds(j * tile, tile)] = piece[a * rows_each:(a + 1) * rows_each]

        def swap_copy(d):
            peer = angle_peer(d)
            return remote(filt.at[peer[0]], sino.at[d], swap_send.at[d], swap_recv.at[d], peer)

        for d in (4, 5, 7, 6, 1, 3, 2):
            swap_copy(d).start()
        sino[0] = filt[me_a]

        for d in range(1, positions):
            part_copy(d).wait_recv()
        own_share = pl.ds(pl.multiple_of(lot * share, share), share)
        total = part[:, own_share, :]
        for d in range(1, positions):
            total += parts[d]
        merged[...] = total
        place_in_line = far * 4 + side

        def merge_copy(d):
            return remote(merged, merges.at[place_in_line], merge_send.at[d], merge_recv.at[d], line_peer(d))

        for d in range(1, angles):
            merge_copy(d).start()
        merges[place_in_line] = merged[...]

        loads[4].wait()
        loads[5].wait()
        total_recon[...] = jnp.zeros(total_recon.shape, F32)

        def back(d, _):
            @pl.when(d > 0)
            def _():
                swap_copy(d).wait_recv()

            a = angle_source(d)
            rows = sino[d]
            rise = pltpu.roll(rows, width - 1, 1) - rows
            for depth in range(zwin):
                for b in range(blocks):
                    at = pl.ds(b * LANES, LANES)
                    k = jnp.broadcast_to(index[a, pl.ds(depth, 1), at], (rows_each, LANES))
                    w = jnp.broadcast_to(weight[a, pl.ds(depth, 1), at], (rows_each, LANES))
                    block = k >> 7
                    inside = k & (LANES - 1)
                    lower = jnp.zeros((rows_each, LANES), F32)
                    slope = jnp.zeros((rows_each, LANES), F32)
                    for s in range(blocks):
                        here = block == s
                        cut = slice(s * LANES, (s + 1) * LANES)
                        lower = jnp.where(here, pick(rows[:, cut], inside), lower)
                        slope = jnp.where(here, pick(rise[:, cut], inside), slope)
                    total_recon[depth, :, at] += lower + w * slope
            return 0

        lax.fori_loop(0, 4, back, 0)

        for d in range(1, angles):
            merge_copy(d).wait_recv()
        total = merges[0]
        for a in range(1, angles):
            total += merges[a]
        bottom = total[2] + 1.0
        for c in range(2):
            new_probe[c, own_share, :] = probe[c, own_share, :] + total[c] / bottom

        def share_copy(d):
            return remote(new_probe.at[:, own_share, :], new_probe.at[:, own_share, :],
                          share_send.at[d], share_recv.at[d], plane_peer(d))

        for d in range(1, positions):
            share_copy(d).start()
        for p in range(per_device):
            for which in range(2):
                halo_copy(p, which).wait_send()
                grad_copy(p, which).wait_send()
        for d in range(1, positions):
            part_copy(d).wait_send()

        lax.fori_loop(4, angles, back, 0)
        for depth in range(zwin):
            recon[depth] = total_recon[depth] * (math.pi / angles)

        for d in range(1, angles):
            swap_copy(d).wait_send()
            merge_copy(d).wait_send()
        for d in range(1, positions):
            share_copy(d).wait_recv()
        probe_out[...] = new_probe[...]
        for d in range(1, positions):
            share_copy(d).wait_send()

    def scratch():
        vm = pltpu.VMEM
        dma = pltpu.SemaphoreType.DMA
        slab = (per_device, 2, half, LANES)
        tile = 256
        return [
            pltpu.SMEM((1, 2, per_device), jnp.int32),
            pltpu.SMEM((1, 2, per_device), jnp.int32),
            pltpu.SMEM((1, 2, per_device), jnp.int32),
            vm((per_device, patch, patch), F32),
            vm((2, patch, patch), F32),
            vm((2, blocks + 1, band + patch, LANES), F32),
            vm((angles, zwin, width), jnp.int32),
            vm((angles, zwin, width), F32),
            vm((4, 2 * patch, 2 * patch), BF16),
            vm((2, 2 * width - tile, tile), BF16),
            vm(slab, F32),
            vm(slab, F32),
            vm(slab, F32),
            vm(slab, F32),
            vm((per_device, 2, patch, LANES), F32),
            vm(slab, F32),
            vm(slab, F32),
            vm((2, patch, LANES), F32),
            vm((2, patch, LANES), F32),
            vm((2 * patch, LANES), F32),
            vm((blocks, band, LANES), F32),
            vm((3 * per_device, 2, half, LANES), F32),
            vm((angles, rows_each, width), F32),
            vm((angles, rows_each, width), F32),
            vm((zwin, rows_each, width), F32),
            vm((3, patch, LANES), F32),
            vm((positions, 3, share, LANES), F32),
            vm((3, share, LANES), F32),
            vm((angles, 3, share, LANES), F32),
            vm((2, patch, LANES), F32),
            dma((7,)),
            dma((2 * blocks,)),
            dma((2,)), dma((2,)),
            dma((2, per_device)), dma((2, per_device)),
            dma((2, per_device)), dma((2, per_device)),
            dma((angles,)), dma((angles,)),
            dma((positions,)), dma((positions,)),
            dma((angles,)), dma((angles,)),
            dma((positions,)), dma((positions,)),
        ]

    return kernel, scratch


def solution(mesh):
    angles, positions = mesh.shape["angle"], mesh.shape["pos"]

    def on_device(amplitude, offsets, probe_field, object_field, interp_index, interp_weight):
        band, width = object_field.shape[2:]
        patch = probe_field.shape[1]
        zwin = interp_index.shape[1]
        kernel, scratch = make_kernel(angles, positions, patch, band, offsets.shape[1], width, zwin)
        anywhere = pl.BlockSpec(memory_space=pl.ANY)
        in_hbm = pl.BlockSpec(memory_space=pltpu.HBM)
        in_vmem = pl.BlockSpec(memory_space=pltpu.VMEM)
        rows_each = band // angles
        ready = pl.pallas_call(
            kernel,
            name="ptycho",
            out_shape=(
                jax.ShapeDtypeStruct(object_field.shape, F32),
                jax.ShapeDtypeStruct(probe_field.shape, F32),
                jax.ShapeDtypeStruct((zwin, rows_each, width), F32),
            ),
            in_specs=[in_hbm] * 8,
            out_specs=(in_vmem,) * 3,
            scratch_shapes=scratch(),
            compiler_params=pltpu.CompilerParams(
                collective_id=0, has_side_effects=True, vmem_limit_bytes=32 * 1024 * 1024
            ),
        )(
            *(
                pltpu.with_memory_space_constraint(x, pltpu.HBM)
                for x in (
                    jnp.swapaxes(offsets, 1, 2), amplitude, probe_field, object_field, interp_index, interp_weight,
                    jnp.asarray(dft_constant(patch)), jnp.asarray(ramp_constant(width, 256)),
                )
            ),
        )
        return pl.pallas_call(
            put_out,
            name="put_out",
            out_shape=(
                jax.ShapeDtypeStruct(object_field.shape, F32),
                jax.ShapeDtypeStruct(probe_field.shape, F32),
                jax.ShapeDtypeStruct((1, rows_each, zwin, width), F32),
            ),
            in_specs=[in_vmem] * 3,
            out_specs=(anywhere,) * 3,
            scratch_shapes=[pltpu.SemaphoreType.DMA((2 + zwin,))],
            compiler_params=pltpu.CompilerParams(vmem_limit_bytes=4 * 1024 * 1024),
        )(*ready)

    return jax.shard_map(
        on_device,
        mesh=mesh,
        in_specs=(
            P("angle", "pos", None, None),
            P("angle", "pos", None),
            P(),
            P("angle", None, "pos", None),
            P(),
            P(),
        ),
        out_specs=(P("angle", None, "pos", None), P(), P("pos", "angle", None, None)),
        check_vma=False,
    )
```

```python
import math

import jax
import jax.numpy as jnp
import ml_dtypes
import numpy as np
from jax import lax
from jax.experimental import pallas as pl
from jax.experimental.pallas import tpu as pltpu
from jax.sharding import PartitionSpec as P

MESH = pl.DeviceIdType.MESH
F32 = jnp.float32
BF16 = jnp.bfloat16
LANES = 128
EARLY = 2


def halves(table):
    high = table.astype(np.float32).astype(ml_dtypes.bfloat16)
    low = (table.astype(np.float32) - high.astype(np.float32)).astype(ml_dtypes.bfloat16)
    return high, low


def dft_constant(n):
    ramp = np.arange(n)
    theta = (ramp[:, None] * ramp[None, :] % n) * (2.0 * math.pi / n)
    real, imag = np.cos(theta) / math.sqrt(n), -np.sin(theta) / math.sqrt(n)
    forward = np.block([[real, imag], [-imag, real]])
    return np.stack([*halves(forward), *halves(forward.T)])


def ramp_constant(length, tile):
    differ = (length - tile) + np.arange(tile)[None, :] - np.arange(2 * length - tile)[:, None]
    squared = np.maximum(differ.astype(np.float64) ** 2, 1.0)
    odd = np.where(differ % 2 != 0, -1.0 / (math.pi * math.pi * squared), 0.0)
    return np.stack(halves(np.where(differ == 0, 0.25, odd)))


def split(value):
    high = value.astype(BF16)
    return high, (value - high.astype(F32)).astype(BF16)


def dot(left, right):
    return jnp.dot(left, right, preferred_element_type=F32)


def product(left, right):
    return dot(left[0], right[0]) + (dot(left[1], right[0]) + dot(left[0], right[1]))


def pick(values, lanes):
    return jnp.take_along_axis(values, lanes, axis=1, mode="promise_in_bounds")


def put_out(obj, probe, recon, obj_out, probe_out, recon_out, sems):
    copies = [
        pltpu.make_async_copy(obj, obj_out, sems.at[0]),
        pltpu.make_async_copy(probe, probe_out, sems.at[1]),
    ]
    for depth in range(recon.shape[0]):
        copies.append(pltpu.make_async_copy(recon.at[depth], recon_out.at[0, :, depth, :], sems.at[2 + depth]))
    for copy in copies:
        copy.start()
    for copy in copies:
        copy.wait()


def make_kernel(angles, positions, patch, band, per_device, width, zwin):
    blocks = width // LANES
    half = patch // 2
    rows_each = band // angles
    share = patch // positions

    def kernel(
        off_hbm, amp_hbm, probe_hbm, obj_hbm, index_hbm, weight_hbm, dft_hbm, ramp_hbm,
        fresh, probe_out, recon,
        off, off_up, off_down, amp, probe, field, index, weight, dft, ramp,
        send_down, send_up, halo_up, halo_down, grad, grad_up, grad_down, pad_up, pad_down,
        power, inverse, spread, filt, sino, total_recon,
        part, parts, merges, new_probe,
        load_sem, field_sem, off_send, off_recv,
        halo_send, halo_recv, grad_send, grad_recv,
        swap_send, swap_recv, group_send, group_recv,
    ):
        me_a = lax.axis_index("angle")
        me_p = lax.axis_index("pos")
        down = lax.rem(me_p + 1, positions)
        up = lax.rem(me_p + positions - 1, positions)

        def remote(src, dst, send, recv, peer):
            return pltpu.make_async_remote_copy(
                src_ref=src, dst_ref=dst, send_sem=send, recv_sem=recv,
                device_id=peer, device_id_type=MESH,
            )

        field_loads = []
        for c in range(2):
            for b in range(blocks):
                field_loads.append(pltpu.make_async_copy(
                    obj_hbm.at[0, c, :, pl.ds(b * LANES, LANES)],
                    field.at[c, b, pl.ds(half, band), :], field_sem.at[c * blocks + b]))
        loads = [
            pltpu.make_async_copy(probe_hbm, probe, load_sem.at[0]),
            pltpu.make_async_copy(amp_hbm.at[0], amp, load_sem.at[1]),
            pltpu.make_async_copy(dft_hbm, dft, load_sem.at[2]),
            pltpu.make_async_copy(ramp_hbm, ramp, load_sem.at[3]),
            pltpu.make_async_copy(index_hbm, index, load_sem.at[4]),
            pltpu.make_async_copy(weight_hbm, weight, load_sem.at[5]),
        ]
        off_load = pltpu.make_async_copy(off_hbm, off, load_sem.at[6])
        for copy in [off_load] + field_loads + loads:
            copy.start()

        z, far = me_a >> 1, me_a & 1
        y, side = me_p >> 2, me_p & 3

        def plane_peer(d):
            return (((z + (d >> 2)) & 3) * 2 + far, ((y + (d & 3)) & 3) * 4 + side)

        def line_peer(d):
            return (z * 2 + (far ^ (d >> 2)), y * 4 + (side ^ (d & 3)))

        def angle_peer(d):
            return (((z + (d & 3)) & 3) * 2 + (far ^ (d >> 2)), me_p)

        def angle_source(d):
            return ((z - (d & 3)) & 3) * 2 + (far ^ (d >> 2))

        barrier = pltpu.get_barrier_semaphore()
        greeted = [(me_a, up), (me_a, down)]
        greeted += [line_peer(d) for d in range(1, 8)]
        greeted += [plane_peer(d) for d in range(1, 16)]
        greeted += [angle_peer(d) for d in range(5, 8)]
        for peer in greeted:
            pl.semaphore_signal(barrier, inc=1, device_id=peer, device_id_type=MESH)
        pl.semaphore_wait(barrier, len(greeted))

        off_copies = [
            remote(off, off_up, off_send.at[0], off_recv.at[0], (me_a, down)),
            remote(off, off_down, off_send.at[1], off_recv.at[1], (me_a, up)),
        ]
        off_load.wait()
        for copy in off_copies:
            copy.start()

        lane = lax.broadcasted_iota(jnp.int32, (half, LANES), 1)
        row = lax.broadcasted_iota(jnp.int32, (half, LANES), 0)

        loads[0].wait()
        pr = probe[0]
        pi = probe[1]
        power[pl.ds(0, half), :] = jnp.zeros((half, LANES), F32)
        power[pl.ds(half, patch), :] = pr * pr + pi * pi
        power[pl.ds(half + patch, half), :] = jnp.zeros((half, LANES), F32)
        for c in range(2):
            pad_up[c, pl.ds(half, half), :] = jnp.zeros((half, LANES), F32)
            pad_down[c, pl.ds(0, half), :] = jnp.zeros((half, LANES), F32)
        part[...] = jnp.zeros(part.shape, F32)
        for copy in field_loads:
            copy.wait()

        def place(table, owner, p):
            first = table[0, 0, p] - (owner * band - half)
            return jnp.minimum(jnp.maximum(first, 0), band), jnp.minimum(jnp.maximum(table[0, 1, p], 0), width - patch)

        def window(c, first, count, column):
            block = column >> 7
            shift = column & (LANES - 1)
            back = (LANES - shift) & (LANES - 1)
            left = pltpu.roll(field[c, block, pl.ds(first, count), :], back, 1)
            right = pltpu.roll(field[c, block + 1, pl.ds(first, count), :], back, 1)
            if count == half:
                return jnp.where(lane < LANES - shift, left, right)
            wide = lax.broadcasted_iota(jnp.int32, (count, LANES), 1)
            return jnp.where(wide < LANES - shift, left, right)

        for copy in off_copies:
            copy.wait()

        def halo_copy(p, which):
            if which == 0:
                return remote(send_down.at[p], halo_up.at[p], halo_send.at[0, p], halo_recv.at[0, p], (me_a, down))
            return remote(send_up.at[p], halo_down.at[p], halo_send.at[1, p], halo_recv.at[1, p], (me_a, up))

        def send_halo(p, _):
            r, column = place(off_down, down, p)
            for c in range(2):
                send_down[p, c] = window(c, half + r, half, column)
            halo_copy(p, 0).start()
            r, column = place(off_up, up, p)
            for c in range(2):
                send_up[p, c] = window(c, r, half, column)
            halo_copy(p, 1).start()
            return 0

        lax.fori_loop(0, per_device, send_halo, 0)

        tables = ((off, me_p, 2 * half), (off_up, up, 3 * half), (off_down, down, half))

        def spread_power(p, _):
            for k, (table, owner, base) in enumerate(tables):
                r, column = place(table, owner, p)
                spread[k * per_device + p, 0] = pltpu.roll(
                    power[pl.ds(base - r, half), :], column & (LANES - 1), 1)
            return 0

        lax.fori_loop(0, per_device, spread_power, 0)

        def covers(b, k, p):
            table, _, _ = tables[k]
            away = lane + (b * LANES - table[0, 1, p])
            return (away >= 0) & (away < LANES)

        def weigh(b, _):
            total = jnp.ones((half, LANES), F32)
            for k in range(3):
                for p in range(per_device):
                    total += jnp.where(covers(b, k, p), spread[k * per_device + p, 0], 0.0)
            inverse[b] = 1.0 / total
            return 0

        lax.fori_loop(0, blocks, weigh, 0)

        loads[1].wait()
        loads[2].wait()

        def grad_copy(p, which):
            if which == 0:
                return remote(grad.at[p, :, pl.ds(half, half), :], grad_up.at[p],
                              grad_send.at[0, p], grad_recv.at[0, p], (me_a, down))
            return remote(grad.at[p, :, pl.ds(0, half), :], grad_down.at[p],
                          grad_send.at[1, p], grad_recv.at[1, p], (me_a, up))

        def one_patch(p, _):
            r, column = place(off, me_p, p)
            own = [window(c, r, patch, column) for c in range(2)]
            halo_copy(p, 0).wait_recv()
            halo_copy(p, 1).wait_recv()
            low = row < half - r
            q = [
                jnp.concatenate([
                    jnp.where(low, halo_up[p, c], own[c][:half]),
                    jnp.where(low, own[c][half:], halo_down[p, c])], axis=0)
                for c in range(2)
            ]
            qr, qi = q
            pr = probe[0]
            pi = probe[1]
            wr = pr * qr - pi * qi
            wi = pr * qi + pi * qr
            forward = (dft[0], dft[1])
            backward = (dft[2], dft[3])
            mid = product(split(jnp.concatenate([wr, wi], axis=1)), forward)
            spec = product(backward, split(jnp.concatenate([mid[:, :patch], mid[:, patch:]], axis=0)))
            sr, si = spec[:patch], spec[patch:]
            factor = amp[p] / jnp.maximum(jnp.sqrt(sr * sr + si * si), 0.5)
            mid = product(split(jnp.concatenate([factor * sr, factor * si], axis=1)), backward)
            wave = product(forward, split(jnp.concatenate([mid[:, :patch], mid[:, patch:]], axis=0)))
            dr = wave[:patch] - wr
            di = wave[patch:] - wi
            grad[p, 0] = pr * dr + pi * di
            grad[p, 1] = pr * di - pi * dr
            grad_copy(p, 0).start()
            grad_copy(p, 1).start()
            part[0] += qr * dr + qi * di
            part[1] += qr * di - qi * dr
            part[2] += qr * qr + qi * qi
            return 0

        lax.fori_loop(0, per_device, one_patch, 0)

        lot = z * 4 + y

        def part_copy(d):
            theirs = ((z + (d >> 2)) & 3) * 4 + ((y + (d & 3)) & 3)
            return remote(part.at[:, pl.ds(pl.multiple_of(theirs * share, share), share), :], parts.at[d],
                          group_send.at[0], group_recv.at[0], plane_peer(d))

        for d in range(1, positions):
            part_copy(d).start()

        def spread_grad(k, p, source):
            table, owner, _ = tables[k]
            r, column = place(table, owner, p)
            for c in range(2):
                spread[k * per_device + p, c] = pltpu.roll(
                    source(c)[pl.ds(half - r, half), :], column & (LANES - 1), 1)

        def spread_own(p, _):
            spread_grad(0, p, lambda c: grad.at[p, c])
            return 0

        lax.fori_loop(0, per_device, spread_own, 0)

        def spread_near(p, _):
            grad_copy(p, 0).wait_recv()
            for c in range(2):
                pad_up[c, pl.ds(0, half), :] = grad_up[p, c]
            spread_grad(1, p, lambda c: pad_up.at[c])
            grad_copy(p, 1).wait_recv()
            for c in range(2):
                pad_down[c, pl.ds(half, half), :] = grad_down[p, c]
            spread_grad(2, p, lambda c: pad_down.at[c])
            return 0

        lax.fori_loop(0, per_device, spread_near, 0)

        def update(b, _):
            total = [jnp.zeros((half, LANES), F32) for _ in range(2)]
            for k in range(3):
                for p in range(per_device):
                    inside = covers(b, k, p)
                    for c in range(2):
                        total[c] += jnp.where(inside, spread[k * per_device + p, c], 0.0)
            at = pl.ds(pl.multiple_of(b * LANES, LANES), LANES)
            for c in range(2):
                fresh[0, c, :, at] = field[c, b, pl.ds(half, band), :] + total[c] * inverse[b]
            return 0

        lax.fori_loop(0, blocks, update, 0)

        loads[3].wait()
        high, low = split(fresh[0, 1])
        both = jnp.concatenate([high, low], axis=0)
        tile = ramp.shape[2]
        for j in range(width // tile):
            rows = pl.ds(width - tile - j * tile, width)
            twice = dot(both, ramp[0, rows, :])
            piece = twice[:band] + (twice[band:] + dot(high, ramp[1, rows, :]))
            for a in range(angles):
                filt[a, :, pl.ds(j * tile, tile)] = piece[a * rows_each:(a + 1) * rows_each]

        def together(ref, kind):
            return remote(ref, ref, group_send.at[kind], group_recv.at[kind], plane_peer(1))

        all_parts = together(parts.at[pl.ds(1, positions - 1)], 0)
        all_merges = together(merges.at[pl.ds(1, angles - 1)], 1)
        all_shares = together(new_probe.at[:, pl.ds(0, patch - share), :], 2)

        all_parts.wait_recv()
        own_share = pl.ds(pl.multiple_of(lot * share, share), share)
        total = part[:, own_share, :]
        for d in range(1, positions):
            total += parts[d]
        merges[0] = total
        place_in_line = far * 4 + side

        def merge_copy(d):
            return remote(merges.at[0], merges.at[d], group_send.at[1], group_recv.at[1], line_peer(d))

        for d in range(1, angles):
            merge_copy(d).start()

        def swap_copy(d):
            peer = angle_peer(d)
            return remote(filt.at[peer[0]], sino.at[d], swap_send.at[d], swap_recv.at[d], peer)

        for d in (4, 5, 7, 6, 1, 3, 2):
            swap_copy(d).start()
        sino[0] = filt[me_a]

        loads[4].wait()
        loads[5].wait()
        total_recon[...] = jnp.zeros(total_recon.shape, F32)

        def back(d, _):
            @pl.when(d > 0)
            def _():
                swap_copy(d).wait_recv()

            a = angle_source(d)
            rows = sino[d]
            rise = pltpu.roll(rows, width - 1, 1) - rows
            for depth in range(zwin):
                for b in range(blocks):
                    at = pl.ds(b * LANES, LANES)
                    k = jnp.broadcast_to(index[a, pl.ds(depth, 1), at], (rows_each, LANES))
                    w = jnp.broadcast_to(weight[a, pl.ds(depth, 1), at], (rows_each, LANES))
                    block = k >> 7
                    inside = k & (LANES - 1)
                    lower = jnp.zeros((rows_each, LANES), F32)
                    slope = jnp.zeros((rows_each, LANES), F32)
                    for s in range(blocks):
                        here = block == s
                        cut = slice(s * LANES, (s + 1) * LANES)
                        lower = jnp.where(here, pick(rows[:, cut], inside), lower)
                        slope = jnp.where(here, pick(rise[:, cut], inside), slope)
                    total_recon[depth, :, at] += lower + w * slope
            return 0

        def share_copy(d):
            return remote(new_probe.at[:, own_share, :], new_probe.at[:, own_share, :],
                          group_send.at[2], group_recv.at[2], plane_peer(d))

        def step(d, _):
            @pl.when(d == EARLY)
            def _():
                all_merges.wait_recv()
                total = merges[place_in_line]
                for place in range(1, angles):
                    total += merges[place_in_line ^ place]
                bottom = total[2] + 1.0
                for c in range(2):
                    new_probe[c, own_share, :] = probe[c, own_share, :] + total[c] / bottom
                for k in range(1, positions):
                    share_copy(k).start()

            return back(d, 0)

        lax.fori_loop(0, angles, step, 0)
        for depth in range(zwin):
            recon[depth] = total_recon[depth] * (math.pi / angles)

        for p in range(per_device):
            for which in range(2):
                halo_copy(p, which).wait_send()
                grad_copy(p, which).wait_send()
        for d in range(1, angles):
            swap_copy(d).wait_send()
        all_parts.wait_send()
        all_merges.wait_send()
        all_shares.wait_recv()
        probe_out[...] = new_probe[...]
        all_shares.wait_send()

    def scratch():
        vm = pltpu.VMEM
        dma = pltpu.SemaphoreType.DMA
        slab = (per_device, 2, half, LANES)
        tile = 256
        return [
            pltpu.SMEM((1, 2, per_device), jnp.int32),
            pltpu.SMEM((1, 2, per_device), jnp.int32),
            pltpu.SMEM((1, 2, per_device), jnp.int32),
            vm((per_device, patch, patch), F32),
            vm((2, patch, patch), F32),
            vm((2, blocks + 1, band + patch, LANES), F32),
            vm((angles, zwin, width), jnp.int32),
            vm((angles, zwin, width), F32),
            vm((4, 2 * patch, 2 * patch), BF16),
            vm((2, 2 * width - tile, tile), BF16),
            vm(slab, F32),
            vm(slab, F32),
            vm(slab, F32),
            vm(slab, F32),
            vm((per_device, 2, patch, LANES), F32),
            vm(slab, F32),
            vm(slab, F32),
            vm((2, patch, LANES), F32),
            vm((2, patch, LANES), F32),
            vm((2 * patch, LANES), F32),
            vm((blocks, band, LANES), F32),
            vm((3 * per_device, 2, half, LANES), F32),
            vm((angles, rows_each, width), F32),
            vm((angles, rows_each, width), F32),
            vm((zwin, rows_each, width), F32),
            vm((3, patch, LANES), F32),
            vm((positions, 3, share, LANES), F32),
            vm((angles, 3, share, LANES), F32),
            vm((2, patch, LANES), F32),
            dma((7,)),
            dma((2 * blocks,)),
            dma((2,)), dma((2,)),
            dma((2, per_device)), dma((2, per_device)),
            dma((2, per_device)), dma((2, per_device)),
            dma((angles,)), dma((angles,)),
            dma((3,)), dma((3,)),
        ]

    return kernel, scratch


def solution(mesh):
    angles, positions = mesh.shape["angle"], mesh.shape["pos"]

    def on_device(amplitude, offsets, probe_field, object_field, interp_index, interp_weight):
        band, width = object_field.shape[2:]
        patch = probe_field.shape[1]
        zwin = interp_index.shape[1]
        kernel, scratch = make_kernel(angles, positions, patch, band, offsets.shape[1], width, zwin)
        anywhere = pl.BlockSpec(memory_space=pl.ANY)
        in_hbm = pl.BlockSpec(memory_space=pltpu.HBM)
        in_vmem = pl.BlockSpec(memory_space=pltpu.VMEM)
        rows_each = band // angles
        ready = pl.pallas_call(
            kernel,
            name="ptycho",
            out_shape=(
                jax.ShapeDtypeStruct(object_field.shape, F32),
                jax.ShapeDtypeStruct(probe_field.shape, F32),
                jax.ShapeDtypeStruct((zwin, rows_each, width), F32),
            ),
            in_specs=[in_hbm] * 8,
            out_specs=(in_vmem,) * 3,
            scratch_shapes=scratch(),
            compiler_params=pltpu.CompilerParams(
                collective_id=0, has_side_effects=True, vmem_limit_bytes=32 * 1024 * 1024
            ),
        )(
            *(
                pltpu.with_memory_space_constraint(x, pltpu.HBM)
                for x in (
                    jnp.swapaxes(offsets, 1, 2), amplitude, probe_field, object_field, interp_index, interp_weight,
                    jnp.asarray(dft_constant(patch)), jnp.asarray(ramp_constant(width, 256)),
                )
            ),
        )
        return pl.pallas_call(
            put_out,
            name="put_out",
            out_shape=(
                jax.ShapeDtypeStruct(object_field.shape, F32),
                jax.ShapeDtypeStruct(probe_field.shape, F32),
                jax.ShapeDtypeStruct((1, rows_each, zwin, width), F32),
            ),
            in_specs=[in_vmem] * 3,
            out_specs=(anywhere,) * 3,
            scratch_shapes=[pltpu.SemaphoreType.DMA((2 + zwin,))],
            compiler_params=pltpu.CompilerParams(vmem_limit_bytes=4 * 1024 * 1024),
        )(*ready)

    return jax.shard_map(
        on_device,
        mesh=mesh,
        in_specs=(
            P("angle", "pos", None, None),
            P("angle", "pos", None),
            P(),
            P("angle", None, "pos", None),
            P(),
            P(),
        ),
        out_specs=(P("angle", None, "pos", None), P(), P("pos", "angle", None, None)),
        check_vma=False,
    )
```

```python
import math

import jax
import jax.numpy as jnp
import ml_dtypes
import numpy as np
from jax import lax
from jax.experimental import pallas as pl
from jax.experimental.pallas import tpu as pltpu
from jax.sharding import PartitionSpec as P

MESH = pl.DeviceIdType.MESH
F32 = jnp.float32
BF16 = jnp.bfloat16
LANES = 128
EARLY = 2


def halves(table):
    high = table.astype(np.float32).astype(ml_dtypes.bfloat16)
    low = (table.astype(np.float32) - high.astype(np.float32)).astype(ml_dtypes.bfloat16)
    return high, low


def dft_constant(n):
    ramp = np.arange(n)
    theta = (ramp[:, None] * ramp[None, :] % n) * (2.0 * math.pi / n)
    real, imag = np.cos(theta) / math.sqrt(n), -np.sin(theta) / math.sqrt(n)
    forward = np.block([[real, imag], [-imag, real]])
    return np.stack([*halves(forward), *halves(forward.T)])


def ramp_constant(length, tile):
    differ = (length - tile) + np.arange(tile)[None, :] - np.arange(2 * length - tile)[:, None]
    squared = np.maximum(differ.astype(np.float64) ** 2, 1.0)
    odd = np.where(differ % 2 != 0, -1.0 / (math.pi * math.pi * squared), 0.0)
    return np.stack(halves(np.where(differ == 0, 0.25, odd)))


def split(value):
    high = value.astype(BF16)
    return high, (value - high.astype(F32)).astype(BF16)


def dot(left, right):
    return jnp.dot(left, right, preferred_element_type=F32)


def times_table(value, table):
    n = value.shape[0]
    high, low = split(value)
    twice = dot(jnp.concatenate([high, low], axis=0), table[0])
    return twice[:n] + (twice[n:] + dot(high, table[1]))


def table_times(table, value):
    n = value.shape[1]
    high, low = split(value)
    twice = dot(table[0], jnp.concatenate([high, low], axis=1))
    return twice[:, :n] + (twice[:, n:] + dot(table[1], high))


def pick(values, lanes):
    return jnp.take_along_axis(values, lanes, axis=1, mode="promise_in_bounds")


def put_out(obj, probe, recon, obj_out, probe_out, recon_out, sems):
    copies = [
        pltpu.make_async_copy(obj, obj_out, sems.at[0]),
        pltpu.make_async_copy(probe, probe_out, sems.at[1]),
    ]
    for depth in range(recon.shape[0]):
        copies.append(pltpu.make_async_copy(recon.at[depth], recon_out.at[0, :, depth, :], sems.at[2 + depth]))
    for copy in copies:
        copy.start()
    for copy in copies:
        copy.wait()


def make_kernel(angles, positions, patch, band, per_device, width, zwin):
    blocks = width // LANES
    half = patch // 2
    rows_each = band // angles
    plane = 16
    share = patch // (2 * plane)

    def kernel(
        off_hbm, amp_hbm, probe_hbm, obj_hbm, index_hbm, weight_hbm, dft_hbm, ramp_hbm,
        fresh, probe_out, recon,
        off, off_up, off_down, amp, probe, field, index, weight, dft, ramp,
        send_down, send_up, halo_up, halo_down, grad, grad_up, grad_down, pad_up, pad_down,
        power, inverse, spread, filt, sino, total_recon,
        part, half_in, lots, parts, merges, shares,
        load_sem, field_sem, word, off_send, off_recv,
        halo_send, halo_recv, grad_send, grad_recv,
        swap_send, swap_recv, group_send, group_recv,
    ):
        me_a = lax.axis_index("angle")
        me_p = lax.axis_index("pos")
        down = lax.rem(me_p + 1, positions)
        up = lax.rem(me_p + positions - 1, positions)

        def remote(src, dst, send, recv, peer):
            return pltpu.make_async_remote_copy(
                src_ref=src, dst_ref=dst, send_sem=send, recv_sem=recv,
                device_id=peer, device_id_type=MESH,
            )

        field_loads = []
        for c in range(2):
            for b in range(blocks):
                field_loads.append(pltpu.make_async_copy(
                    obj_hbm.at[0, c, :, pl.ds(b * LANES, LANES)],
                    field.at[c, b, pl.ds(half, band), :], field_sem.at[c * blocks + b]))
        loads = [
            pltpu.make_async_copy(probe_hbm, probe, load_sem.at[0]),
            pltpu.make_async_copy(amp_hbm.at[0], amp, load_sem.at[1]),
            pltpu.make_async_copy(dft_hbm, dft, load_sem.at[2]),
            pltpu.make_async_copy(ramp_hbm, ramp, load_sem.at[3]),
            pltpu.make_async_copy(index_hbm, index, load_sem.at[4]),
            pltpu.make_async_copy(weight_hbm, weight, load_sem.at[5]),
        ]
        off_load = pltpu.make_async_copy(off_hbm, off, load_sem.at[6])
        for copy in [off_load] + field_loads + loads:
            copy.start()

        z, far = me_a >> 1, me_a & 1
        y, side = me_p >> 2, me_p & 3
        core = me_p & 1

        def plane_peer(d, other=0):
            return (((z + (d >> 2)) & 3) * 2 + far, ((y + (d & 3)) & 3) * 4 + (side ^ other))

        def line_peer(d):
            return (z * 2 + (far ^ (d >> 1)), y * 4 + (side ^ ((d & 1) * 2)))

        def angle_peer(d):
            return (((z + (d & 3)) & 3) * 2 + (far ^ (d >> 2)), me_p)

        def angle_source(d):
            return ((z - (d & 3)) & 3) * 2 + (far ^ (d >> 2))

        def signal(sem, peers):
            for peer in peers:
                pl.semaphore_signal(sem, inc=1, device_id=peer, device_id_type=MESH)

        near = [plane_peer(4), plane_peer(12), plane_peer(1), plane_peer(3), plane_peer(0, 1), line_peer(1), line_peer(2)]
        barrier = pltpu.get_barrier_semaphore()
        signal(barrier, [(me_a, up), (me_a, down)] + near)
        pl.semaphore_wait(barrier, 2 + len(near))

        def tell(k):
            signal(word.at[k], near)

        def hear(k):
            pl.semaphore_wait(word.at[k], len(near))

        off_copies = [
            remote(off, off_up, off_send.at[0], off_recv.at[0], (me_a, down)),
            remote(off, off_down, off_send.at[1], off_recv.at[1], (me_a, up)),
        ]
        off_load.wait()
        for copy in off_copies:
            copy.start()
        tell(0)

        lane = lax.broadcasted_iota(jnp.int32, (half, LANES), 1)
        row = lax.broadcasted_iota(jnp.int32, (half, LANES), 0)

        loads[0].wait()
        pr = probe[0]
        pi = probe[1]
        power[pl.ds(0, half), :] = jnp.zeros((half, LANES), F32)
        power[pl.ds(half, patch), :] = pr * pr + pi * pi
        power[pl.ds(half + patch, half), :] = jnp.zeros((half, LANES), F32)
        for c in range(2):
            pad_up[c, pl.ds(half, half), :] = jnp.zeros((half, LANES), F32)
            pad_down[c, pl.ds(0, half), :] = jnp.zeros((half, LANES), F32)
        part[...] = jnp.zeros(part.shape, F32)
        for copy in field_loads:
            copy.wait()

        def place(table, owner, p):
            first = table[0, 0, p] - (owner * band - half)
            return jnp.minimum(jnp.maximum(first, 0), band), jnp.minimum(jnp.maximum(table[0, 1, p], 0), width - patch)

        def window(c, first, count, column):
            block = column >> 7
            shift = column & (LANES - 1)
            back = (LANES - shift) & (LANES - 1)
            left = pltpu.roll(field[c, block, pl.ds(first, count), :], back, 1)
            right = pltpu.roll(field[c, block + 1, pl.ds(first, count), :], back, 1)
            if count == half:
                return jnp.where(lane < LANES - shift, left, right)
            wide = lax.broadcasted_iota(jnp.int32, (count, LANES), 1)
            return jnp.where(wide < LANES - shift, left, right)

        for copy in off_copies:
            copy.wait()
        hear(0)
        tell(1)

        def halo_copy(p, which):
            if which == 0:
                return remote(send_down.at[p], halo_up.at[p], halo_send.at[0, p], halo_recv.at[0, p], (me_a, down))
            return remote(send_up.at[p], halo_down.at[p], halo_send.at[1, p], halo_recv.at[1, p], (me_a, up))

        def send_halo(p, _):
            r, column = place(off_down, down, p)
            for c in range(2):
                send_down[p, c] = window(c, half + r, half, column)
            halo_copy(p, 0).start()
            r, column = place(off_up, up, p)
            for c in range(2):
                send_up[p, c] = window(c, r, half, column)
            halo_copy(p, 1).start()
            return 0

        lax.fori_loop(0, per_device, send_halo, 0)

        tables = ((off, me_p, 2 * half), (off_up, up, 3 * half), (off_down, down, half))

        def spread_power(p, _):
            for k, (table, owner, base) in enumerate(tables):
                r, column = place(table, owner, p)
                spread[k * per_device + p, 0] = pltpu.roll(
                    power[pl.ds(base - r, half), :], column & (LANES - 1), 1)
            return 0

        lax.fori_loop(0, per_device, spread_power, 0)

        def covers(b, k, p):
            table, _, _ = tables[k]
            away = lane + (b * LANES - table[0, 1, p])
            return (away >= 0) & (away < LANES)

        def weigh(b, _):
            total = jnp.ones((half, LANES), F32)
            for k in range(3):
                for p in range(per_device):
                    total += jnp.where(covers(b, k, p), spread[k * per_device + p, 0], 0.0)
            inverse[b] = 1.0 / total
            return 0

        lax.fori_loop(0, blocks, weigh, 0)

        hear(1)
        tell(2)
        loads[1].wait()
        loads[2].wait()

        def grad_copy(p, which):
            if which == 0:
                return remote(grad.at[p, :, pl.ds(half, half), :], grad_up.at[p],
                              grad_send.at[0, p], grad_recv.at[0, p], (me_a, down))
            return remote(grad.at[p, :, pl.ds(0, half), :], grad_down.at[p],
                          grad_send.at[1, p], grad_recv.at[1, p], (me_a, up))

        def one_patch(p, _):
            @pl.when(p == 1)
            def _():
                hear(2)
                tell(3)

            r, column = place(off, me_p, p)
            own = [window(c, r, patch, column) for c in range(2)]
            halo_copy(p, 0).wait_recv()
            halo_copy(p, 1).wait_recv()
            low = row < half - r
            q = [
                jnp.concatenate([
                    jnp.where(low, halo_up[p, c], own[c][:half]),
                    jnp.where(low, own[c][half:], halo_down[p, c])], axis=0)
                for c in range(2)
            ]
            qr, qi = q
            pr = probe[0]
            pi = probe[1]
            wr = pr * qr - pi * qi
            wi = pr * qi + pi * qr
            forward = (dft[0], dft[1])
            backward = (dft[2], dft[3])
            mid = times_table(jnp.concatenate([wr, wi], axis=1), forward)
            spec = table_times(backward, jnp.concatenate([mid[:, :patch], mid[:, patch:]], axis=0))
            sr, si = spec[:patch], spec[patch:]
            factor = amp[p] / jnp.maximum(jnp.sqrt(sr * sr + si * si), 0.5)
            mid = times_table(jnp.concatenate([factor * sr, factor * si], axis=1), backward)
            wave = table_times(forward, jnp.concatenate([mid[:, :patch], mid[:, patch:]], axis=0))
            dr = wave[:patch] - wr
            di = wave[patch:] - wi
            grad[p, 0] = pr * dr + pi * di
            grad[p, 1] = pr * di - pi * dr
            grad_copy(p, 0).start()
            grad_copy(p, 1).start()
            part[0] += qr * dr + qi * di
            part[1] += qr * di - qi * dr
            part[2] += qr * qr + qi * qi
            return 0

        lax.fori_loop(0, per_device, one_patch, 0)

        hear(3)
        lot = z * 4 + y
        mine_half = pl.ds(pl.multiple_of(core * half, half), half)
        half_copy = remote(part.at[:, pl.ds(pl.multiple_of((1 - core) * half, half), half), :], half_in,
                           group_send.at[0], group_recv.at[0], plane_peer(0, 1))
        half_copy.start()

        def spread_grad(k, p, source):
            table, owner, _ = tables[k]
            r, column = place(table, owner, p)
            for c in range(2):
                spread[k * per_device + p, c] = pltpu.roll(
                    source(c)[pl.ds(half - r, half), :], column & (LANES - 1), 1)

        def spread_own(p, _):
            spread_grad(0, p, lambda c: grad.at[p, c])
            return 0

        lax.fori_loop(0, per_device, spread_own, 0)

        half_copy.wait()
        total = part[:, mine_half, :] + half_in[...]
        for k in range(plane):
            lots[k] = total[:, k * share:(k + 1) * share, :]

        def part_copy(d):
            theirs = ((z + (d >> 2)) & 3) * 4 + ((y + (d & 3)) & 3)
            return remote(lots.at[theirs], parts.at[d], group_send.at[1], group_recv.at[1], plane_peer(d))

        for d in range(1, plane):
            part_copy(d).start()

        def spread_near(p, _):
            grad_copy(p, 0).wait_recv()
            for c in range(2):
                pad_up[c, pl.ds(0, half), :] = grad_up[p, c]
            spread_grad(1, p, lambda c: pad_up.at[c])
            grad_copy(p, 1).wait_recv()
            for c in range(2):
                pad_down[c, pl.ds(half, half), :] = grad_down[p, c]
            spread_grad(2, p, lambda c: pad_down.at[c])
            return 0

        lax.fori_loop(0, per_device, spread_near, 0)

        def update(b, _):
            total = [jnp.zeros((half, LANES), F32) for _ in range(2)]
            for k in range(3):
                for p in range(per_device):
                    inside = covers(b, k, p)
                    for c in range(2):
                        total[c] += jnp.where(inside, spread[k * per_device + p, c], 0.0)
            at = pl.ds(pl.multiple_of(b * LANES, LANES), LANES)
            for c in range(2):
                fresh[0, c, :, at] = field[c, b, pl.ds(half, band), :] + total[c] * inverse[b]
            return 0

        lax.fori_loop(0, blocks, update, 0)

        loads[3].wait()
        high, low = split(fresh[0, 1])
        both = jnp.concatenate([high, low], axis=0)
        tile = ramp.shape[2]
        for j in range(width // tile):
            rows = pl.ds(width - tile - j * tile, width)
            twice = dot(both, ramp[0, rows, :])
            piece = twice[:band] + (twice[band:] + dot(high, ramp[1, rows, :]))
            for a in range(angles):
                filt[a, :, pl.ds(j * tile, tile)] = piece[a * rows_each:(a + 1) * rows_each]

        def together(ref, kind):
            return remote(ref, ref, group_send.at[kind], group_recv.at[kind], plane_peer(1))

        all_parts = together(parts.at[pl.ds(1, plane - 1)], 1)
        all_merges = together(merges.at[pl.ds(1, 3)], 2)
        all_shares = together(shares.at[pl.ds(0, 2 * plane - 1)], 3)

        all_parts.wait_recv()
        total = lots[lot]
        for d in range(1, plane):
            total += parts[d]
        merges[0] = total
        place_in_line = far * 2 + (side >> 1)

        def merge_copy(d):
            return remote(merges.at[0], merges.at[d], group_send.at[2], group_recv.at[2], line_peer(d))

        for d in range(1, 4):
            merge_copy(d).start()

        def swap_copy(d):
            peer = angle_peer(d)
            return remote(filt.at[peer[0]], sino.at[d], swap_send.at[d], swap_recv.at[d], peer)

        for d in (4, 5, 7, 6, 1, 3, 2):
            swap_copy(d).start()
        sino[0] = filt[me_a]

        loads[4].wait()
        loads[5].wait()
        total_recon[...] = jnp.zeros(total_recon.shape, F32)

        def back(d, _):
            @pl.when(d > 0)
            def _():
                swap_copy(d).wait_recv()

            a = angle_source(d)
            rows = sino[d]
            rise = pltpu.roll(rows, width - 1, 1) - rows
            for depth in range(zwin):
                for b in range(blocks):
                    at = pl.ds(b * LANES, LANES)
                    k = jnp.broadcast_to(index[a, pl.ds(depth, 1), at], (rows_each, LANES))
                    w = jnp.broadcast_to(weight[a, pl.ds(depth, 1), at], (rows_each, LANES))
                    block = k >> 7
                    inside = k & (LANES - 1)
                    lower = jnp.zeros((rows_each, LANES), F32)
                    slope = jnp.zeros((rows_each, LANES), F32)
                    for s in range(blocks):
                        here = block == s
                        cut = slice(s * LANES, (s + 1) * LANES)
                        lower = jnp.where(here, pick(rows[:, cut], inside), lower)
                        slope = jnp.where(here, pick(rise[:, cut], inside), slope)
                    total_recon[depth, :, at] += lower + w * slope
            return 0

        slot = core * plane + lot
        share_copies = [
            remote(shares.at[slot], shares.at[slot], group_send.at[3], group_recv.at[3], plane_peer(d, other))
            for d in range(plane) for other in range(2) if d or other
        ]

        def step(d, _):
            @pl.when(d == EARLY)
            def _():
                all_merges.wait_recv()
                total = merges[place_in_line]
                for place in range(1, 4):
                    total += merges[place_in_line ^ place]
                bottom = total[2] + 1.0
                for c in range(2):
                    shares[slot, c] = probe[c, pl.ds(slot * share, share), :] + total[c] / bottom
                for copy in share_copies:
                    copy.start()

            return back(d, 0)

        lax.fori_loop(0, angles, step, 0)
        for depth in range(zwin):
            recon[depth] = total_recon[depth] * (math.pi / angles)

        for p in range(per_device):
            for which in range(2):
                halo_copy(p, which).wait_send()
                grad_copy(p, which).wait_send()
        for d in range(1, angles):
            swap_copy(d).wait_send()
        all_parts.wait_send()
        all_merges.wait_send()
        all_shares.wait_recv()
        for k in range(2 * plane):
            for c in range(2):
                probe_out[c, pl.ds(k * share, share), :] = shares[k, c]
        all_shares.wait_send()

    def scratch():
        vm = pltpu.VMEM
        dma = pltpu.SemaphoreType.DMA
        slab = (per_device, 2, half, LANES)
        tile = 256
        return [
            pltpu.SMEM((1, 2, per_device), jnp.int32),
            pltpu.SMEM((1, 2, per_device), jnp.int32),
            pltpu.SMEM((1, 2, per_device), jnp.int32),
            vm((per_device, patch, patch), F32),
            vm((2, patch, patch), F32),
            vm((2, blocks + 1, band + patch, LANES), F32),
            vm((angles, zwin, width), jnp.int32),
            vm((angles, zwin, width), F32),
            vm((4, 2 * patch, 2 * patch), BF16),
            vm((2, 2 * width - tile, tile), BF16),
            vm(slab, F32),
            vm(slab, F32),
            vm(slab, F32),
            vm(slab, F32),
            vm((per_device, 2, patch, LANES), F32),
            vm(slab, F32),
            vm(slab, F32),
            vm((2, patch, LANES), F32),
            vm((2, patch, LANES), F32),
            vm((2 * patch, LANES), F32),
            vm((blocks, band, LANES), F32),
            vm((3 * per_device, 2, half, LANES), F32),
            vm((angles, rows_each, width), F32),
            vm((angles, rows_each, width), F32),
            vm((zwin, rows_each, width), F32),
            vm((3, patch, LANES), F32),
            vm((3, half, LANES), F32),
            vm((plane, 3, share, LANES), F32),
            vm((plane, 3, share, LANES), F32),
            vm((4, 3, share, LANES), F32),
            vm((2 * plane, 2, share, LANES), F32),
            dma((7,)),
            dma((2 * blocks,)),
            pltpu.SemaphoreType.REGULAR((4,)),
            dma((2,)), dma((2,)),
            dma((2, per_device)), dma((2, per_device)),
            dma((2, per_device)), dma((2, per_device)),
            dma((angles,)), dma((angles,)),
            dma((4,)), dma((4,)),
        ]

    return kernel, scratch


def solution(mesh):
    angles, positions = mesh.shape["angle"], mesh.shape["pos"]

    def on_device(amplitude, offsets, probe_field, object_field, interp_index, interp_weight):
        band, width = object_field.shape[2:]
        patch = probe_field.shape[1]
        zwin = interp_index.shape[1]
        kernel, scratch = make_kernel(angles, positions, patch, band, offsets.shape[1], width, zwin)
        anywhere = pl.BlockSpec(memory_space=pl.ANY)
        in_hbm = pl.BlockSpec(memory_space=pltpu.HBM)
        in_vmem = pl.BlockSpec(memory_space=pltpu.VMEM)
        rows_each = band // angles
        ready = pl.pallas_call(
            kernel,
            name="ptycho",
            out_shape=(
                jax.ShapeDtypeStruct(object_field.shape, F32),
                jax.ShapeDtypeStruct(probe_field.shape, F32),
                jax.ShapeDtypeStruct((zwin, rows_each, width), F32),
            ),
            in_specs=[in_hbm] * 8,
            out_specs=(in_vmem,) * 3,
            scratch_shapes=scratch(),
            compiler_params=pltpu.CompilerParams(
                collective_id=0, has_side_effects=True, vmem_limit_bytes=32 * 1024 * 1024
            ),
        )(
            *(
                pltpu.with_memory_space_constraint(x, pltpu.HBM)
                for x in (
                    jnp.swapaxes(offsets, 1, 2), amplitude, probe_field, object_field, interp_index, interp_weight,
                    jnp.asarray(dft_constant(patch)), jnp.asarray(ramp_constant(width, 256)),
                )
            ),
        )
        return pl.pallas_call(
            put_out,
            name="put_out",
            out_shape=(
                jax.ShapeDtypeStruct(object_field.shape, F32),
                jax.ShapeDtypeStruct(probe_field.shape, F32),
                jax.ShapeDtypeStruct((1, rows_each, zwin, width), F32),
            ),
            in_specs=[in_vmem] * 3,
            out_specs=(anywhere,) * 3,
            scratch_shapes=[pltpu.SemaphoreType.DMA((2 + zwin,))],
            compiler_params=pltpu.CompilerParams(vmem_limit_bytes=4 * 1024 * 1024),
        )(*ready)

    return jax.shard_map(
        on_device,
        mesh=mesh,
        in_specs=(
            P("angle", "pos", None, None),
            P("angle", "pos", None),
            P(),
            P("angle", None, "pos", None),
            P(),
            P(),
        ),
        out_specs=(P("angle", None, "pos", None), P(), P("pos", "angle", None, None)),
        check_vma=False,
    )
```

```python
import math

import jax
import jax.numpy as jnp
import ml_dtypes
import numpy as np
from jax import lax
from jax.experimental import pallas as pl
from jax.experimental.pallas import tpu as pltpu
from jax.sharding import PartitionSpec as P

MESH = pl.DeviceIdType.MESH
F32 = jnp.float32
BF16 = jnp.bfloat16
LANES = 128
EARLY = 1
EDGE = 16


def halves(table):
    high = table.astype(np.float32).astype(ml_dtypes.bfloat16)
    low = (table.astype(np.float32) - high.astype(np.float32)).astype(ml_dtypes.bfloat16)
    return high, low


def dft_constant(n):
    ramp = np.arange(n)
    theta = (ramp[:, None] * ramp[None, :] % n) * (2.0 * math.pi / n)
    real, imag = np.cos(theta) / math.sqrt(n), -np.sin(theta) / math.sqrt(n)
    forward = np.block([[real, imag], [-imag, real]])
    return np.stack([*halves(forward), *halves(forward.T)])


def ramp_constant(length, tile):
    differ = (length - tile) + np.arange(tile)[None, :] - np.arange(2 * length - tile)[:, None]
    squared = np.maximum(differ.astype(np.float64) ** 2, 1.0)
    odd = np.where(differ % 2 != 0, -1.0 / (math.pi * math.pi * squared), 0.0)
    return np.stack(halves(np.where(differ == 0, 0.25, odd)))


def split(value):
    high = value.astype(BF16)
    return high, (value - high.astype(F32)).astype(BF16)


def dot(left, right):
    return jnp.dot(left, right, preferred_element_type=F32)


def times_table(value, table):
    n = value.shape[0]
    high, low = split(value)
    twice = dot(jnp.concatenate([high, low], axis=0), table[0])
    return twice[:n] + (twice[n:] + dot(high, table[1]))


def table_times(table, value):
    n = value.shape[1]
    high, low = split(value)
    twice = dot(table[0], jnp.concatenate([high, low], axis=1))
    return twice[:, :n] + (twice[:, n:] + dot(table[1], high))


def pick(values, lanes):
    return jnp.take_along_axis(values, lanes, axis=1, mode="promise_in_bounds")


def put_out(obj, probe, recon, obj_out, probe_out, recon_out, sems):
    copies = [
        pltpu.make_async_copy(obj, obj_out, sems.at[0]),
        pltpu.make_async_copy(probe, probe_out, sems.at[1]),
    ]
    for depth in range(recon.shape[0]):
        copies.append(pltpu.make_async_copy(recon.at[depth], recon_out.at[0, :, depth, :], sems.at[2 + depth]))
    for copy in copies:
        copy.start()
    for copy in copies:
        copy.wait()


def make_kernel(angles, positions, patch, band, per_device, width, zwin):
    blocks = width // LANES
    half = patch // 2
    slab_rows = half - EDGE
    rows_each = band // angles
    plane = 16
    share = patch // (2 * plane)

    def kernel(
        off_hbm, amp_hbm, probe_hbm, obj_hbm, index_hbm, weight_hbm, dft_hbm, ramp_hbm,
        fresh, probe_out, recon,
        off, off_up, off_down, amp, probe, field, wide, index, weight, dft, ramp,
        send_down, send_up, halo_up, halo_down, grad, grad_up, grad_down, pad_up, pad_down,
        power, inverse, spread, filt, sino, total_recon,
        part, half_in, lots, parts, merges, shares,
        load_sem, field_sem, word, edge_send, edge_recv, off_send, off_recv,
        halo_send, halo_recv, grad_send, grad_recv,
        swap_send, swap_recv, group_send, group_recv,
    ):
        me_a = lax.axis_index("angle")
        me_p = lax.axis_index("pos")
        down = lax.rem(me_p + 1, positions)
        up = lax.rem(me_p + positions - 1, positions)

        def remote(src, dst, send, recv, peer):
            return pltpu.make_async_remote_copy(
                src_ref=src, dst_ref=dst, send_sem=send, recv_sem=recv,
                device_id=peer, device_id_type=MESH,
            )

        field_loads = []
        for c in range(2):
            for b in range(blocks):
                field_loads.append(pltpu.make_async_copy(
                    obj_hbm.at[0, c, :, pl.ds(b * LANES, LANES)],
                    field.at[c, b, pl.ds(half, band), :], field_sem.at[c * blocks + b]))
        loads = [
            pltpu.make_async_copy(probe_hbm, probe, load_sem.at[0]),
            pltpu.make_async_copy(amp_hbm.at[0], amp, load_sem.at[1]),
            pltpu.make_async_copy(dft_hbm, dft, load_sem.at[2]),
            pltpu.make_async_copy(ramp_hbm, ramp, load_sem.at[3]),
            pltpu.make_async_copy(index_hbm, index, load_sem.at[4]),
            pltpu.make_async_copy(weight_hbm, weight, load_sem.at[5]),
        ]
        off_load = pltpu.make_async_copy(off_hbm, off, load_sem.at[6])
        for copy in [off_load] + field_loads + loads:
            copy.start()

        z, far = me_a >> 1, me_a & 1
        y, side = me_p >> 2, me_p & 3
        core = me_p & 1

        def plane_peer(d, other=0):
            return (((z + (d >> 2)) & 3) * 2 + far, ((y + (d & 3)) & 3) * 4 + (side ^ other))

        def line_peer(d):
            return (z * 2 + (far ^ (d >> 1)), y * 4 + (side ^ ((d & 1) * 2)))

        def angle_peer(d):
            return (((z + (d & 3)) & 3) * 2 + (far ^ (d >> 2)), me_p)

        def angle_source(d):
            return ((z - (d & 3)) & 3) * 2 + (far ^ (d >> 2))

        def signal(sem, peers):
            for peer in peers:
                pl.semaphore_signal(sem, inc=1, device_id=peer, device_id_type=MESH)

        near = [plane_peer(4), plane_peer(12), plane_peer(1), plane_peer(3), plane_peer(0, 1), line_peer(1), line_peer(2)]
        barrier = pltpu.get_barrier_semaphore()
        signal(barrier, [(me_a, up), (me_a, down)] + near)
        pl.semaphore_wait(barrier, 2 + len(near))

        def tell(k):
            signal(word.at[k], near)

        def hear(k):
            pl.semaphore_wait(word.at[k], len(near))

        off_copies = [
            remote(off, off_up, off_send.at[0], off_recv.at[0], (me_a, down)),
            remote(off, off_down, off_send.at[1], off_recv.at[1], (me_a, up)),
        ]
        off_load.wait()
        for copy in off_copies:
            copy.start()
        tell(0)

        for copy in field_loads:
            copy.wait()
        edge_copies = [
            remote(field.at[:, pl.ds(0, blocks), pl.ds(half + band - EDGE, EDGE), :],
                   wide.at[:, pl.ds(0, blocks), pl.ds(half - EDGE, EDGE), :],
                   edge_send.at[0], edge_recv.at[0], (me_a, down)),
            remote(field.at[:, pl.ds(0, blocks), pl.ds(half, EDGE), :],
                   wide.at[:, pl.ds(0, blocks), pl.ds(half + band, EDGE), :],
                   edge_send.at[1], edge_recv.at[1], (me_a, up)),
        ]
        for copy in edge_copies:
            copy.start()
        for c in range(2):
            for b in range(blocks):
                wide[c, b, pl.ds(half, band), :] = field[c, b, pl.ds(half, band), :]

        lane = lax.broadcasted_iota(jnp.int32, (half, LANES), 1)
        slab_row = lax.broadcasted_iota(jnp.int32, (slab_rows, LANES), 0)

        loads[0].wait()
        pr = probe[0]
        pi = probe[1]
        power[pl.ds(0, half), :] = jnp.zeros((half, LANES), F32)
        power[pl.ds(half, patch), :] = pr * pr + pi * pi
        power[pl.ds(half + patch, half), :] = jnp.zeros((half, LANES), F32)
        for c in range(2):
            pad_up[c, pl.ds(half, half), :] = jnp.zeros((half, LANES), F32)
            pad_down[c, pl.ds(0, half), :] = jnp.zeros((half, LANES), F32)
        part[...] = jnp.zeros(part.shape, F32)

        def place(table, owner, p):
            first = table[0, 0, p] - (owner * band - half)
            return jnp.minimum(jnp.maximum(first, 0), band), jnp.minimum(jnp.maximum(table[0, 1, p], 0), width - patch)

        def window(source, c, first, count, column):
            block = column >> 7
            shift = column & (LANES - 1)
            back = (LANES - shift) & (LANES - 1)
            left = pltpu.roll(source[c, block, pl.ds(first, count), :], back, 1)
            right = pltpu.roll(source[c, block + 1, pl.ds(first, count), :], back, 1)
            lanes = lax.broadcasted_iota(jnp.int32, (count, LANES), 1)
            return jnp.where(lanes < LANES - shift, left, right)

        for copy in off_copies:
            copy.wait()
        hear(0)
        tell(1)

        def halo_copy(p, which):
            if which == 0:
                return remote(send_down.at[p], halo_up.at[p], halo_send.at[0, p], halo_recv.at[0, p], (me_a, down))
            return remote(send_up.at[p], halo_down.at[p], halo_send.at[1, p], halo_recv.at[1, p], (me_a, up))

        def send_halo(p, _):
            r, column = place(off_down, down, p)
            for c in range(2):
                send_down[p, c] = window(field, c, half + r, slab_rows, column)
            halo_copy(p, 0).start()
            r, column = place(off_up, up, p)
            for c in range(2):
                send_up[p, c] = window(field, c, r + EDGE, slab_rows, column)
            halo_copy(p, 1).start()
            return 0

        lax.fori_loop(0, per_device, send_halo, 0)

        tables = ((off, me_p, 2 * half), (off_up, up, 3 * half), (off_down, down, half))

        def spread_power(p, _):
            for k, (table, owner, base) in enumerate(tables):
                r, column = place(table, owner, p)
                spread[k * per_device + p, 0] = pltpu.roll(
                    power[pl.ds(base - r, half), :], column & (LANES - 1), 1)
            return 0

        lax.fori_loop(0, per_device, spread_power, 0)

        def covers(b, k, p):
            table, _, _ = tables[k]
            away = lane + (b * LANES - table[0, 1, p])
            return (away >= 0) & (away < LANES)

        def weigh(b, _):
            total = jnp.ones((half, LANES), F32)
            for k in range(3):
                for p in range(per_device):
                    total += jnp.where(covers(b, k, p), spread[k * per_device + p, 0], 0.0)
            inverse[b] = 1.0 / total
            return 0

        lax.fori_loop(0, blocks, weigh, 0)

        hear(1)
        tell(2)
        for copy in edge_copies:
            copy.wait_recv()
        loads[1].wait()
        loads[2].wait()

        def grad_copy(p, which):
            if which == 0:
                return remote(grad.at[p, :, pl.ds(half, half), :], grad_up.at[p],
                              grad_send.at[0, p], grad_recv.at[0, p], (me_a, down))
            return remote(grad.at[p, :, pl.ds(0, half), :], grad_down.at[p],
                          grad_send.at[1, p], grad_recv.at[1, p], (me_a, up))

        def one_patch(p, _):
            @pl.when(p == 1)
            def _():
                hear(2)
                tell(3)

            r, column = place(off, me_p, p)
            own = [window(wide, c, r, patch, column) for c in range(2)]
            halo_copy(p, 0).wait_recv()
            halo_copy(p, 1).wait_recv()
            above = slab_row < slab_rows - r
            below = slab_row >= half - r
            q = [
                jnp.concatenate([
                    jnp.where(above, halo_up[p, c], own[c][:slab_rows]),
                    own[c][slab_rows:patch - slab_rows],
                    jnp.where(below, halo_down[p, c], own[c][patch - slab_rows:])], axis=0)
                for c in range(2)
            ]
            qr, qi = q
            pr = probe[0]
            pi = probe[1]
            wr = pr * qr - pi * qi
            wi = pr * qi + pi * qr
            forward = (dft[0], dft[1])
            backward = (dft[2], dft[3])
            mid = times_table(jnp.concatenate([wr, wi], axis=1), forward)
            spec = table_times(backward, jnp.concatenate([mid[:, :patch], mid[:, patch:]], axis=0))
            sr, si = spec[:patch], spec[patch:]
            factor = amp[p] / jnp.maximum(jnp.sqrt(sr * sr + si * si), 0.5)
            mid = times_table(jnp.concatenate([factor * sr, factor * si], axis=1), backward)
            wave = table_times(forward, jnp.concatenate([mid[:, :patch], mid[:, patch:]], axis=0))
            dr = wave[:patch] - wr
            di = wave[patch:] - wi
            grad[p, 0] = pr * dr + pi * di
            grad[p, 1] = pr * di - pi * dr
            grad_copy(p, 0).start()
            grad_copy(p, 1).start()
            part[0] += qr * dr + qi * di
            part[1] += qr * di - qi * dr
            part[2] += qr * qr + qi * qi
            return 0

        lax.fori_loop(0, per_device, one_patch, 0)

        hear(3)
        lot = z * 4 + y
        mine_half = pl.ds(pl.multiple_of(core * half, half), half)
        half_copy = remote(part.at[:, pl.ds(pl.multiple_of((1 - core) * half, half), half), :], half_in,
                           group_send.at[0], group_recv.at[0], plane_peer(0, 1))
        half_copy.start()

        def spread_grad(k, p, source):
            table, owner, _ = tables[k]
            r, column = place(table, owner, p)
            for c in range(2):
                spread[k * per_device + p, c] = pltpu.roll(
                    source(c)[pl.ds(half - r, half), :], column & (LANES - 1), 1)

        def spread_own(p, _):
            spread_grad(0, p, lambda c: grad.at[p, c])
            return 0

        lax.fori_loop(0, per_device, spread_own, 0)

        half_copy.wait()
        total = part[:, mine_half, :] + half_in[...]
        for k in range(plane):
            lots[k] = total[:, k * share:(k + 1) * share, :]

        def part_copy(d):
            theirs = ((z + (d >> 2)) & 3) * 4 + ((y + (d & 3)) & 3)
            return remote(lots.at[theirs], parts.at[d], group_send.at[1], group_recv.at[1], plane_peer(d))

        for d in range(1, plane):
            part_copy(d).start()

        def spread_near(p, _):
            grad_copy(p, 0).wait_recv()
            for c in range(2):
                pad_up[c, pl.ds(0, half), :] = grad_up[p, c]
            spread_grad(1, p, lambda c: pad_up.at[c])
            grad_copy(p, 1).wait_recv()
            for c in range(2):
                pad_down[c, pl.ds(half, half), :] = grad_down[p, c]
            spread_grad(2, p, lambda c: pad_down.at[c])
            return 0

        lax.fori_loop(0, per_device, spread_near, 0)

        def update(b, _):
            total = [jnp.zeros((half, LANES), F32) for _ in range(2)]
            for k in range(3):
                for p in range(per_device):
                    inside = covers(b, k, p)
                    for c in range(2):
                        total[c] += jnp.where(inside, spread[k * per_device + p, c], 0.0)
            at = pl.ds(pl.multiple_of(b * LANES, LANES), LANES)
            for c in range(2):
                fresh[0, c, :, at] = field[c, b, pl.ds(half, band), :] + total[c] * inverse[b]
            return 0

        lax.fori_loop(0, blocks, update, 0)

        loads[3].wait()
        high, low = split(fresh[0, 1])
        both = jnp.concatenate([high, low], axis=0)
        tile = ramp.shape[2]
        for j in range(width // tile):
            rows = pl.ds(width - tile - j * tile, width)
            twice = dot(both, ramp[0, rows, :])
            piece = twice[:band] + (twice[band:] + dot(high, ramp[1, rows, :]))
            for a in range(angles):
                filt[a, :, pl.ds(j * tile, tile)] = piece[a * rows_each:(a + 1) * rows_each]

        def together(ref, kind):
            return remote(ref, ref, group_send.at[kind], group_recv.at[kind], plane_peer(1))

        all_parts = together(parts.at[pl.ds(1, plane - 1)], 1)
        all_merges = together(merges.at[pl.ds(1, 3)], 2)
        all_shares = together(shares.at[pl.ds(0, 2 * plane - 1)], 3)

        all_parts.wait_recv()
        total = lots[lot]
        for d in range(1, plane):
            total += parts[d]
        merges[0] = total
        place_in_line = far * 2 + (side >> 1)

        def merge_copy(d):
            return remote(merges.at[0], merges.at[d], group_send.at[2], group_recv.at[2], line_peer(d))

        for d in range(1, 4):
            merge_copy(d).start()

        def swap_copy(d):
            peer = angle_peer(d)
            return remote(filt.at[peer[0]], sino.at[d], swap_send.at[d], swap_recv.at[d], peer)

        for d in (4, 5, 7, 6, 1, 3, 2):
            swap_copy(d).start()
        sino[0] = filt[me_a]

        loads[4].wait()
        loads[5].wait()
        total_recon[...] = jnp.zeros(total_recon.shape, F32)

        def back(d, _):
            @pl.when(d > 0)
            def _():
                swap_copy(d).wait_recv()

            a = angle_source(d)
            rows = sino[d]
            rise = pltpu.roll(rows, width - 1, 1) - rows
            for depth in range(zwin):
                for b in range(blocks):
                    at = pl.ds(b * LANES, LANES)
                    k = jnp.broadcast_to(index[a, pl.ds(depth, 1), at], (rows_each, LANES))
                    w = jnp.broadcast_to(weight[a, pl.ds(depth, 1), at], (rows_each, LANES))
                    block = k >> 7
                    inside = k & (LANES - 1)
                    lower = jnp.zeros((rows_each, LANES), F32)
                    slope = jnp.zeros((rows_each, LANES), F32)
                    for s in range(blocks):
                        here = block == s
                        cut = slice(s * LANES, (s + 1) * LANES)
                        lower = jnp.where(here, pick(rows[:, cut], inside), lower)
                        slope = jnp.where(here, pick(rise[:, cut], inside), slope)
                    total_recon[depth, :, at] += lower + w * slope
            return 0

        slot = core * plane + lot
        share_copies = [
            remote(shares.at[slot], shares.at[slot], group_send.at[3], group_recv.at[3], plane_peer(d, other))
            for d in range(plane) for other in range(2) if d or other
        ]

        def step(d, _):
            @pl.when(d == EARLY)
            def _():
                all_merges.wait_recv()
                total = merges[place_in_line]
                for place in range(1, 4):
                    total += merges[place_in_line ^ place]
                bottom = total[2] + 1.0
                for c in range(2):
                    shares[slot, c] = probe[c, pl.ds(slot * share, share), :] + total[c] / bottom
                for copy in share_copies:
                    copy.start()

            return back(d, 0)

        lax.fori_loop(0, angles, step, 0)
        for depth in range(zwin):
            recon[depth] = total_recon[depth] * (math.pi / angles)

        for copy in edge_copies:
            copy.wait_send()
        for p in range(per_device):
            for which in range(2):
                halo_copy(p, which).wait_send()
                grad_copy(p, which).wait_send()
        for d in range(1, angles):
            swap_copy(d).wait_send()
        all_parts.wait_send()
        all_merges.wait_send()
        all_shares.wait_recv()
        for k in range(2 * plane):
            for c in range(2):
                probe_out[c, pl.ds(k * share, share), :] = shares[k, c]
        all_shares.wait_send()

    def scratch():
        vm = pltpu.VMEM
        dma = pltpu.SemaphoreType.DMA
        slab = (per_device, 2, slab_rows, LANES)
        rim = (per_device, 2, half, LANES)
        tile = 256
        return [
            pltpu.SMEM((1, 2, per_device), jnp.int32),
            pltpu.SMEM((1, 2, per_device), jnp.int32),
            pltpu.SMEM((1, 2, per_device), jnp.int32),
            vm((per_device, patch, patch), F32),
            vm((2, patch, patch), F32),
            vm((2, blocks + 1, band + patch, LANES), F32),
            vm((2, blocks + 1, band + patch, LANES), F32),
            vm((angles, zwin, width), jnp.int32),
            vm((angles, zwin, width), F32),
            vm((4, 2 * patch, 2 * patch), BF16),
            vm((2, 2 * width - tile, tile), BF16),
            vm(slab, F32),
            vm(slab, F32),
            vm(slab, F32),
            vm(slab, F32),
            vm((per_device, 2, patch, LANES), F32),
            vm(rim, F32),
            vm(rim, F32),
            vm((2, patch, LANES), F32),
            vm((2, patch, LANES), F32),
            vm((2 * patch, LANES), F32),
            vm((blocks, band, LANES), F32),
            vm((3 * per_device, 2, half, LANES), F32),
            vm((angles, rows_each, width), F32),
            vm((angles, rows_each, width), F32),
            vm((zwin, rows_each, width), F32),
            vm((3, patch, LANES), F32),
            vm((3, half, LANES), F32),
            vm((plane, 3, share, LANES), F32),
            vm((plane, 3, share, LANES), F32),
            vm((4, 3, share, LANES), F32),
            vm((2 * plane, 2, share, LANES), F32),
            dma((7,)),
            dma((2 * blocks,)),
            pltpu.SemaphoreType.REGULAR((4,)),
            dma((2,)), dma((2,)),
            dma((2,)), dma((2,)),
            dma((2, per_device)), dma((2, per_device)),
            dma((2, per_device)), dma((2, per_device)),
            dma((angles,)), dma((angles,)),
            dma((4,)), dma((4,)),
        ]

    return kernel, scratch


def solution(mesh):
    angles, positions = mesh.shape["angle"], mesh.shape["pos"]

    def on_device(amplitude, offsets, probe_field, object_field, interp_index, interp_weight):
        band, width = object_field.shape[2:]
        patch = probe_field.shape[1]
        zwin = interp_index.shape[1]
        kernel, scratch = make_kernel(angles, positions, patch, band, offsets.shape[1], width, zwin)
        anywhere = pl.BlockSpec(memory_space=pl.ANY)
        in_hbm = pl.BlockSpec(memory_space=pltpu.HBM)
        in_vmem = pl.BlockSpec(memory_space=pltpu.VMEM)
        rows_each = band // angles
        ready = pl.pallas_call(
            kernel,
            name="ptycho",
            out_shape=(
                jax.ShapeDtypeStruct(object_field.shape, F32),
                jax.ShapeDtypeStruct(probe_field.shape, F32),
                jax.ShapeDtypeStruct((zwin, rows_each, width), F32),
            ),
            in_specs=[in_hbm] * 8,
            out_specs=(in_vmem,) * 3,
            scratch_shapes=scratch(),
            compiler_params=pltpu.CompilerParams(
                collective_id=0, has_side_effects=True, vmem_limit_bytes=32 * 1024 * 1024
            ),
        )(
            *(
                pltpu.with_memory_space_constraint(x, pltpu.HBM)
                for x in (
                    jnp.swapaxes(offsets, 1, 2), amplitude, probe_field, object_field, interp_index, interp_weight,
                    jnp.asarray(dft_constant(patch)), jnp.asarray(ramp_constant(width, 256)),
                )
            ),
        )
        return pl.pallas_call(
            put_out,
            name="put_out",
            out_shape=(
                jax.ShapeDtypeStruct(object_field.shape, F32),
                jax.ShapeDtypeStruct(probe_field.shape, F32),
                jax.ShapeDtypeStruct((1, rows_each, zwin, width), F32),
            ),
            in_specs=[in_vmem] * 3,
            out_specs=(anywhere,) * 3,
            scratch_shapes=[pltpu.SemaphoreType.DMA((2 + zwin,))],
            compiler_params=pltpu.CompilerParams(vmem_limit_bytes=4 * 1024 * 1024),
        )(*ready)

    return jax.shard_map(
        on_device,
        mesh=mesh,
        in_specs=(
            P("angle", "pos", None, None),
            P("angle", "pos", None),
            P(),
            P("angle", None, "pos", None),
            P(),
            P(),
        ),
        out_specs=(P("angle", None, "pos", None), P(), P("pos", "angle", None, None)),
        check_vma=False,
    )
```

```python
import math

import jax
import jax.numpy as jnp
import ml_dtypes
import numpy as np
from jax import lax
from jax.experimental import pallas as pl
from jax.experimental.pallas import tpu as pltpu
from jax.sharding import PartitionSpec as P

MESH = pl.DeviceIdType.MESH
F32 = jnp.float32
BF16 = jnp.bfloat16
LANES = 128
EARLY = 1
EDGE = 16
PAIR = 2


def halves(table):
    high = table.astype(np.float32).astype(ml_dtypes.bfloat16)
    low = (table.astype(np.float32) - high.astype(np.float32)).astype(ml_dtypes.bfloat16)
    return high, low


def dft_constant(n):
    ramp = np.arange(n)
    theta = (ramp[:, None] * ramp[None, :] % n) * (2.0 * math.pi / n)
    real, imag = np.cos(theta) / math.sqrt(n), -np.sin(theta) / math.sqrt(n)
    forward = np.block([[real, imag], [-imag, real]])
    return np.stack([*halves(forward), *halves(forward.T)])


def ramp_constant(length, tile):
    differ = (length - tile) + np.arange(tile)[None, :] - np.arange(2 * length - tile)[:, None]
    squared = np.maximum(differ.astype(np.float64) ** 2, 1.0)
    odd = np.where(differ % 2 != 0, -1.0 / (math.pi * math.pi * squared), 0.0)
    return np.stack(halves(np.where(differ == 0, 0.25, odd)))


def split(value):
    high = value.astype(BF16)
    return high, (value - high.astype(F32)).astype(BF16)


def dot(left, right):
    return jnp.dot(left, right, preferred_element_type=F32)


def times_table(value, table):
    n = value.shape[0]
    high, low = split(value)
    twice = dot(jnp.concatenate([high, low], axis=0), table[0])
    return twice[:n] + (twice[n:] + dot(high, table[1]))


def table_times(table, value):
    n = value.shape[1]
    high, low = split(value)
    twice = dot(table[0], jnp.concatenate([high, low], axis=1))
    return twice[:, :n] + (twice[:, n:] + dot(table[1], high))


def pick(values, lanes):
    return jnp.take_along_axis(values, lanes, axis=1, mode="promise_in_bounds")


def put_out(obj, probe, recon, obj_out, probe_out, recon_out, sems):
    copies = [
        pltpu.make_async_copy(obj, obj_out, sems.at[0]),
        pltpu.make_async_copy(probe, probe_out, sems.at[1]),
    ]
    for depth in range(recon.shape[0]):
        copies.append(pltpu.make_async_copy(recon.at[depth], recon_out.at[0, :, depth, :], sems.at[2 + depth]))
    for copy in copies:
        copy.start()
    for copy in copies:
        copy.wait()


def make_kernel(angles, positions, patch, band, per_device, width, zwin):
    blocks = width // LANES
    half = patch // 2
    slab_rows = half - EDGE
    rows_each = band // angles
    plane = 16
    share = patch // (2 * plane)

    def kernel(
        off_hbm, amp_hbm, probe_hbm, obj_hbm, index_hbm, weight_hbm, dft_hbm, ramp_hbm,
        fresh, probe_out, recon,
        off, off_near, amp, probe, field, wide, index, weight, dft, ramp,
        slabs, halo, grad, rims, pad_up, pad_down,
        power, inverse, spread, filt, sino, total_recon,
        part, half_in, lots, parts, merges, shares,
        load_sem, field_sem, word, edge_sem, off_sem,
        halo_send, halo_recv, grad_send, grad_recv,
        swap_send, swap_recv, group_send, group_recv,
    ):
        me_a = lax.axis_index("angle")
        me_p = lax.axis_index("pos")
        down = lax.rem(me_p + 1, positions)
        up = lax.rem(me_p + positions - 1, positions)

        def remote(src, dst, send, recv, peer):
            return pltpu.make_async_remote_copy(
                src_ref=src, dst_ref=dst, send_sem=send, recv_sem=recv,
                device_id=peer, device_id_type=MESH,
            )

        field_loads = []
        for c in range(2):
            for b in range(blocks):
                field_loads.append(pltpu.make_async_copy(
                    obj_hbm.at[0, c, :, pl.ds(b * LANES, LANES)],
                    field.at[c, b, pl.ds(half, band), :], field_sem.at[0]))
        own_rows = field.at[:, pl.ds(0, blocks), pl.ds(half, band), :]
        field_load = pltpu.make_async_copy(own_rows, own_rows, field_sem.at[0])
        loads = [
            pltpu.make_async_copy(probe_hbm, probe, load_sem.at[0]),
            pltpu.make_async_copy(amp_hbm.at[0], amp, load_sem.at[1]),
            pltpu.make_async_copy(dft_hbm, dft, load_sem.at[2]),
            pltpu.make_async_copy(ramp_hbm, ramp, load_sem.at[3]),
            pltpu.make_async_copy(index_hbm, index, load_sem.at[4]),
            pltpu.make_async_copy(weight_hbm, weight, load_sem.at[5]),
        ]
        off_load = pltpu.make_async_copy(off_hbm, off, load_sem.at[6])
        for copy in [off_load] + field_loads + loads:
            copy.start()

        z, far = me_a >> 1, me_a & 1
        y, side = me_p >> 2, me_p & 3
        core = me_p & 1

        def plane_peer(d, other=0):
            return (((z + (d >> 2)) & 3) * 2 + far, ((y + (d & 3)) & 3) * 4 + (side ^ other))

        def line_peer(d):
            return (z * 2 + (far ^ (d >> 1)), y * 4 + (side ^ ((d & 1) * 2)))

        def angle_peer(d):
            return (((z + (d & 3)) & 3) * 2 + (far ^ (d >> 2)), me_p)

        def angle_source(d):
            return ((z - (d & 3)) & 3) * 2 + (far ^ (d >> 2))

        def signal(sem, peers):
            for peer in peers:
                pl.semaphore_signal(sem, inc=1, device_id=peer, device_id_type=MESH)

        near = [plane_peer(4), plane_peer(12), plane_peer(1), plane_peer(3), plane_peer(0, 1), line_peer(1), line_peer(2)]
        barrier = pltpu.get_barrier_semaphore()
        signal(barrier, [(me_a, up), (me_a, down)] + near)
        pl.semaphore_wait(barrier, 2 + len(near))

        jumps = near + [plane_peer(8), plane_peer(2)]

        def tell(k):
            signal(word.at[k], jumps if k else near)

        def hear(k):
            pl.semaphore_wait(word.at[k], len(jumps if k else near))

        def together(ref, send, recv):
            return remote(ref, ref, send, recv, plane_peer(1))

        off_copies = [
            remote(off, off_near.at[0], off_sem.at[0], off_sem.at[1], (me_a, down)),
            remote(off, off_near.at[1], off_sem.at[0], off_sem.at[1], (me_a, up)),
        ]
        off_load.wait()
        for copy in off_copies:
            copy.start()
        tell(0)

        field_load.wait()
        edge_copies = [
            remote(field.at[:, pl.ds(0, blocks), pl.ds(half + band - EDGE, EDGE), :],
                   wide.at[:, pl.ds(0, blocks), pl.ds(half - EDGE, EDGE), :],
                   edge_sem.at[0], edge_sem.at[1], (me_a, down)),
            remote(field.at[:, pl.ds(0, blocks), pl.ds(half, EDGE), :],
                   wide.at[:, pl.ds(0, blocks), pl.ds(half + band, EDGE), :],
                   edge_sem.at[0], edge_sem.at[1], (me_a, up)),
        ]
        all_edges = together(wide.at[:, pl.ds(0, blocks), pl.ds(0, 2 * EDGE), :], edge_sem.at[0], edge_sem.at[1])
        for copy in edge_copies:
            copy.start()
        for c in range(2):
            for b in range(blocks):
                wide[c, b, pl.ds(half, band), :] = field[c, b, pl.ds(half, band), :]

        lane = lax.broadcasted_iota(jnp.int32, (half, LANES), 1)
        slab_row = lax.broadcasted_iota(jnp.int32, (slab_rows, LANES), 0)

        loads[0].wait()
        pr = probe[0]
        pi = probe[1]
        power[pl.ds(0, half), :] = jnp.zeros((half, LANES), F32)
        power[pl.ds(half, patch), :] = pr * pr + pi * pi
        power[pl.ds(half + patch, half), :] = jnp.zeros((half, LANES), F32)
        for c in range(2):
            pad_up[c, pl.ds(half, half), :] = jnp.zeros((half, LANES), F32)
            pad_down[c, pl.ds(0, half), :] = jnp.zeros((half, LANES), F32)
        part[...] = jnp.zeros(part.shape, F32)

        def place(table, owner, p):
            first = table[0, p] - (owner * band - half)
            return jnp.minimum(jnp.maximum(first, 0), band), jnp.minimum(jnp.maximum(table[1, p], 0), width - patch)

        def window(source, c, first, count, column):
            block = column >> 7
            shift = column & (LANES - 1)
            back = (LANES - shift) & (LANES - 1)
            left = pltpu.roll(source[c, block, pl.ds(first, count), :], back, 1)
            right = pltpu.roll(source[c, block + 1, pl.ds(first, count), :], back, 1)
            lanes = lax.broadcasted_iota(jnp.int32, (count, LANES), 1)
            return jnp.where(lanes < LANES - shift, left, right)

        together(off_near, off_sem.at[0], off_sem.at[1]).wait()
        own_off, off_up, off_down = off.at[0], off_near.at[0, 0], off_near.at[1, 0]
        hear(0)
        tell(1)

        def halo_copy(p, which):
            if which == 0:
                return remote(slabs.at[0, p], halo.at[0, p], halo_send.at[0], halo_recv.at[p // PAIR], (me_a, down))
            return remote(slabs.at[1, p], halo.at[1, p], halo_send.at[0], halo_recv.at[p // PAIR], (me_a, up))

        def send_halo(p, _):
            r, column = place(off_down, down, p)
            for c in range(2):
                slabs[0, p, c] = window(field, c, half + r, slab_rows, column)
            halo_copy(p, 0).start()
            r, column = place(off_up, up, p)
            for c in range(2):
                slabs[1, p, c] = window(field, c, r + EDGE, slab_rows, column)
            halo_copy(p, 1).start()
            return 0

        lax.fori_loop(0, per_device, send_halo, 0)

        tables = ((own_off, me_p, 2 * half), (off_up, up, 3 * half), (off_down, down, half))

        def spread_power(p, _):
            for k, (table, owner, base) in enumerate(tables):
                r, column = place(table, owner, p)
                spread[k * per_device + p, 0] = pltpu.roll(
                    power[pl.ds(base - r, half), :], column & (LANES - 1), 1)
            return 0

        lax.fori_loop(0, per_device, spread_power, 0)

        def covers(b, k, p):
            table, _, _ = tables[k]
            away = lane + (b * LANES - table[1, p])
            return (away >= 0) & (away < LANES)

        def weigh(b, _):
            total = jnp.ones((half, LANES), F32)
            for k in range(3):
                for p in range(per_device):
                    total += jnp.where(covers(b, k, p), spread[k * per_device + p, 0], 0.0)
            inverse[b] = 1.0 / total
            return 0

        lax.fori_loop(0, blocks, weigh, 0)

        hear(1)
        tell(2)
        all_edges.wait_recv()
        loads[1].wait()
        loads[2].wait()

        def grad_copy(p, which):
            if which == 0:
                return remote(grad.at[p, :, pl.ds(half, half), :], rims.at[0, p],
                              grad_send.at[0], grad_recv.at[p // PAIR], (me_a, down))
            return remote(grad.at[p, :, pl.ds(0, half), :], rims.at[1, p],
                          grad_send.at[0], grad_recv.at[p // PAIR], (me_a, up))

        def some_patches(i, _):
            ps = [i * PAIR + j for j in range(PAIR)]
            places = [place(own_off, me_p, p) for p in ps]
            own = [[window(wide, c, r, patch, column) for c in range(2)] for r, column in places]
            together(halo.at[:, pl.ds(i * PAIR, PAIR)], halo_send.at[0], halo_recv.at[i]).wait_recv()
            pr = probe[0]
            pi = probe[1]
            forward = (dft[0], dft[1])
            backward = (dft[2], dft[3])
            q, waves = [], []
            for j, p in enumerate(ps):
                above = slab_row < slab_rows - places[j][0]
                below = slab_row >= half - places[j][0]
                qr, qi = [
                    jnp.concatenate([
                        jnp.where(above, halo[0, p, c], own[j][c][:slab_rows]),
                        own[j][c][slab_rows:patch - slab_rows],
                        jnp.where(below, halo[1, p, c], own[j][c][patch - slab_rows:])], axis=0)
                    for c in range(2)
                ]
                q.append((qr, qi))
                waves.append((pr * qr - pi * qi, pr * qi + pi * qr))
            mid = [times_table(jnp.concatenate(w, axis=1), forward) for w in waves]
            spec = [table_times(backward, jnp.concatenate([m[:, :patch], m[:, patch:]], axis=0)) for m in mid]
            fixed = []
            for p, s in zip(ps, spec):
                sr, si = s[:patch], s[patch:]
                factor = amp[p] / jnp.maximum(jnp.sqrt(sr * sr + si * si), 0.5)
                fixed.append(jnp.concatenate([factor * sr, factor * si], axis=1))
            mid = [times_table(f, backward) for f in fixed]
            back = [table_times(forward, jnp.concatenate([m[:, :patch], m[:, patch:]], axis=0)) for m in mid]
            sums = [part[k] for k in range(3)]
            for j, p in enumerate(ps):
                qr, qi = q[j]
                dr = back[j][:patch] - waves[j][0]
                di = back[j][patch:] - waves[j][1]
                grad[p, 0] = pr * dr + pi * di
                grad[p, 1] = pr * di - pi * dr
                grad_copy(p, 0).start()
                grad_copy(p, 1).start()
                sums[0] += qr * dr + qi * di
                sums[1] += qr * di - qi * dr
                sums[2] += qr * qr + qi * qi
            for k in range(3):
                part[k] = sums[k]
            return 0

        lax.fori_loop(0, per_device // PAIR, some_patches, 0)

        hear(2)
        lot = z * 4 + y
        mine_half = pl.ds(pl.multiple_of(core * half, half), half)
        half_copy = remote(part.at[:, pl.ds(pl.multiple_of((1 - core) * half, half), half), :], half_in,
                           group_send.at[0], group_recv.at[0], plane_peer(0, 1))
        half_copy.start()

        def spread_grad(k, p, source):
            table, owner, _ = tables[k]
            r, column = place(table, owner, p)
            for c in range(2):
                spread[k * per_device + p, c] = pltpu.roll(
                    source(c)[pl.ds(half - r, half), :], column & (LANES - 1), 1)

        def spread_own(p, _):
            spread_grad(0, p, lambda c: grad.at[p, c])
            return 0

        lax.fori_loop(0, per_device, spread_own, 0)

        half_copy.wait()
        total = part[:, mine_half, :] + half_in[...]
        for k in range(plane):
            lots[k] = total[:, k * share:(k + 1) * share, :]

        def part_copy(d):
            theirs = ((z + (d >> 2)) & 3) * 4 + ((y + (d & 3)) & 3)
            return remote(lots.at[theirs], parts.at[d], group_send.at[1], group_recv.at[1], plane_peer(d))

        for d in range(1, plane):
            part_copy(d).start()

        def spread_near(i, _):
            together(rims.at[:, pl.ds(i * PAIR, PAIR)], grad_send.at[0], grad_recv.at[i]).wait_recv()
            for j in range(PAIR):
                p = i * PAIR + j
                for c in range(2):
                    pad_up[c, pl.ds(0, half), :] = rims[0, p, c]
                    pad_down[c, pl.ds(half, half), :] = rims[1, p, c]
                spread_grad(1, p, lambda c: pad_up.at[c])
                spread_grad(2, p, lambda c: pad_down.at[c])
            return 0

        lax.fori_loop(0, per_device // PAIR, spread_near, 0)

        all_parts = together(parts.at[pl.ds(1, plane - 1)], group_send.at[1], group_recv.at[1])
        all_merges = together(merges.at[pl.ds(1, 3)], group_send.at[2], group_recv.at[2])
        all_shares = together(shares.at[pl.ds(0, 2 * plane - 1)], group_send.at[3], group_recv.at[3])

        all_parts.wait_recv()
        total = lots[lot]
        for d in range(1, plane):
            total += parts[d]
        merges[0] = total
        place_in_line = far * 2 + (side >> 1)

        def merge_copy(d):
            return remote(merges.at[0], merges.at[d], group_send.at[2], group_recv.at[2], line_peer(d))

        for d in range(1, 4):
            merge_copy(d).start()

        def update(b, _):
            total = [jnp.zeros((half, LANES), F32) for _ in range(2)]
            for k in range(3):
                for p in range(per_device):
                    inside = covers(b, k, p)
                    for c in range(2):
                        total[c] += jnp.where(inside, spread[k * per_device + p, c], 0.0)
            at = pl.ds(pl.multiple_of(b * LANES, LANES), LANES)
            for c in range(2):
                fresh[0, c, :, at] = field[c, b, pl.ds(half, band), :] + total[c] * inverse[b]
            return 0

        lax.fori_loop(0, blocks, update, 0)

        loads[3].wait()
        high, low = split(fresh[0, 1])
        both = jnp.concatenate([high, low], axis=0)
        tile = ramp.shape[2]
        for j in range(width // tile):
            rows = pl.ds(width - tile - j * tile, width)
            twice = dot(both, ramp[0, rows, :])
            piece = twice[:band] + (twice[band:] + dot(high, ramp[1, rows, :]))
            for a in range(angles):
                filt[a, :, pl.ds(j * tile, tile)] = piece[a * rows_each:(a + 1) * rows_each]

        def swap_copy(d):
            peer = angle_peer(d)
            return remote(filt.at[peer[0]], sino.at[d], swap_send.at[0], swap_recv.at[d >> 2], peer)

        for d in (4, 5, 7, 6, 1, 3, 2):
            swap_copy(d).start()
        sino[0] = filt[me_a]

        loads[4].wait()
        loads[5].wait()
        total_recon[...] = jnp.zeros(total_recon.shape, F32)

        def back(d, _):
            @pl.when(d == 1)
            def _():
                together(sino.at[pl.ds(1, 3)], swap_send.at[0], swap_recv.at[0]).wait_recv()

            @pl.when(d == 4)
            def _():
                together(sino.at[pl.ds(4, 4)], swap_send.at[0], swap_recv.at[1]).wait_recv()

            a = angle_source(d)
            rows = sino[d]
            rise = pltpu.roll(rows, width - 1, 1) - rows
            for depth in range(zwin):
                for b in range(blocks):
                    at = pl.ds(b * LANES, LANES)
                    k = jnp.broadcast_to(index[a, pl.ds(depth, 1), at], (rows_each, LANES))
                    w = jnp.broadcast_to(weight[a, pl.ds(depth, 1), at], (rows_each, LANES))
                    block = k >> 7
                    inside = k & (LANES - 1)
                    lower = jnp.zeros((rows_each, LANES), F32)
                    slope = jnp.zeros((rows_each, LANES), F32)
                    for s in range(blocks):
                        here = block == s
                        cut = slice(s * LANES, (s + 1) * LANES)
                        lower = jnp.where(here, pick(rows[:, cut], inside), lower)
                        slope = jnp.where(here, pick(rise[:, cut], inside), slope)
                    total_recon[depth, :, at] += lower + w * slope
            return 0

        slot = core * plane + lot
        share_copies = [
            remote(shares.at[slot], shares.at[slot], group_send.at[3], group_recv.at[3], plane_peer(d, other))
            for d in range(plane) for other in range(2) if d or other
        ]

        def step(d, _):
            @pl.when(d == EARLY)
            def _():
                all_merges.wait_recv()
                total = merges[place_in_line]
                for place in range(1, 4):
                    total += merges[place_in_line ^ place]
                bottom = total[2] + 1.0
                for c in range(2):
                    shares[slot, c] = probe[c, pl.ds(slot * share, share), :] + total[c] / bottom
                for copy in share_copies:
                    copy.start()

            return back(d, 0)

        lax.fori_loop(0, angles, step, 0)
        for depth in range(zwin):
            recon[depth] = total_recon[depth] * (math.pi / angles)

        all_edges.wait_send()
        together(halo, halo_send.at[0], halo_recv.at[0]).wait_send()
        together(rims, grad_send.at[0], grad_recv.at[0]).wait_send()
        together(sino.at[pl.ds(1, angles - 1)], swap_send.at[0], swap_recv.at[0]).wait_send()
        all_parts.wait_send()
        all_merges.wait_send()
        all_shares.wait_recv()
        for k in range(2 * plane):
            for c in range(2):
                probe_out[c, pl.ds(k * share, share), :] = shares[k, c]
        all_shares.wait_send()

    def scratch():
        vm = pltpu.VMEM
        dma = pltpu.SemaphoreType.DMA
        slab = (2, per_device, 2, slab_rows, LANES)
        rim = (2, per_device, 2, half, LANES)
        tile = 256
        return [
            pltpu.SMEM((1, 2, per_device), jnp.int32),
            pltpu.SMEM((2, 1, 2, per_device), jnp.int32),
            vm((per_device, patch, patch), F32),
            vm((2, patch, patch), F32),
            vm((2, blocks + 1, band + patch, LANES), F32),
            vm((2, blocks + 1, band + patch, LANES), F32),
            vm((angles, zwin, width), jnp.int32),
            vm((angles, zwin, width), F32),
            vm((4, 2 * patch, 2 * patch), BF16),
            vm((2, 2 * width - tile, tile), BF16),
            vm(slab, F32),
            vm(slab, F32),
            vm((per_device, 2, patch, LANES), F32),
            vm(rim, F32),
            vm((2, patch, LANES), F32),
            vm((2, patch, LANES), F32),
            vm((2 * patch, LANES), F32),
            vm((blocks, band, LANES), F32),
            vm((3 * per_device, 2, half, LANES), F32),
            vm((angles, rows_each, width), F32),
            vm((angles, rows_each, width), F32),
            vm((zwin, rows_each, width), F32),
            vm((3, patch, LANES), F32),
            vm((3, half, LANES), F32),
            vm((plane, 3, share, LANES), F32),
            vm((plane, 3, share, LANES), F32),
            vm((4, 3, share, LANES), F32),
            vm((2 * plane, 2, share, LANES), F32),
            dma((7,)),
            dma((1,)),
            pltpu.SemaphoreType.REGULAR((3,)),
            dma((2,)),
            dma((2,)),
            dma((1,)), dma((per_device // PAIR,)),
            dma((1,)), dma((per_device // PAIR,)),
            dma((1,)), dma((2,)),
            dma((4,)), dma((4,)),
        ]

    return kernel, scratch


def solution(mesh):
    angles, positions = mesh.shape["angle"], mesh.shape["pos"]

    def on_device(amplitude, offsets, probe_field, object_field, interp_index, interp_weight):
        band, width = object_field.shape[2:]
        patch = probe_field.shape[1]
        zwin = interp_index.shape[1]
        kernel, scratch = make_kernel(angles, positions, patch, band, offsets.shape[1], width, zwin)
        anywhere = pl.BlockSpec(memory_space=pl.ANY)
        in_hbm = pl.BlockSpec(memory_space=pltpu.HBM)
        in_vmem = pl.BlockSpec(memory_space=pltpu.VMEM)
        rows_each = band // angles
        ready = pl.pallas_call(
            kernel,
            name="ptycho",
            out_shape=(
                jax.ShapeDtypeStruct(object_field.shape, F32),
                jax.ShapeDtypeStruct(probe_field.shape, F32),
                jax.ShapeDtypeStruct((zwin, rows_each, width), F32),
            ),
            in_specs=[in_hbm] * 8,
            out_specs=(in_vmem,) * 3,
            scratch_shapes=scratch(),
            compiler_params=pltpu.CompilerParams(
                collective_id=0, has_side_effects=True, vmem_limit_bytes=32 * 1024 * 1024
            ),
        )(
            *(
                pltpu.with_memory_space_constraint(x, pltpu.HBM)
                for x in (
                    jnp.swapaxes(offsets, 1, 2), amplitude, probe_field, object_field, interp_index, interp_weight,
                    jnp.asarray(dft_constant(patch)), jnp.asarray(ramp_constant(width, 256)),
                )
            ),
        )
        return pl.pallas_call(
            put_out,
            name="put_out",
            out_shape=(
                jax.ShapeDtypeStruct(object_field.shape, F32),
                jax.ShapeDtypeStruct(probe_field.shape, F32),
                jax.ShapeDtypeStruct((1, rows_each, zwin, width), F32),
            ),
            in_specs=[in_vmem] * 3,
            out_specs=(anywhere,) * 3,
            scratch_shapes=[pltpu.SemaphoreType.DMA((2 + zwin,))],
            compiler_params=pltpu.CompilerParams(vmem_limit_bytes=4 * 1024 * 1024),
        )(*ready)

    return jax.shard_map(
        on_device,
        mesh=mesh,
        in_specs=(
            P("angle", "pos", None, None),
            P("angle", "pos", None),
            P(),
            P("angle", None, "pos", None),
            P(),
            P(),
        ),
        out_specs=(P("angle", None, "pos", None), P(), P("pos", "angle", None, None)),
        check_vma=False,
    )
```

```python
import math

import jax
import jax.numpy as jnp
import ml_dtypes
import numpy as np
from jax import lax
from jax.experimental import pallas as pl
from jax.experimental.pallas import tpu as pltpu
from jax.sharding import PartitionSpec as P

MESH = pl.DeviceIdType.MESH
F32 = jnp.float32
BF16 = jnp.bfloat16
LANES = 128
EARLY = 1
EDGE = 16
GROUPS = ((0,), (1,), (2, 3))


def halves(table):
    high = table.astype(np.float32).astype(ml_dtypes.bfloat16)
    low = (table.astype(np.float32) - high.astype(np.float32)).astype(ml_dtypes.bfloat16)
    return high, low


def dft_constant(n):
    ramp = np.arange(n)
    theta = (ramp[:, None] * ramp[None, :] % n) * (2.0 * math.pi / n)
    real, imag = np.cos(theta) / math.sqrt(n), -np.sin(theta) / math.sqrt(n)
    forward = np.block([[real, imag], [-imag, real]])
    return np.stack([*halves(forward), *halves(forward.T)])


def ramp_constant(length, tile):
    differ = (length - tile) + np.arange(tile)[None, :] - np.arange(2 * length - tile)[:, None]
    squared = np.maximum(differ.astype(np.float64) ** 2, 1.0)
    odd = np.where(differ % 2 != 0, -1.0 / (math.pi * math.pi * squared), 0.0)
    return np.stack(halves(np.where(differ == 0, 0.25, odd)))


def split(value):
    high = value.astype(BF16)
    return high, (value - high.astype(F32)).astype(BF16)


def dot(left, right):
    return jnp.dot(left, right, preferred_element_type=F32)


def times_table(value, table):
    n = value.shape[0]
    high, low = split(value)
    twice = dot(jnp.concatenate([high, low], axis=0), table[0])
    return twice[:n] + (twice[n:] + dot(high, table[1]))


def table_times(table, value):
    n = value.shape[1]
    high, low = split(value)
    twice = dot(table[0], jnp.concatenate([high, low], axis=1))
    return twice[:, :n] + (twice[:, n:] + dot(table[1], high))


def pick(values, lanes):
    return jnp.take_along_axis(values, lanes, axis=1, mode="promise_in_bounds")


def put_out(obj, probe, recon, obj_out, probe_out, recon_out, sems):
    copies = [
        pltpu.make_async_copy(obj, obj_out, sems.at[0]),
        pltpu.make_async_copy(probe, probe_out, sems.at[1]),
    ]
    for depth in range(recon.shape[0]):
        copies.append(pltpu.make_async_copy(recon.at[depth], recon_out.at[0, :, depth, :], sems.at[2 + depth]))
    for copy in copies:
        copy.start()
    for copy in copies:
        copy.wait()


def make_kernel(angles, positions, patch, band, per_device, width, zwin):
    blocks = width // LANES
    half = patch // 2
    slab_rows = half - EDGE
    rows_each = band // angles
    plane = 16
    share = patch // (2 * plane)

    def kernel(
        off_hbm, amp_hbm, probe_hbm, obj_hbm, index_hbm, weight_hbm, dft_hbm, ramp_hbm,
        fresh, probe_out, recon,
        off, off_near, amp, probe, field, wide, index, weight, dft, ramp,
        slabs, halo, grad, rims, pad_up, pad_down,
        power, inverse, spread, terms, filt, sino, total_recon,
        part, half_in, lots, parts, merges, shares,
        load_sem, field_sem, word, edge_sem, off_sem,
        halo_send, halo_recv, grad_send, grad_recv,
        swap_send, swap_recv, group_send, group_recv,
    ):
        me_a = lax.axis_index("angle")
        me_p = lax.axis_index("pos")
        down = lax.rem(me_p + 1, positions)
        up = lax.rem(me_p + positions - 1, positions)

        def remote(src, dst, send, recv, peer):
            return pltpu.make_async_remote_copy(
                src_ref=src, dst_ref=dst, send_sem=send, recv_sem=recv,
                device_id=peer, device_id_type=MESH,
            )

        field_loads = []
        for c in range(2):
            for b in range(blocks):
                field_loads.append(pltpu.make_async_copy(
                    obj_hbm.at[0, c, :, pl.ds(b * LANES, LANES)],
                    field.at[c, b, pl.ds(half, band), :], field_sem.at[0]))
        own_rows = field.at[:, pl.ds(0, blocks), pl.ds(half, band), :]
        field_load = pltpu.make_async_copy(own_rows, own_rows, field_sem.at[0])
        loads = [
            pltpu.make_async_copy(probe_hbm, probe, load_sem.at[0]),
            pltpu.make_async_copy(amp_hbm.at[0], amp, load_sem.at[1]),
            pltpu.make_async_copy(dft_hbm, dft, load_sem.at[2]),
            pltpu.make_async_copy(ramp_hbm, ramp, load_sem.at[3]),
            pltpu.make_async_copy(index_hbm, index, load_sem.at[4]),
            pltpu.make_async_copy(weight_hbm, weight, load_sem.at[5]),
        ]
        off_load = pltpu.make_async_copy(off_hbm, off, load_sem.at[6])
        for copy in [off_load] + field_loads + loads:
            copy.start()

        z, far = me_a >> 1, me_a & 1
        y, side = me_p >> 2, me_p & 3
        core = me_p & 1

        def plane_peer(d, other=0):
            return (((z + (d >> 2)) & 3) * 2 + far, ((y + (d & 3)) & 3) * 4 + (side ^ other))

        def line_peer(d):
            return (z * 2 + (far ^ (d >> 1)), y * 4 + (side ^ ((d & 1) * 2)))

        def angle_peer(d):
            return (((z + (d & 3)) & 3) * 2 + (far ^ (d >> 2)), me_p)

        def angle_source(d):
            return ((z - (d & 3)) & 3) * 2 + (far ^ (d >> 2))

        def signal(sem, peers):
            for peer in peers:
                pl.semaphore_signal(sem, inc=1, device_id=peer, device_id_type=MESH)

        near = [plane_peer(4), plane_peer(12), plane_peer(1), plane_peer(3), plane_peer(0, 1), line_peer(1), line_peer(2)]
        barrier = pltpu.get_barrier_semaphore()
        signal(barrier, [(me_a, up), (me_a, down)] + near)
        pl.semaphore_wait(barrier, 2 + len(near))

        jumps = near + [plane_peer(8), plane_peer(2)]

        def tell(k):
            signal(word.at[k], jumps if k else near)

        def hear(k):
            pl.semaphore_wait(word.at[k], len(jumps if k else near))

        def together(ref, send, recv):
            return remote(ref, ref, send, recv, plane_peer(1))

        off_copies = [
            remote(off, off_near.at[0], off_sem.at[0], off_sem.at[1], (me_a, down)),
            remote(off, off_near.at[1], off_sem.at[0], off_sem.at[1], (me_a, up)),
        ]
        off_load.wait()
        for copy in off_copies:
            copy.start()
        tell(0)

        field_load.wait()
        edge_copies = [
            remote(field.at[:, pl.ds(0, blocks), pl.ds(half + band - EDGE, EDGE), :],
                   wide.at[:, pl.ds(0, blocks), pl.ds(half - EDGE, EDGE), :],
                   edge_sem.at[0], edge_sem.at[1], (me_a, down)),
            remote(field.at[:, pl.ds(0, blocks), pl.ds(half, EDGE), :],
                   wide.at[:, pl.ds(0, blocks), pl.ds(half + band, EDGE), :],
                   edge_sem.at[0], edge_sem.at[1], (me_a, up)),
        ]
        all_edges = together(wide.at[:, pl.ds(0, blocks), pl.ds(0, 2 * EDGE), :], edge_sem.at[0], edge_sem.at[1])
        for copy in edge_copies:
            copy.start()
        for c in range(2):
            for b in range(blocks):
                wide[c, b, pl.ds(half, band), :] = field[c, b, pl.ds(half, band), :]

        lane = lax.broadcasted_iota(jnp.int32, (half, LANES), 1)
        slab_row = lax.broadcasted_iota(jnp.int32, (slab_rows, LANES), 0)

        loads[0].wait()
        pr = probe[0]
        pi = probe[1]
        power[pl.ds(0, half), :] = jnp.zeros((half, LANES), F32)
        power[pl.ds(half, patch), :] = pr * pr + pi * pi
        power[pl.ds(half + patch, half), :] = jnp.zeros((half, LANES), F32)
        for c in range(2):
            pad_up[c, pl.ds(half, half), :] = jnp.zeros((half, LANES), F32)
            pad_down[c, pl.ds(0, half), :] = jnp.zeros((half, LANES), F32)
        part[...] = jnp.zeros(part.shape, F32)

        def place(table, owner, p):
            first = table[0, p] - (owner * band - half)
            return jnp.minimum(jnp.maximum(first, 0), band), jnp.minimum(jnp.maximum(table[1, p], 0), width - patch)

        def window(source, c, first, count, column):
            block = column >> 7
            shift = column & (LANES - 1)
            back = (LANES - shift) & (LANES - 1)
            left = pltpu.roll(source[c, block, pl.ds(first, count), :], back, 1)
            right = pltpu.roll(source[c, block + 1, pl.ds(first, count), :], back, 1)
            lanes = lax.broadcasted_iota(jnp.int32, (count, LANES), 1)
            return jnp.where(lanes < LANES - shift, left, right)

        together(off_near, off_sem.at[0], off_sem.at[1]).wait()
        own_off, off_up, off_down = off.at[0], off_near.at[0, 0], off_near.at[1, 0]
        hear(0)
        tell(1)

        def halo_copy(g, p, which):
            if which == 0:
                return remote(slabs.at[0, p], halo.at[0, p], halo_send.at[0], halo_recv.at[g], (me_a, down))
            return remote(slabs.at[1, p], halo.at[1, p], halo_send.at[0], halo_recv.at[g], (me_a, up))

        for g, ps in enumerate(GROUPS):
            for p in ps:
                r, column = place(off_down, down, p)
                for c in range(2):
                    slabs[0, p, c] = window(field, c, half + r, slab_rows, column)
                halo_copy(g, p, 0).start()
                r, column = place(off_up, up, p)
                for c in range(2):
                    slabs[1, p, c] = window(field, c, r + EDGE, slab_rows, column)
                halo_copy(g, p, 1).start()

        tables = ((own_off, me_p, 2 * half), (off_up, up, 3 * half), (off_down, down, half))

        def spread_power(p, _):
            for k, (table, owner, base) in enumerate(tables):
                r, column = place(table, owner, p)
                spread[k * per_device + p, 0] = pltpu.roll(
                    power[pl.ds(base - r, half), :], column & (LANES - 1), 1)
            return 0

        lax.fori_loop(0, per_device, spread_power, 0)

        def covers(b, k, p):
            table, _, _ = tables[k]
            away = lane + (b * LANES - table[1, p])
            return (away >= 0) & (away < LANES)

        def weigh(b, _):
            total = jnp.ones((half, LANES), F32)
            for k in range(3):
                for p in range(per_device):
                    total += jnp.where(covers(b, k, p), spread[k * per_device + p, 0], 0.0)
            inverse[b] = 1.0 / total
            return 0

        lax.fori_loop(0, blocks, weigh, 0)

        hear(1)
        tell(2)
        all_edges.wait_recv()
        loads[1].wait()
        loads[2].wait()

        def grad_copy(g, p, which):
            if which == 0:
                return remote(grad.at[p, :, pl.ds(half, half), :], rims.at[0, p],
                              grad_send.at[0], grad_recv.at[g], (me_a, down))
            return remote(grad.at[p, :, pl.ds(0, half), :], rims.at[1, p],
                          grad_send.at[0], grad_recv.at[g], (me_a, up))

        def some_patches(g, ps):
            places = [place(own_off, me_p, p) for p in ps]
            own = [[window(wide, c, r, patch, column) for c in range(2)] for r, column in places]
            together(halo.at[:, pl.ds(ps[0], len(ps))], halo_send.at[0], halo_recv.at[g]).wait_recv()
            pr = probe[0]
            pi = probe[1]
            forward = (dft[0], dft[1])
            backward = (dft[2], dft[3])
            q, waves = [], []
            for j, p in enumerate(ps):
                above = slab_row < slab_rows - places[j][0]
                below = slab_row >= half - places[j][0]
                qr, qi = [
                    jnp.concatenate([
                        jnp.where(above, halo[0, p, c], own[j][c][:slab_rows]),
                        own[j][c][slab_rows:patch - slab_rows],
                        jnp.where(below, halo[1, p, c], own[j][c][patch - slab_rows:])], axis=0)
                    for c in range(2)
                ]
                q.append((qr, qi))
                waves.append((pr * qr - pi * qi, pr * qi + pi * qr))
            mid = [times_table(jnp.concatenate(w, axis=1), forward) for w in waves]
            spec = [table_times(backward, jnp.concatenate([m[:, :patch], m[:, patch:]], axis=0)) for m in mid]
            fixed = []
            for p, s in zip(ps, spec):
                sr, si = s[:patch], s[patch:]
                factor = amp[p] / jnp.maximum(jnp.sqrt(sr * sr + si * si), 0.5)
                fixed.append(jnp.concatenate([factor * sr, factor * si], axis=1))
            mid = [times_table(f, backward) for f in fixed]
            back = [table_times(forward, jnp.concatenate([m[:, :patch], m[:, patch:]], axis=0)) for m in mid]
            sums = [part[k] for k in range(3)]
            for j, p in enumerate(ps):
                qr, qi = q[j]
                dr = back[j][:patch] - waves[j][0]
                di = back[j][patch:] - waves[j][1]
                grad[p, 0] = pr * dr + pi * di
                grad[p, 1] = pr * di - pi * dr
                grad_copy(g, p, 0).start()
                grad_copy(g, p, 1).start()
                sums[0] += qr * dr + qi * di
                sums[1] += qr * di - qi * dr
                sums[2] += qr * qr + qi * qi
            for k in range(3):
                part[k] = sums[k]

        for g, ps in enumerate(GROUPS):
            some_patches(g, ps)

        hear(2)
        lot = z * 4 + y
        mine_half = pl.ds(pl.multiple_of(core * half, half), half)
        half_copy = remote(part.at[:, pl.ds(pl.multiple_of((1 - core) * half, half), half), :], half_in,
                           group_send.at[0], group_recv.at[0], plane_peer(0, 1))
        half_copy.start()

        def spread_grad(k, p, source):
            table, owner, _ = tables[k]
            r, column = place(table, owner, p)
            for c in range(2):
                spread[k * per_device + p, c] = pltpu.roll(
                    source(c)[pl.ds(half - r, half), :], column & (LANES - 1), 1)

        def spread_own(p, _):
            spread_grad(0, p, lambda c: grad.at[p, c])
            return 0

        lax.fori_loop(0, per_device, spread_own, 0)

        half_copy.wait()
        total = part[:, mine_half, :] + half_in[...]
        for k in range(plane):
            lots[k] = total[:, k * share:(k + 1) * share, :]

        def part_copy(d):
            theirs = ((z + (d >> 2)) & 3) * 4 + ((y + (d & 3)) & 3)
            return remote(lots.at[theirs], parts.at[d], group_send.at[1], group_recv.at[1], plane_peer(d))

        for d in range(1, plane):
            part_copy(d).start()

        def add_terms(keys, first=False, last=False):
            def body(b, _):
                total = [jnp.zeros((half, LANES), F32) if first else terms[c, b] for c in range(2)]
                for k, p in keys:
                    inside = covers(b, k, p)
                    for c in range(2):
                        total[c] += jnp.where(inside, spread[k * per_device + p, c], 0.0)
                at = pl.ds(pl.multiple_of(b * LANES, LANES), LANES)
                for c in range(2):
                    if last:
                        fresh[0, c, :, at] = field[c, b, pl.ds(half, band), :] + total[c] * inverse[b]
                    else:
                        terms[c, b] = total[c]
                return 0

            lax.fori_loop(0, blocks, body, 0)

        add_terms([(0, p) for p in range(per_device)], first=True)
        for g, ps in enumerate(GROUPS):
            together(rims.at[:, pl.ds(ps[0], len(ps))], grad_send.at[0], grad_recv.at[g]).wait_recv()
            for p in ps:
                for c in range(2):
                    pad_up[c, pl.ds(0, half), :] = rims[0, p, c]
                    pad_down[c, pl.ds(half, half), :] = rims[1, p, c]
                spread_grad(1, p, lambda c: pad_up.at[c])
                spread_grad(2, p, lambda c: pad_down.at[c])
            add_terms([(k, p) for p in ps for k in (1, 2)], last=g == len(GROUPS) - 1)

        loads[3].wait()
        high, low = split(fresh[0, 1])
        both = jnp.concatenate([high, low], axis=0)
        tile = ramp.shape[2]
        for j in range(width // tile):
            rows = pl.ds(width - tile - j * tile, width)
            twice = dot(both, ramp[0, rows, :])
            piece = twice[:band] + (twice[band:] + dot(high, ramp[1, rows, :]))
            for a in range(angles):
                filt[a, :, pl.ds(j * tile, tile)] = piece[a * rows_each:(a + 1) * rows_each]

        all_parts = together(parts.at[pl.ds(1, plane - 1)], group_send.at[1], group_recv.at[1])
        all_merges = together(merges.at[pl.ds(1, 3)], group_send.at[2], group_recv.at[2])
        all_shares = together(shares.at[pl.ds(0, 2 * plane - 1)], group_send.at[3], group_recv.at[3])

        all_parts.wait_recv()
        total = lots[lot]
        for d in range(1, plane):
            total += parts[d]
        merges[0] = total
        place_in_line = far * 2 + (side >> 1)

        def merge_copy(d):
            return remote(merges.at[0], merges.at[d], group_send.at[2], group_recv.at[2], line_peer(d))

        for d in range(1, 4):
            merge_copy(d).start()

        def swap_copy(d):
            peer = angle_peer(d)
            return remote(filt.at[peer[0]], sino.at[d], swap_send.at[0], swap_recv.at[max(d - 3, 0)], peer)

        for d in (4, 5, 7, 6, 1, 3, 2):
            swap_copy(d).start()
        sino[0] = filt[me_a]

        loads[4].wait()
        loads[5].wait()
        total_recon[...] = jnp.zeros(total_recon.shape, F32)

        def back(d, _):
            @pl.when(d == 1)
            def _():
                together(sino.at[pl.ds(1, 3)], swap_send.at[0], swap_recv.at[0]).wait_recv()

            @pl.when(d >= 4)
            def _():
                together(sino.at[d], swap_send.at[0], swap_recv.at[d - 3]).wait_recv()

            a = angle_source(d)
            rows = sino[d]
            rise = pltpu.roll(rows, width - 1, 1) - rows
            for depth in range(zwin):
                for b in range(blocks):
                    at = pl.ds(b * LANES, LANES)
                    k = jnp.broadcast_to(index[a, pl.ds(depth, 1), at], (rows_each, LANES))
                    w = jnp.broadcast_to(weight[a, pl.ds(depth, 1), at], (rows_each, LANES))
                    block = k >> 7
                    inside = k & (LANES - 1)
                    lower = jnp.zeros((rows_each, LANES), F32)
                    slope = jnp.zeros((rows_each, LANES), F32)
                    for s in range(blocks):
                        here = block == s
                        cut = slice(s * LANES, (s + 1) * LANES)
                        lower = jnp.where(here, pick(rows[:, cut], inside), lower)
                        slope = jnp.where(here, pick(rise[:, cut], inside), slope)
                    total_recon[depth, :, at] += lower + w * slope
            return 0

        slot = core * plane + lot
        share_copies = [
            remote(shares.at[slot], shares.at[slot], group_send.at[3], group_recv.at[3], plane_peer(d, other))
            for d in range(plane) for other in range(2) if d or other
        ]

        def step(d, _):
            @pl.when(d == EARLY)
            def _():
                all_merges.wait_recv()
                total = merges[place_in_line]
                for place in range(1, 4):
                    total += merges[place_in_line ^ place]
                bottom = total[2] + 1.0
                for c in range(2):
                    shares[slot, c] = probe[c, pl.ds(slot * share, share), :] + total[c] / bottom
                for copy in share_copies:
                    copy.start()

            return back(d, 0)

        lax.fori_loop(0, angles, step, 0)
        for depth in range(zwin):
            recon[depth] = total_recon[depth] * (math.pi / angles)

        all_edges.wait_send()
        together(halo, halo_send.at[0], halo_recv.at[0]).wait_send()
        together(rims, grad_send.at[0], grad_recv.at[0]).wait_send()
        together(sino.at[pl.ds(1, angles - 1)], swap_send.at[0], swap_recv.at[0]).wait_send()
        all_parts.wait_send()
        all_merges.wait_send()
        all_shares.wait_recv()
        for k in range(2 * plane):
            for c in range(2):
                probe_out[c, pl.ds(k * share, share), :] = shares[k, c]
        all_shares.wait_send()

    def scratch():
        vm = pltpu.VMEM
        dma = pltpu.SemaphoreType.DMA
        slab = (2, per_device, 2, slab_rows, LANES)
        rim = (2, per_device, 2, half, LANES)
        tile = 256
        return [
            pltpu.SMEM((1, 2, per_device), jnp.int32),
            pltpu.SMEM((2, 1, 2, per_device), jnp.int32),
            vm((per_device, patch, patch), F32),
            vm((2, patch, patch), F32),
            vm((2, blocks + 1, band + patch, LANES), F32),
            vm((2, blocks + 1, band + patch, LANES), F32),
            vm((angles, zwin, width), jnp.int32),
            vm((angles, zwin, width), F32),
            vm((4, 2 * patch, 2 * patch), BF16),
            vm((2, 2 * width - tile, tile), BF16),
            vm(slab, F32),
            vm(slab, F32),
            vm((per_device, 2, patch, LANES), F32),
            vm(rim, F32),
            vm((2, patch, LANES), F32),
            vm((2, patch, LANES), F32),
            vm((2 * patch, LANES), F32),
            vm((blocks, band, LANES), F32),
            vm((3 * per_device, 2, half, LANES), F32),
            vm((2, blocks, band, LANES), F32),
            vm((angles, rows_each, width), F32),
            vm((angles, rows_each, width), F32),
            vm((zwin, rows_each, width), F32),
            vm((3, patch, LANES), F32),
            vm((3, half, LANES), F32),
            vm((plane, 3, share, LANES), F32),
            vm((plane, 3, share, LANES), F32),
            vm((4, 3, share, LANES), F32),
            vm((2 * plane, 2, share, LANES), F32),
            dma((7,)),
            dma((1,)),
            pltpu.SemaphoreType.REGULAR((3,)),
            dma((2,)),
            dma((2,)),
            dma((1,)), dma((len(GROUPS),)),
            dma((1,)), dma((len(GROUPS),)),
            dma((1,)), dma((5,)),
            dma((4,)), dma((4,)),
        ]

    return kernel, scratch


def solution(mesh):
    angles, positions = mesh.shape["angle"], mesh.shape["pos"]

    def on_device(amplitude, offsets, probe_field, object_field, interp_index, interp_weight):
        band, width = object_field.shape[2:]
        patch = probe_field.shape[1]
        zwin = interp_index.shape[1]
        kernel, scratch = make_kernel(angles, positions, patch, band, offsets.shape[1], width, zwin)
        anywhere = pl.BlockSpec(memory_space=pl.ANY)
        in_hbm = pl.BlockSpec(memory_space=pltpu.HBM)
        in_vmem = pl.BlockSpec(memory_space=pltpu.VMEM)
        rows_each = band // angles
        ready = pl.pallas_call(
            kernel,
            name="ptycho",
            out_shape=(
                jax.ShapeDtypeStruct(object_field.shape, F32),
                jax.ShapeDtypeStruct(probe_field.shape, F32),
                jax.ShapeDtypeStruct((zwin, rows_each, width), F32),
            ),
            in_specs=[in_hbm] * 8,
            out_specs=(in_vmem,) * 3,
            scratch_shapes=scratch(),
            compiler_params=pltpu.CompilerParams(
                collective_id=0, has_side_effects=True, vmem_limit_bytes=32 * 1024 * 1024
            ),
        )(
            *(
                pltpu.with_memory_space_constraint(x, pltpu.HBM)
                for x in (
                    jnp.swapaxes(offsets, 1, 2), amplitude, probe_field, object_field, interp_index, interp_weight,
                    jnp.asarray(dft_constant(patch)), jnp.asarray(ramp_constant(width, 256)),
                )
            ),
        )
        return pl.pallas_call(
            put_out,
            name="put_out",
            out_shape=(
                jax.ShapeDtypeStruct(object_field.shape, F32),
                jax.ShapeDtypeStruct(probe_field.shape, F32),
                jax.ShapeDtypeStruct((1, rows_each, zwin, width), F32),
            ),
            in_specs=[in_vmem] * 3,
            out_specs=(anywhere,) * 3,
            scratch_shapes=[pltpu.SemaphoreType.DMA((2 + zwin,))],
            compiler_params=pltpu.CompilerParams(vmem_limit_bytes=4 * 1024 * 1024),
        )(*ready)

    return jax.shard_map(
        on_device,
        mesh=mesh,
        in_specs=(
            P("angle", "pos", None, None),
            P("angle", "pos", None),
            P(),
            P("angle", None, "pos", None),
            P(),
            P(),
        ),
        out_specs=(P("angle", None, "pos", None), P(), P("pos", "angle", None, None)),
        check_vma=False,
    )
```

```python
import math

import jax
import jax.numpy as jnp
import ml_dtypes
import numpy as np
from jax import lax
from jax.experimental import pallas as pl
from jax.experimental.pallas import tpu as pltpu
from jax.sharding import PartitionSpec as P

MESH = pl.DeviceIdType.MESH
F32 = jnp.float32
BF16 = jnp.bfloat16
LANES = 128
EDGE = 16
GROUPS = ((0,), (1,), (2, 3))


def halves(table):
    high = table.astype(np.float32).astype(ml_dtypes.bfloat16)
    low = (table.astype(np.float32) - high.astype(np.float32)).astype(ml_dtypes.bfloat16)
    return high, low


def dft_constant(n):
    ramp = np.arange(n)
    theta = (ramp[:, None] * ramp[None, :] % n) * (2.0 * math.pi / n)
    real, imag = np.cos(theta) / math.sqrt(n), -np.sin(theta) / math.sqrt(n)
    forward = np.block([[real, imag], [-imag, real]])
    return np.stack([*halves(forward), *halves(forward.T)])


def ramp_constant(length, tile):
    differ = (length - tile) + np.arange(tile)[None, :] - np.arange(2 * length - tile)[:, None]
    squared = np.maximum(differ.astype(np.float64) ** 2, 1.0)
    odd = np.where(differ % 2 != 0, -1.0 / (math.pi * math.pi * squared), 0.0)
    return np.stack(halves(np.where(differ == 0, 0.25, odd)))


def split(value):
    high = value.astype(BF16)
    return high, (value - high.astype(F32)).astype(BF16)


def dot(left, right):
    return jnp.dot(left, right, preferred_element_type=F32)


def times_table(value, table):
    n = value.shape[0]
    high, low = split(value)
    twice = dot(jnp.concatenate([high, low], axis=0), table[0])
    return twice[:n] + (twice[n:] + dot(high, table[1]))


def table_times(table, value):
    n = value.shape[1]
    high, low = split(value)
    twice = dot(table[0], jnp.concatenate([high, low], axis=1))
    return twice[:, :n] + (twice[:, n:] + dot(table[1], high))


def pick(values, lanes):
    return jnp.take_along_axis(values, lanes, axis=1, mode="promise_in_bounds")


def put_out(obj, probe, recon, obj_out, probe_out, recon_out, sems):
    copies = [
        pltpu.make_async_copy(obj, obj_out, sems.at[0]),
        pltpu.make_async_copy(probe, probe_out, sems.at[1]),
    ]
    for depth in range(recon.shape[0]):
        copies.append(pltpu.make_async_copy(recon.at[depth], recon_out.at[0, :, depth, :], sems.at[2 + depth]))
    for copy in copies:
        copy.start()
    for copy in copies:
        copy.wait()


def make_kernel(angles, positions, patch, band, per_device, width, zwin):
    blocks = width // LANES
    half = patch // 2
    slab_rows = half - EDGE
    rows_each = band // angles
    plane = 16
    share = patch // (2 * plane)

    def kernel(
        off_hbm, amp_hbm, probe_hbm, obj_hbm, index_hbm, weight_hbm, dft_hbm, ramp_hbm,
        fresh, probe_out, recon,
        off, off_near, amp, probe, field, wide, index, weight, dft, ramp,
        slabs, halo, grad, rims, pad_up, pad_down,
        power, inverse, spread, terms, filt, sino, total_recon,
        part, half_in, lots, parts, merges, shares,
        load_sem, field_sem, word, edge_sem, off_sem,
        halo_send, halo_recv, grad_send, grad_recv,
        swap_send, swap_recv, group_send, group_recv,
    ):
        me_a = lax.axis_index("angle")
        me_p = lax.axis_index("pos")
        down = lax.rem(me_p + 1, positions)
        up = lax.rem(me_p + positions - 1, positions)

        def remote(src, dst, send, recv, peer):
            return pltpu.make_async_remote_copy(
                src_ref=src, dst_ref=dst, send_sem=send, recv_sem=recv,
                device_id=peer, device_id_type=MESH,
            )

        field_loads = []
        for c in range(2):
            for b in range(blocks):
                field_loads.append(pltpu.make_async_copy(
                    obj_hbm.at[0, c, :, pl.ds(b * LANES, LANES)],
                    field.at[c, b, pl.ds(half, band), :], field_sem.at[0]))
        own_rows = field.at[:, pl.ds(0, blocks), pl.ds(half, band), :]
        field_load = pltpu.make_async_copy(own_rows, own_rows, field_sem.at[0])
        loads = [
            pltpu.make_async_copy(probe_hbm, probe, load_sem.at[0]),
            pltpu.make_async_copy(amp_hbm.at[0], amp, load_sem.at[1]),
            pltpu.make_async_copy(dft_hbm, dft, load_sem.at[2]),
            pltpu.make_async_copy(ramp_hbm, ramp, load_sem.at[3]),
            pltpu.make_async_copy(index_hbm, index, load_sem.at[4]),
            pltpu.make_async_copy(weight_hbm, weight, load_sem.at[5]),
        ]
        off_load = pltpu.make_async_copy(off_hbm, off, load_sem.at[6])
        for copy in [off_load] + field_loads + loads:
            copy.start()

        z, far = me_a >> 1, me_a & 1
        y, side = me_p >> 2, me_p & 3
        core = me_p & 1

        def plane_peer(d, other=0):
            return (((z + (d >> 2)) & 3) * 2 + far, ((y + (d & 3)) & 3) * 4 + (side ^ other))

        def line_peer(d):
            return (z * 2 + (far ^ (d >> 1)), y * 4 + (side ^ ((d & 1) * 2)))

        def angle_peer(d):
            return (((z + (d & 3)) & 3) * 2 + (far ^ (d >> 2)), me_p)

        def angle_source(d):
            return ((z - (d & 3)) & 3) * 2 + (far ^ (d >> 2))

        def signal(sem, peers):
            for peer in peers:
                pl.semaphore_signal(sem, inc=1, device_id=peer, device_id_type=MESH)

        near = [plane_peer(4), plane_peer(12), plane_peer(1), plane_peer(3), plane_peer(0, 1), line_peer(1), line_peer(2)]
        barrier = pltpu.get_barrier_semaphore()
        signal(barrier, [(me_a, up), (me_a, down)] + near)
        pl.semaphore_wait(barrier, 2 + len(near))

        jumps = near + [plane_peer(8), plane_peer(2)]

        def tell(k):
            signal(word.at[k], jumps if k else near)

        def hear(k):
            pl.semaphore_wait(word.at[k], len(jumps if k else near))

        def together(ref, send, recv):
            return remote(ref, ref, send, recv, plane_peer(1))

        off_copies = [
            remote(off, off_near.at[0], off_sem.at[0], off_sem.at[1], (me_a, down)),
            remote(off, off_near.at[1], off_sem.at[0], off_sem.at[1], (me_a, up)),
        ]
        off_load.wait()
        for copy in off_copies:
            copy.start()
        tell(0)

        field_load.wait()
        edge_copies = [
            remote(field.at[:, pl.ds(0, blocks), pl.ds(half + band - EDGE, EDGE), :],
                   wide.at[:, pl.ds(0, blocks), pl.ds(half - EDGE, EDGE), :],
                   edge_sem.at[0], edge_sem.at[1], (me_a, down)),
            remote(field.at[:, pl.ds(0, blocks), pl.ds(half, EDGE), :],
                   wide.at[:, pl.ds(0, blocks), pl.ds(half + band, EDGE), :],
                   edge_sem.at[0], edge_sem.at[1], (me_a, up)),
        ]
        all_edges = together(wide.at[:, pl.ds(0, blocks), pl.ds(0, 2 * EDGE), :], edge_sem.at[0], edge_sem.at[1])
        for copy in edge_copies:
            copy.start()
        for c in range(2):
            for b in range(blocks):
                wide[c, b, pl.ds(half, band), :] = field[c, b, pl.ds(half, band), :]

        lane = lax.broadcasted_iota(jnp.int32, (half, LANES), 1)
        slab_row = lax.broadcasted_iota(jnp.int32, (slab_rows, LANES), 0)

        loads[0].wait()
        pr = probe[0]
        pi = probe[1]
        power[pl.ds(0, half), :] = jnp.zeros((half, LANES), F32)
        power[pl.ds(half, patch), :] = pr * pr + pi * pi
        power[pl.ds(half + patch, half), :] = jnp.zeros((half, LANES), F32)
        for c in range(2):
            pad_up[c, pl.ds(half, half), :] = jnp.zeros((half, LANES), F32)
            pad_down[c, pl.ds(0, half), :] = jnp.zeros((half, LANES), F32)
        part[...] = jnp.zeros(part.shape, F32)

        def place(table, owner, p):
            first = table[0, p] - (owner * band - half)
            return jnp.minimum(jnp.maximum(first, 0), band), jnp.minimum(jnp.maximum(table[1, p], 0), width - patch)

        def window(source, c, first, count, column):
            block = column >> 7
            shift = column & (LANES - 1)
            back = (LANES - shift) & (LANES - 1)
            left = pltpu.roll(source[c, block, pl.ds(first, count), :], back, 1)
            right = pltpu.roll(source[c, block + 1, pl.ds(first, count), :], back, 1)
            lanes = lax.broadcasted_iota(jnp.int32, (count, LANES), 1)
            return jnp.where(lanes < LANES - shift, left, right)

        together(off_near, off_sem.at[0], off_sem.at[1]).wait()
        own_off, off_up, off_down = off.at[0], off_near.at[0, 0], off_near.at[1, 0]
        hear(0)
        tell(1)

        def halo_copy(g, p, which):
            if which == 0:
                return remote(slabs.at[0, p], halo.at[0, p], halo_send.at[0], halo_recv.at[g], (me_a, down))
            return remote(slabs.at[1, p], halo.at[1, p], halo_send.at[0], halo_recv.at[g], (me_a, up))

        for g, ps in enumerate(GROUPS):
            for p in ps:
                r, column = place(off_down, down, p)
                for c in range(2):
                    slabs[0, p, c] = window(field, c, half + r, slab_rows, column)
                halo_copy(g, p, 0).start()
                r, column = place(off_up, up, p)
                for c in range(2):
                    slabs[1, p, c] = window(field, c, r + EDGE, slab_rows, column)
                halo_copy(g, p, 1).start()

        tables = ((own_off, me_p, 2 * half), (off_up, up, 3 * half), (off_down, down, half))

        def spread_power(p, _):
            for k, (table, owner, base) in enumerate(tables):
                r, column = place(table, owner, p)
                spread[k * per_device + p, 0] = pltpu.roll(
                    power[pl.ds(base - r, half), :], column & (LANES - 1), 1)
            return 0

        lax.fori_loop(0, per_device, spread_power, 0)

        def covers(b, k, p):
            table, _, _ = tables[k]
            away = lane + (b * LANES - table[1, p])
            return (away >= 0) & (away < LANES)

        def weigh(b, _):
            total = jnp.ones((half, LANES), F32)
            for k in range(3):
                for p in range(per_device):
                    total += jnp.where(covers(b, k, p), spread[k * per_device + p, 0], 0.0)
            inverse[b] = 1.0 / total
            return 0

        lax.fori_loop(0, blocks, weigh, 0)

        hear(1)
        tell(2)
        all_edges.wait_recv()
        loads[1].wait()
        loads[2].wait()

        def grad_copy(g, p, which):
            if which == 0:
                return remote(grad.at[p, :, pl.ds(half, half), :], rims.at[0, p],
                              grad_send.at[0], grad_recv.at[g], (me_a, down))
            return remote(grad.at[p, :, pl.ds(0, half), :], rims.at[1, p],
                          grad_send.at[0], grad_recv.at[g], (me_a, up))

        def some_patches(g, ps):
            places = [place(own_off, me_p, p) for p in ps]
            own = [[window(wide, c, r, patch, column) for c in range(2)] for r, column in places]
            together(halo.at[:, pl.ds(ps[0], len(ps))], halo_send.at[0], halo_recv.at[g]).wait_recv()
            pr = probe[0]
            pi = probe[1]
            forward = (dft[0], dft[1])
            backward = (dft[2], dft[3])
            q, waves = [], []
            for j, p in enumerate(ps):
                above = slab_row < slab_rows - places[j][0]
                below = slab_row >= half - places[j][0]
                qr, qi = [
                    jnp.concatenate([
                        jnp.where(above, halo[0, p, c], own[j][c][:slab_rows]),
                        own[j][c][slab_rows:patch - slab_rows],
                        jnp.where(below, halo[1, p, c], own[j][c][patch - slab_rows:])], axis=0)
                    for c in range(2)
                ]
                q.append((qr, qi))
                waves.append((pr * qr - pi * qi, pr * qi + pi * qr))
            mid = [times_table(jnp.concatenate(w, axis=1), forward) for w in waves]
            spec = [table_times(backward, jnp.concatenate([m[:, :patch], m[:, patch:]], axis=0)) for m in mid]
            fixed = []
            for p, s in zip(ps, spec):
                sr, si = s[:patch], s[patch:]
                factor = amp[p] / jnp.maximum(jnp.sqrt(sr * sr + si * si), 0.5)
                fixed.append(jnp.concatenate([factor * sr, factor * si], axis=1))
            mid = [times_table(f, backward) for f in fixed]
            back = [table_times(forward, jnp.concatenate([m[:, :patch], m[:, patch:]], axis=0)) for m in mid]
            sums = [part[k] for k in range(3)]
            for j, p in enumerate(ps):
                qr, qi = q[j]
                dr = back[j][:patch] - waves[j][0]
                di = back[j][patch:] - waves[j][1]
                grad[p, 0] = pr * dr + pi * di
                grad[p, 1] = pr * di - pi * dr
                grad_copy(g, p, 0).start()
                grad_copy(g, p, 1).start()
                sums[0] += qr * dr + qi * di
                sums[1] += qr * di - qi * dr
                sums[2] += qr * qr + qi * qi
            for k in range(3):
                part[k] = sums[k]

        for g, ps in enumerate(GROUPS):
            some_patches(g, ps)

        hear(2)
        lot = z * 4 + y
        mine_half = pl.ds(pl.multiple_of(core * half, half), half)
        half_copy = remote(part.at[:, pl.ds(pl.multiple_of((1 - core) * half, half), half), :], half_in,
                           group_send.at[0], group_recv.at[0], plane_peer(0, 1))
        half_copy.start()

        def spread_grad(k, p, source):
            table, owner, _ = tables[k]
            r, column = place(table, owner, p)
            for c in range(2):
                spread[k * per_device + p, c] = pltpu.roll(
                    source(c)[pl.ds(half - r, half), :], column & (LANES - 1), 1)

        def spread_own(p, _):
            spread_grad(0, p, lambda c: grad.at[p, c])
            return 0

        lax.fori_loop(0, per_device, spread_own, 0)

        half_copy.wait()
        total = part[:, mine_half, :] + half_in[...]
        for k in range(plane):
            lots[k] = total[:, k * share:(k + 1) * share, :]

        def part_copy(d):
            theirs = ((z + (d >> 2)) & 3) * 4 + ((y + (d & 3)) & 3)
            return remote(lots.at[theirs], parts.at[d], group_send.at[1], group_recv.at[1], plane_peer(d))

        for d in range(1, plane):
            part_copy(d).start()

        def add_terms(keys, first=False, last=False):
            def body(b, _):
                total = [jnp.zeros((half, LANES), F32) if first else terms[c, b] for c in range(2)]
                for k, p in keys:
                    inside = covers(b, k, p)
                    for c in range(2):
                        total[c] += jnp.where(inside, spread[k * per_device + p, c], 0.0)
                at = pl.ds(pl.multiple_of(b * LANES, LANES), LANES)
                for c in range(2):
                    if last:
                        fresh[0, c, :, at] = field[c, b, pl.ds(half, band), :] + total[c] * inverse[b]
                    else:
                        terms[c, b] = total[c]
                return 0

            lax.fori_loop(0, blocks, body, 0)

        add_terms([(0, p) for p in range(per_device)], first=True)
        all_parts = together(parts.at[pl.ds(1, plane - 1)], group_send.at[1], group_recv.at[1])
        all_merges = together(merges.at[pl.ds(1, 3)], group_send.at[2], group_recv.at[2])
        all_shares = together(shares.at[pl.ds(0, 2 * plane - 1)], group_send.at[3], group_recv.at[3])
        place_in_line = far * 2 + (side >> 1)

        def merge_copy(d):
            return remote(merges.at[0], merges.at[d], group_send.at[2], group_recv.at[2], line_peer(d))

        def take_parts():
            all_parts.wait_recv()
            total = lots[lot]
            for d in range(1, plane):
                total += parts[d]
            merges[0] = total
            for d in range(1, 4):
                merge_copy(d).start()

        for g, ps in enumerate(GROUPS):
            if g == len(GROUPS) - 1:
                take_parts()
            together(rims.at[:, pl.ds(ps[0], len(ps))], grad_send.at[0], grad_recv.at[g]).wait_recv()
            for p in ps:
                for c in range(2):
                    pad_up[c, pl.ds(0, half), :] = rims[0, p, c]
                    pad_down[c, pl.ds(half, half), :] = rims[1, p, c]
                spread_grad(1, p, lambda c: pad_up.at[c])
                spread_grad(2, p, lambda c: pad_down.at[c])
            add_terms([(k, p) for p in ps for k in (1, 2)], last=g == len(GROUPS) - 1)

        loads[3].wait()
        high, low = split(fresh[0, 1])
        both = jnp.concatenate([high, low], axis=0)
        tile = ramp.shape[2]
        for j in range(width // tile):
            rows = pl.ds(width - tile - j * tile, width)
            twice = dot(both, ramp[0, rows, :])
            piece = twice[:band] + (twice[band:] + dot(high, ramp[1, rows, :]))
            for a in range(angles):
                filt[a, :, pl.ds(j * tile, tile)] = piece[a * rows_each:(a + 1) * rows_each]

        def swap_copy(d):
            peer = angle_peer(d)
            return remote(filt.at[peer[0]], sino.at[d], swap_send.at[0], swap_recv.at[max(d - 3, 0)], peer)

        for d in (4, 5, 7, 6, 1, 3, 2):
            swap_copy(d).start()

        slot = core * plane + lot
        share_copies = [
            remote(shares.at[slot], shares.at[slot], group_send.at[3], group_recv.at[3], plane_peer(d, other))
            for d in range(plane) for other in range(2) if d or other
        ]

        all_merges.wait_recv()
        total = merges[place_in_line]
        for other in range(1, 4):
            total += merges[place_in_line ^ other]
        bottom = total[2] + 1.0
        for c in range(2):
            shares[slot, c] = probe[c, pl.ds(slot * share, share), :] + total[c] / bottom
        for copy in share_copies:
            copy.start()

        sino[0] = filt[me_a]

        loads[4].wait()
        loads[5].wait()
        total_recon[...] = jnp.zeros(total_recon.shape, F32)

        def back(d, _):
            @pl.when(d == 1)
            def _():
                together(sino.at[pl.ds(1, 3)], swap_send.at[0], swap_recv.at[0]).wait_recv()

            @pl.when(d >= 4)
            def _():
                together(sino.at[d], swap_send.at[0], swap_recv.at[d - 3]).wait_recv()

            a = angle_source(d)
            rows = sino[d]
            rise = pltpu.roll(rows, width - 1, 1) - rows
            for depth in range(zwin):
                for b in range(blocks):
                    at = pl.ds(b * LANES, LANES)
                    k = jnp.broadcast_to(index[a, pl.ds(depth, 1), at], (rows_each, LANES))
                    w = jnp.broadcast_to(weight[a, pl.ds(depth, 1), at], (rows_each, LANES))
                    block = k >> 7
                    inside = k & (LANES - 1)
                    lower = jnp.zeros((rows_each, LANES), F32)
                    slope = jnp.zeros((rows_each, LANES), F32)
                    for s in range(blocks):
                        here = block == s
                        cut = slice(s * LANES, (s + 1) * LANES)
                        lower = jnp.where(here, pick(rows[:, cut], inside), lower)
                        slope = jnp.where(here, pick(rise[:, cut], inside), slope)
                    total_recon[depth, :, at] += lower + w * slope
            return 0

        lax.fori_loop(0, angles, back, 0)
        for depth in range(zwin):
            recon[depth] = total_recon[depth] * (math.pi / angles)

        all_edges.wait_send()
        together(halo, halo_send.at[0], halo_recv.at[0]).wait_send()
        together(rims, grad_send.at[0], grad_recv.at[0]).wait_send()
        together(sino.at[pl.ds(1, angles - 1)], swap_send.at[0], swap_recv.at[0]).wait_send()
        all_parts.wait_send()
        all_merges.wait_send()
        all_shares.wait_recv()
        for k in range(2 * plane):
            for c in range(2):
                probe_out[c, pl.ds(k * share, share), :] = shares[k, c]
        all_shares.wait_send()

    def scratch():
        vm = pltpu.VMEM
        dma = pltpu.SemaphoreType.DMA
        slab = (2, per_device, 2, slab_rows, LANES)
        rim = (2, per_device, 2, half, LANES)
        tile = 256
        return [
            pltpu.SMEM((1, 2, per_device), jnp.int32),
            pltpu.SMEM((2, 1, 2, per_device), jnp.int32),
            vm((per_device, patch, patch), F32),
            vm((2, patch, patch), F32),
            vm((2, blocks + 1, band + patch, LANES), F32),
            vm((2, blocks + 1, band + patch, LANES), F32),
            vm((angles, zwin, width), jnp.int32),
            vm((angles, zwin, width), F32),
            vm((4, 2 * patch, 2 * patch), BF16),
            vm((2, 2 * width - tile, tile), BF16),
            vm(slab, F32),
            vm(slab, F32),
            vm((per_device, 2, patch, LANES), F32),
            vm(rim, F32),
            vm((2, patch, LANES), F32),
            vm((2, patch, LANES), F32),
            vm((2 * patch, LANES), F32),
            vm((blocks, band, LANES), F32),
            vm((3 * per_device, 2, half, LANES), F32),
            vm((2, blocks, band, LANES), F32),
            vm((angles, rows_each, width), F32),
            vm((angles, rows_each, width), F32),
            vm((zwin, rows_each, width), F32),
            vm((3, patch, LANES), F32),
            vm((3, half, LANES), F32),
            vm((plane, 3, share, LANES), F32),
            vm((plane, 3, share, LANES), F32),
            vm((4, 3, share, LANES), F32),
            vm((2 * plane, 2, share, LANES), F32),
            dma((7,)),
            dma((1,)),
            pltpu.SemaphoreType.REGULAR((3,)),
            dma((2,)),
            dma((2,)),
            dma((1,)), dma((len(GROUPS),)),
            dma((1,)), dma((len(GROUPS),)),
            dma((1,)), dma((5,)),
            dma((4,)), dma((4,)),
        ]

    return kernel, scratch


def solution(mesh):
    angles, positions = mesh.shape["angle"], mesh.shape["pos"]

    def on_device(amplitude, offsets, probe_field, object_field, interp_index, interp_weight):
        band, width = object_field.shape[2:]
        patch = probe_field.shape[1]
        zwin = interp_index.shape[1]
        kernel, scratch = make_kernel(angles, positions, patch, band, offsets.shape[1], width, zwin)
        anywhere = pl.BlockSpec(memory_space=pl.ANY)
        in_hbm = pl.BlockSpec(memory_space=pltpu.HBM)
        in_vmem = pl.BlockSpec(memory_space=pltpu.VMEM)
        rows_each = band // angles
        ready = pl.pallas_call(
            kernel,
            name="ptycho",
            out_shape=(
                jax.ShapeDtypeStruct(object_field.shape, F32),
                jax.ShapeDtypeStruct(probe_field.shape, F32),
                jax.ShapeDtypeStruct((zwin, rows_each, width), F32),
            ),
            in_specs=[in_hbm] * 8,
            out_specs=(in_vmem,) * 3,
            scratch_shapes=scratch(),
            compiler_params=pltpu.CompilerParams(
                collective_id=0, has_side_effects=True, vmem_limit_bytes=32 * 1024 * 1024
            ),
        )(
            *(
                pltpu.with_memory_space_constraint(x, pltpu.HBM)
                for x in (
                    jnp.swapaxes(offsets, 1, 2), amplitude, probe_field, object_field, interp_index, interp_weight,
                    jnp.asarray(dft_constant(patch)), jnp.asarray(ramp_constant(width, 256)),
                )
            ),
        )
        return pl.pallas_call(
            put_out,
            name="put_out",
            out_shape=(
                jax.ShapeDtypeStruct(object_field.shape, F32),
                jax.ShapeDtypeStruct(probe_field.shape, F32),
                jax.ShapeDtypeStruct((1, rows_each, zwin, width), F32),
            ),
            in_specs=[in_vmem] * 3,
            out_specs=(anywhere,) * 3,
            scratch_shapes=[pltpu.SemaphoreType.DMA((2 + zwin,))],
            compiler_params=pltpu.CompilerParams(vmem_limit_bytes=4 * 1024 * 1024),
        )(*ready)

    return jax.shard_map(
        on_device,
        mesh=mesh,
        in_specs=(
            P("angle", "pos", None, None),
            P("angle", "pos", None),
            P(),
            P("angle", None, "pos", None),
            P(),
            P(),
        ),
        out_specs=(P("angle", None, "pos", None), P(), P("pos", "angle", None, None)),
        check_vma=False,
    )
```

```python
import math

import jax
import jax.numpy as jnp
import ml_dtypes
import numpy as np
from jax import lax
from jax.experimental import pallas as pl
from jax.experimental.pallas import tpu as pltpu
from jax.sharding import PartitionSpec as P

MESH = pl.DeviceIdType.MESH
F32 = jnp.float32
BF16 = jnp.bfloat16
LANES = 128
EDGE = 16
FAR_FIRST = (10, 6, 14, 9, 11, 8, 2, 5, 7, 13, 15, 4, 12, 1, 3, 0)
GROUPS = ((0,), (1,), (2, 3))


def halves(table):
    high = table.astype(np.float32).astype(ml_dtypes.bfloat16)
    low = (table.astype(np.float32) - high.astype(np.float32)).astype(ml_dtypes.bfloat16)
    return high, low


def dft_constant(n):
    ramp = np.arange(n)
    theta = (ramp[:, None] * ramp[None, :] % n) * (2.0 * math.pi / n)
    real, imag = np.cos(theta) / math.sqrt(n), -np.sin(theta) / math.sqrt(n)
    forward = np.block([[real, imag], [-imag, real]])
    return np.stack([*halves(forward), *halves(forward.T)])


def ramp_constant(length, tile):
    differ = (length - tile) + np.arange(tile)[None, :] - np.arange(2 * length - tile)[:, None]
    squared = np.maximum(differ.astype(np.float64) ** 2, 1.0)
    odd = np.where(differ % 2 != 0, -1.0 / (math.pi * math.pi * squared), 0.0)
    return np.stack(halves(np.where(differ == 0, 0.25, odd)))


def split(value):
    high = value.astype(BF16)
    return high, (value - high.astype(F32)).astype(BF16)


def dot(left, right):
    return jnp.dot(left, right, preferred_element_type=F32)


def times_table(value, table):
    n = value.shape[0]
    high, low = split(value)
    twice = dot(jnp.concatenate([high, low], axis=0), table[0])
    return twice[:n] + (twice[n:] + dot(high, table[1]))


def table_times(table, value):
    n = value.shape[1]
    high, low = split(value)
    twice = dot(table[0], jnp.concatenate([high, low], axis=1))
    return twice[:, :n] + (twice[:, n:] + dot(table[1], high))


def pick(values, lanes):
    return jnp.take_along_axis(values, lanes, axis=1, mode="promise_in_bounds")


def put_out(obj, probe, recon, obj_out, probe_out, recon_out, sems):
    copies = [
        pltpu.make_async_copy(obj, obj_out, sems.at[0]),
        pltpu.make_async_copy(probe, probe_out, sems.at[1]),
    ]
    for depth in range(recon.shape[0]):
        copies.append(pltpu.make_async_copy(recon.at[depth], recon_out.at[0, :, depth, :], sems.at[2 + depth]))
    for copy in copies:
        copy.start()
    for copy in copies:
        copy.wait()


def make_kernel(angles, positions, patch, band, per_device, width, zwin):
    blocks = width // LANES
    half = patch // 2
    slab_rows = half - EDGE
    rows_each = band // angles
    plane = 16
    share = patch // (2 * plane)

    def kernel(
        off_hbm, amp_hbm, probe_hbm, obj_hbm, index_hbm, weight_hbm, dft_hbm, ramp_hbm,
        fresh, probe_out, recon,
        off, off_near, amp, probe, field, wide, index, weight, dft, ramp,
        slabs, halo, grad, rims, pad_up, pad_down,
        power, inverse, spread, terms, filt, sino, total_recon,
        part, half_in, lots, parts, merges, shares,
        load_sem, field_sem, word, edge_sem, off_sem,
        halo_send, halo_recv, grad_send, grad_recv,
        swap_send, swap_recv, group_send, group_recv,
    ):
        me_a = lax.axis_index("angle")
        me_p = lax.axis_index("pos")
        down = lax.rem(me_p + 1, positions)
        up = lax.rem(me_p + positions - 1, positions)

        def remote(src, dst, send, recv, peer):
            return pltpu.make_async_remote_copy(
                src_ref=src, dst_ref=dst, send_sem=send, recv_sem=recv,
                device_id=peer, device_id_type=MESH,
            )

        field_loads = []
        for c in range(2):
            for b in range(blocks):
                field_loads.append(pltpu.make_async_copy(
                    obj_hbm.at[0, c, :, pl.ds(b * LANES, LANES)],
                    field.at[c, b, pl.ds(half, band), :], field_sem.at[0]))
        own_rows = field.at[:, pl.ds(0, blocks), pl.ds(half, band), :]
        field_load = pltpu.make_async_copy(own_rows, own_rows, field_sem.at[0])
        loads = [
            pltpu.make_async_copy(probe_hbm, probe, load_sem.at[0]),
            pltpu.make_async_copy(amp_hbm.at[0], amp, load_sem.at[1]),
            pltpu.make_async_copy(dft_hbm, dft, load_sem.at[2]),
            pltpu.make_async_copy(ramp_hbm, ramp, load_sem.at[3]),
            pltpu.make_async_copy(index_hbm, index, load_sem.at[4]),
            pltpu.make_async_copy(weight_hbm, weight, load_sem.at[5]),
        ]
        off_load = pltpu.make_async_copy(off_hbm, off, load_sem.at[6])
        for copy in [off_load] + field_loads + loads:
            copy.start()

        z, far = me_a >> 1, me_a & 1
        y, side = me_p >> 2, me_p & 3
        core = me_p & 1

        def plane_peer(d, other=0):
            return (((z + (d >> 2)) & 3) * 2 + far, ((y + (d & 3)) & 3) * 4 + (side ^ other))

        def line_peer(d):
            return (z * 2 + (far ^ (d >> 1)), y * 4 + (side ^ ((d & 1) * 2)))

        def angle_peer(d):
            return (((z + (d & 3)) & 3) * 2 + (far ^ (d >> 2)), me_p)

        def angle_source(d):
            return ((z - (d & 3)) & 3) * 2 + (far ^ (d >> 2))

        def signal(sem, peers):
            for peer in peers:
                pl.semaphore_signal(sem, inc=1, device_id=peer, device_id_type=MESH)

        near = [plane_peer(4), plane_peer(12), plane_peer(1), plane_peer(3), plane_peer(0, 1), line_peer(1), line_peer(2)]
        barrier = pltpu.get_barrier_semaphore()
        signal(barrier, [(me_a, up), (me_a, down)] + near)
        pl.semaphore_wait(barrier, 2 + len(near))

        jumps = near + [plane_peer(8), plane_peer(2)]

        def tell(k):
            signal(word.at[k], jumps if k else near)

        def hear(k):
            pl.semaphore_wait(word.at[k], len(jumps if k else near))

        def together(ref, send, recv):
            return remote(ref, ref, send, recv, plane_peer(1))

        off_copies = [
            remote(off, off_near.at[0], off_sem.at[0], off_sem.at[1], (me_a, down)),
            remote(off, off_near.at[1], off_sem.at[0], off_sem.at[1], (me_a, up)),
        ]
        off_load.wait()
        for copy in off_copies:
            copy.start()
        tell(0)

        field_load.wait()
        edge_copies = [
            remote(field.at[:, pl.ds(0, blocks), pl.ds(half + band - EDGE, EDGE), :],
                   wide.at[:, pl.ds(0, blocks), pl.ds(half - EDGE, EDGE), :],
                   edge_sem.at[0], edge_sem.at[1], (me_a, down)),
            remote(field.at[:, pl.ds(0, blocks), pl.ds(half, EDGE), :],
                   wide.at[:, pl.ds(0, blocks), pl.ds(half + band, EDGE), :],
                   edge_sem.at[0], edge_sem.at[1], (me_a, up)),
        ]
        all_edges = together(wide.at[:, pl.ds(0, blocks), pl.ds(0, 2 * EDGE), :], edge_sem.at[0], edge_sem.at[1])
        for copy in edge_copies:
            copy.start()
        for c in range(2):
            for b in range(blocks):
                wide[c, b, pl.ds(half, band), :] = field[c, b, pl.ds(half, band), :]

        lane = lax.broadcasted_iota(jnp.int32, (half, LANES), 1)
        slab_row = lax.broadcasted_iota(jnp.int32, (slab_rows, LANES), 0)

        loads[0].wait()
        pr = probe[0]
        pi = probe[1]
        power[pl.ds(0, half), :] = jnp.zeros((half, LANES), F32)
        power[pl.ds(half, patch), :] = pr * pr + pi * pi
        power[pl.ds(half + patch, half), :] = jnp.zeros((half, LANES), F32)
        for c in range(2):
            pad_up[c, pl.ds(half, half), :] = jnp.zeros((half, LANES), F32)
            pad_down[c, pl.ds(0, half), :] = jnp.zeros((half, LANES), F32)
        part[...] = jnp.zeros(part.shape, F32)

        def place(table, owner, p):
            first = table[0, p] - (owner * band - half)
            return jnp.minimum(jnp.maximum(first, 0), band), jnp.minimum(jnp.maximum(table[1, p], 0), width - patch)

        def window(source, c, first, count, column):
            block = column >> 7
            shift = column & (LANES - 1)
            back = (LANES - shift) & (LANES - 1)
            left = pltpu.roll(source[c, block, pl.ds(first, count), :], back, 1)
            right = pltpu.roll(source[c, block + 1, pl.ds(first, count), :], back, 1)
            lanes = lax.broadcasted_iota(jnp.int32, (count, LANES), 1)
            return jnp.where(lanes < LANES - shift, left, right)

        together(off_near, off_sem.at[0], off_sem.at[1]).wait()
        own_off, off_up, off_down = off.at[0], off_near.at[0, 0], off_near.at[1, 0]
        hear(0)
        tell(1)

        def halo_copy(g, p, which):
            if which == 0:
                return remote(slabs.at[0, p], halo.at[0, p], halo_send.at[0], halo_recv.at[g], (me_a, down))
            return remote(slabs.at[1, p], halo.at[1, p], halo_send.at[0], halo_recv.at[g], (me_a, up))

        for g, ps in enumerate(GROUPS):
            for p in ps:
                r, column = place(off_down, down, p)
                for c in range(2):
                    slabs[0, p, c] = window(field, c, half + r, slab_rows, column)
                halo_copy(g, p, 0).start()
                r, column = place(off_up, up, p)
                for c in range(2):
                    slabs[1, p, c] = window(field, c, r + EDGE, slab_rows, column)
                halo_copy(g, p, 1).start()

        tables = ((own_off, me_p, 2 * half), (off_up, up, 3 * half), (off_down, down, half))

        def spread_power(p, _):
            for k, (table, owner, base) in enumerate(tables):
                r, column = place(table, owner, p)
                spread[k * per_device + p, 0] = pltpu.roll(
                    power[pl.ds(base - r, half), :], column & (LANES - 1), 1)
            return 0

        lax.fori_loop(0, per_device, spread_power, 0)

        def covers(b, k, p):
            table, _, _ = tables[k]
            away = lane + (b * LANES - table[1, p])
            return (away >= 0) & (away < LANES)

        def weigh(b, _):
            total = jnp.ones((half, LANES), F32)
            for k in range(3):
                for p in range(per_device):
                    total += jnp.where(covers(b, k, p), spread[k * per_device + p, 0], 0.0)
            inverse[b] = 1.0 / total
            return 0

        lax.fori_loop(0, blocks, weigh, 0)

        hear(1)
        tell(2)
        all_edges.wait_recv()
        loads[1].wait()
        loads[2].wait()

        def grad_copy(g, p, which):
            if which == 0:
                return remote(grad.at[p, :, pl.ds(half, half), :], rims.at[0, p],
                              grad_send.at[0], grad_recv.at[g], (me_a, down))
            return remote(grad.at[p, :, pl.ds(0, half), :], rims.at[1, p],
                          grad_send.at[0], grad_recv.at[g], (me_a, up))

        lot = z * 4 + y
        mine_half = pl.ds(pl.multiple_of(core * half, half), half)
        half_copy = remote(part.at[:, pl.ds(pl.multiple_of((1 - core) * half, half), half), :], half_in,
                           group_send.at[0], group_recv.at[0], plane_peer(0, 1))

        def some_patches(g, ps):
            places = [place(own_off, me_p, p) for p in ps]
            own = [[window(wide, c, r, patch, column) for c in range(2)] for r, column in places]
            together(halo.at[:, pl.ds(ps[0], len(ps))], halo_send.at[0], halo_recv.at[g]).wait_recv()
            pr = probe[0]
            pi = probe[1]
            forward = (dft[0], dft[1])
            backward = (dft[2], dft[3])
            q, waves = [], []
            for j, p in enumerate(ps):
                above = slab_row < slab_rows - places[j][0]
                below = slab_row >= half - places[j][0]
                qr, qi = [
                    jnp.concatenate([
                        jnp.where(above, halo[0, p, c], own[j][c][:slab_rows]),
                        own[j][c][slab_rows:patch - slab_rows],
                        jnp.where(below, halo[1, p, c], own[j][c][patch - slab_rows:])], axis=0)
                    for c in range(2)
                ]
                q.append((qr, qi))
                waves.append((pr * qr - pi * qi, pr * qi + pi * qr))
            mid = [times_table(jnp.concatenate(w, axis=1), forward) for w in waves]
            spec = [table_times(backward, jnp.concatenate([m[:, :patch], m[:, patch:]], axis=0)) for m in mid]
            fixed = []
            for p, s in zip(ps, spec):
                sr, si = s[:patch], s[patch:]
                factor = amp[p] / jnp.maximum(jnp.sqrt(sr * sr + si * si), 0.5)
                fixed.append(jnp.concatenate([factor * sr, factor * si], axis=1))
            mid = [times_table(f, backward) for f in fixed]
            back = [table_times(forward, jnp.concatenate([m[:, :patch], m[:, patch:]], axis=0)) for m in mid]
            sums, changes = [part[k] for k in range(3)], []
            for j, p in enumerate(ps):
                qr, qi = q[j]
                dr = back[j][:patch] - waves[j][0]
                di = back[j][patch:] - waves[j][1]
                changes.append((dr, di))
                sums[0] += qr * dr + qi * di
                sums[1] += qr * di - qi * dr
                sums[2] += qr * qr + qi * qi
            for k in range(3):
                part[k] = sums[k]
            if g == len(GROUPS) - 1:
                half_copy.start()
            for p, (dr, di) in zip(ps, changes):
                grad[p, 0] = pr * dr + pi * di
                grad[p, 1] = pr * di - pi * dr
                grad_copy(g, p, 0).start()
                grad_copy(g, p, 1).start()

        for g, ps in enumerate(GROUPS):
            if g == len(GROUPS) - 1:
                hear(2)
            some_patches(g, ps)

        def spread_grad(k, p, source):
            table, owner, _ = tables[k]
            r, column = place(table, owner, p)
            for c in range(2):
                spread[k * per_device + p, c] = pltpu.roll(
                    source(c)[pl.ds(half - r, half), :], column & (LANES - 1), 1)

        def spread_own(p, _):
            spread_grad(0, p, lambda c: grad.at[p, c])
            return 0

        lax.fori_loop(0, per_device, spread_own, 0)

        half_copy.wait()
        total = part[:, mine_half, :] + half_in[...]
        for k in range(plane):
            lots[k] = total[:, k * share:(k + 1) * share, :]

        def part_copy(d):
            theirs = ((z + (d >> 2)) & 3) * 4 + ((y + (d & 3)) & 3)
            return remote(lots.at[theirs], parts.at[d], group_send.at[1], group_recv.at[1], plane_peer(d))

        for d in FAR_FIRST[:-1]:
            part_copy(d).start()

        def add_terms(keys, first=False, last=False):
            def body(b, _):
                total = [jnp.zeros((half, LANES), F32) if first else terms[c, b] for c in range(2)]
                for k, p in keys:
                    inside = covers(b, k, p)
                    for c in range(2):
                        total[c] += jnp.where(inside, spread[k * per_device + p, c], 0.0)
                at = pl.ds(pl.multiple_of(b * LANES, LANES), LANES)
                for c in range(2):
                    if last:
                        fresh[0, c, :, at] = field[c, b, pl.ds(half, band), :] + total[c] * inverse[b]
                    else:
                        terms[c, b] = total[c]
                return 0

            lax.fori_loop(0, blocks, body, 0)

        add_terms([(0, p) for p in range(per_device)], first=True)
        all_parts = together(parts.at[pl.ds(1, plane - 1)], group_send.at[1], group_recv.at[1])
        all_merges = together(merges.at[pl.ds(1, 3)], group_send.at[2], group_recv.at[2])
        all_shares = together(shares.at[pl.ds(0, 2 * plane - 1)], group_send.at[3], group_recv.at[3])
        place_in_line = far * 2 + (side >> 1)

        def merge_copy(d):
            return remote(merges.at[0], merges.at[d], group_send.at[2], group_recv.at[2], line_peer(d))

        def take_parts():
            all_parts.wait_recv()
            total = lots[lot]
            for d in range(1, plane):
                total += parts[d]
            merges[0] = total
            for d in range(1, 4):
                merge_copy(d).start()

        for g, ps in enumerate(GROUPS):
            if g == len(GROUPS) - 1:
                take_parts()
            together(rims.at[:, pl.ds(ps[0], len(ps))], grad_send.at[0], grad_recv.at[g]).wait_recv()
            for p in ps:
                for c in range(2):
                    pad_up[c, pl.ds(0, half), :] = rims[0, p, c]
                    pad_down[c, pl.ds(half, half), :] = rims[1, p, c]
                spread_grad(1, p, lambda c: pad_up.at[c])
                spread_grad(2, p, lambda c: pad_down.at[c])
            add_terms([(k, p) for p in ps for k in (1, 2)], last=g == len(GROUPS) - 1)

        loads[3].wait()
        high, low = split(fresh[0, 1])
        both = jnp.concatenate([high, low], axis=0)
        tile = ramp.shape[2]
        for j in range(width // tile):
            rows = pl.ds(width - tile - j * tile, width)
            twice = dot(both, ramp[0, rows, :])
            piece = twice[:band] + (twice[band:] + dot(high, ramp[1, rows, :]))
            for a in range(angles):
                filt[a, :, pl.ds(j * tile, tile)] = piece[a * rows_each:(a + 1) * rows_each]

        def swap_copy(d):
            peer = angle_peer(d)
            return remote(filt.at[peer[0]], sino.at[d], swap_send.at[0], swap_recv.at[max(d - 3, 0)], peer)

        for d in (2, 1, 3, 6, 5, 7, 4):
            swap_copy(d).start()

        slot = core * plane + lot
        share_copies = [
            remote(shares.at[slot], shares.at[slot], group_send.at[3], group_recv.at[3], plane_peer(d, other))
            for d in FAR_FIRST for other in (1, 0) if d or other
        ]

        all_merges.wait_recv()
        total = merges[place_in_line]
        for other in range(1, 4):
            total += merges[place_in_line ^ other]
        bottom = total[2] + 1.0
        for c in range(2):
            shares[slot, c] = probe[c, pl.ds(slot * share, share), :] + total[c] / bottom
        for copy in share_copies:
            copy.start()

        sino[0] = filt[me_a]

        loads[4].wait()
        loads[5].wait()
        total_recon[...] = jnp.zeros(total_recon.shape, F32)

        def back(d, _):
            @pl.when(d == 1)
            def _():
                together(sino.at[pl.ds(1, 3)], swap_send.at[0], swap_recv.at[0]).wait_recv()

            @pl.when(d >= 4)
            def _():
                together(sino.at[d], swap_send.at[0], swap_recv.at[d - 3]).wait_recv()

            a = angle_source(d)
            rows = sino[d]
            rise = pltpu.roll(rows, width - 1, 1) - rows
            for depth in range(zwin):
                for b in range(blocks):
                    at = pl.ds(b * LANES, LANES)
                    k = jnp.broadcast_to(index[a, pl.ds(depth, 1), at], (rows_each, LANES))
                    w = jnp.broadcast_to(weight[a, pl.ds(depth, 1), at], (rows_each, LANES))
                    block = k >> 7
                    inside = k & (LANES - 1)
                    lower = jnp.zeros((rows_each, LANES), F32)
                    slope = jnp.zeros((rows_each, LANES), F32)
                    for s in range(blocks):
                        here = block == s
                        cut = slice(s * LANES, (s + 1) * LANES)
                        lower = jnp.where(here, pick(rows[:, cut], inside), lower)
                        slope = jnp.where(here, pick(rise[:, cut], inside), slope)
                    total_recon[depth, :, at] += lower + w * slope
            return 0

        lax.fori_loop(0, angles, back, 0)
        for depth in range(zwin):
            recon[depth] = total_recon[depth] * (math.pi / angles)

        all_edges.wait_send()
        together(halo, halo_send.at[0], halo_recv.at[0]).wait_send()
        together(rims, grad_send.at[0], grad_recv.at[0]).wait_send()
        together(sino.at[pl.ds(1, angles - 1)], swap_send.at[0], swap_recv.at[0]).wait_send()
        all_parts.wait_send()
        all_merges.wait_send()
        all_shares.wait_recv()
        for k in range(2 * plane):
            for c in range(2):
                probe_out[c, pl.ds(k * share, share), :] = shares[k, c]
        all_shares.wait_send()

    def scratch():
        vm = pltpu.VMEM
        dma = pltpu.SemaphoreType.DMA
        slab = (2, per_device, 2, slab_rows, LANES)
        rim = (2, per_device, 2, half, LANES)
        tile = 256
        return [
            pltpu.SMEM((1, 2, per_device), jnp.int32),
            pltpu.SMEM((2, 1, 2, per_device), jnp.int32),
            vm((per_device, patch, patch), F32),
            vm((2, patch, patch), F32),
            vm((2, blocks + 1, band + patch, LANES), F32),
            vm((2, blocks + 1, band + patch, LANES), F32),
            vm((angles, zwin, width), jnp.int32),
            vm((angles, zwin, width), F32),
            vm((4, 2 * patch, 2 * patch), BF16),
            vm((2, 2 * width - tile, tile), BF16),
            vm(slab, F32),
            vm(slab, F32),
            vm((per_device, 2, patch, LANES), F32),
            vm(rim, F32),
            vm((2, patch, LANES), F32),
            vm((2, patch, LANES), F32),
            vm((2 * patch, LANES), F32),
            vm((blocks, band, LANES), F32),
            vm((3 * per_device, 2, half, LANES), F32),
            vm((2, blocks, band, LANES), F32),
            vm((angles, rows_each, width), F32),
            vm((angles, rows_each, width), F32),
            vm((zwin, rows_each, width), F32),
            vm((3, patch, LANES), F32),
            vm((3, half, LANES), F32),
            vm((plane, 3, share, LANES), F32),
            vm((plane, 3, share, LANES), F32),
            vm((4, 3, share, LANES), F32),
            vm((2 * plane, 2, share, LANES), F32),
            dma((7,)),
            dma((1,)),
            pltpu.SemaphoreType.REGULAR((3,)),
            dma((2,)),
            dma((2,)),
            dma((1,)), dma((len(GROUPS),)),
            dma((1,)), dma((len(GROUPS),)),
            dma((1,)), dma((5,)),
            dma((4,)), dma((4,)),
        ]

    return kernel, scratch


def solution(mesh):
    angles, positions = mesh.shape["angle"], mesh.shape["pos"]

    def on_device(amplitude, offsets, probe_field, object_field, interp_index, interp_weight):
        band, width = object_field.shape[2:]
        patch = probe_field.shape[1]
        zwin = interp_index.shape[1]
        kernel, scratch = make_kernel(angles, positions, patch, band, offsets.shape[1], width, zwin)
        anywhere = pl.BlockSpec(memory_space=pl.ANY)
        in_hbm = pl.BlockSpec(memory_space=pltpu.HBM)
        in_vmem = pl.BlockSpec(memory_space=pltpu.VMEM)
        rows_each = band // angles
        ready = pl.pallas_call(
            kernel,
            name="ptycho",
            out_shape=(
                jax.ShapeDtypeStruct(object_field.shape, F32),
                jax.ShapeDtypeStruct(probe_field.shape, F32),
                jax.ShapeDtypeStruct((zwin, rows_each, width), F32),
            ),
            in_specs=[in_hbm] * 8,
            out_specs=(in_vmem,) * 3,
            scratch_shapes=scratch(),
            compiler_params=pltpu.CompilerParams(
                collective_id=0, has_side_effects=True, vmem_limit_bytes=32 * 1024 * 1024
            ),
        )(
            *(
                pltpu.with_memory_space_constraint(x, pltpu.HBM)
                for x in (
                    jnp.swapaxes(offsets, 1, 2), amplitude, probe_field, object_field, interp_index, interp_weight,
                    jnp.asarray(dft_constant(patch)), jnp.asarray(ramp_constant(width, 256)),
                )
            ),
        )
        return pl.pallas_call(
            put_out,
            name="put_out",
            out_shape=(
                jax.ShapeDtypeStruct(object_field.shape, F32),
                jax.ShapeDtypeStruct(probe_field.shape, F32),
                jax.ShapeDtypeStruct((1, rows_each, zwin, width), F32),
            ),
            in_specs=[in_vmem] * 3,
            out_specs=(anywhere,) * 3,
            scratch_shapes=[pltpu.SemaphoreType.DMA((2 + zwin,))],
            compiler_params=pltpu.CompilerParams(vmem_limit_bytes=4 * 1024 * 1024),
        )(*ready)

    return jax.shard_map(
        on_device,
        mesh=mesh,
        in_specs=(
            P("angle", "pos", None, None),
            P("angle", "pos", None),
            P(),
            P("angle", None, "pos", None),
            P(),
            P(),
        ),
        out_specs=(P("angle", None, "pos", None), P(), P("pos", "angle", None, None)),
        check_vma=False,
    )
```
